32 devices in a mesh: seq: 8 (over y, x, core), adapter: 4 (over z).
Axes of the slice: x: 2, y: 2, z: 4, core: 2. Of those that a mesh axis runs over, the one named last changes fastest.
Arguments:
- hidden: bfloat16 [8, 1024, 8192], P('adapter', 'seq'), may hold values from -6 to 6
- response_base_queries: bfloat16 [8, 1024, 1024], P('adapter', 'seq'), may hold values from -6 to 6
- attention_output_gradient: bfloat16 [8, 1024, 1024], P('adapter', 'seq'), may hold values from -6 to 6
- keys: bfloat16 [6144, 128], P('seq'), may hold values from -6 to 6
- values: bfloat16 [6144, 128], P('seq'), may hold values from -6 to 6
- adapter_down_weight: bfloat16 [8, 16, 8192], P('adapter'), may hold values from -0.0625 to 0.0625
- adapter_up_weight: bfloat16 [8, 16, 1024], P('adapter'), may hold values from -1.5 to 1.5
- lengths: int32 [8], P('adapter'), may hold values from 512 to 1024
- offsets: int32 [8, 1024], P('adapter', 'seq'), may hold values from 0 to 6143, as said below
Outputs:
- adapter_down_gradient: float32 [8, 16, 8192], P('adapter', None, 'seq')
- adapter_up_gradient: float32 [8, 16, 1024], P('adapter')
- prompt_key_gradient: float32 [6144, 128], P(('seq', 'adapter'))
- prompt_value_gradient: float32 [6144, 128], P(('seq', 'adapter'))
The draws below stay inside these ranges and needn't reach their ends.
Inputs may be any that keep to these rules, and one draw needn't show every extreme that they name: Row r of every adapter has offsets in [(r // 128) * 768, (r // 128 + 1) * 768).
All inputs are finite; a program needn't handle non-finite values.
Results may differ from the reference program's by a relative error of at most 0.025.
The reference program's roundings to bfloat16 on the way count: a program that leaves them out, or rounds other values in their place, can miss the bound.
Values may be sent and summed in bfloat16 or wider, within the bound.
A program may use at most 192 MiB of HBM per device.

```python
import jax
import jax.numpy as jnp
from jax import lax

MODEL_WIDTH = 8192
GROUP = 8
HD = 128
ADAPTER_RANK = 16
PROMPT_SPAN = 768
RESP_DEV = 128
GROUP_FEATURES = 1024
SPAN = 2304
ADAPTER_COUNT = 8
PROMPT = 6144
RESP = 1024
N_SEQ = 8


def draw_keys(key, part):
    drawn = jnp.clip(jax.random.normal(jax.random.fold_in(key, 11), (PROMPT, HD), jnp.float32), -6.0, 6.0)
    return drawn.astype(jnp.bfloat16)


def draw_response_base_queries(key, part):
    drawn = jnp.clip(jax.random.normal(jax.random.fold_in(key, 13), (ADAPTER_COUNT, RESP, GROUP_FEATURES), jnp.float32), -6.0, 6.0)
    return drawn.astype(jnp.bfloat16)


def draw_offsets(key, part):
    inside = jax.random.randint(key, (ADAPTER_COUNT, RESP), 0, PROMPT_SPAN)
    anchor = jnp.arange(RESP, dtype=jnp.int32) // RESP_DEV * PROMPT_SPAN
    return (inside + anchor[None, :]).astype(jnp.int32)


def with_ends(array, own_key, smallest, top_value):
    shape = array.shape
    place = [jax.random.randint(jax.random.fold_in(own_key, axis), (), 0, shape[axis]) for axis in range(len(shape))]
    array = array.at[tuple(place)].set(smallest)
    longest = shape.index(max(shape))
    place[longest] = (place[longest] + 1) % shape[longest]
    return array.at[tuple(place)].set(top_value)


def level_of(rng, extent, shards, low, high):
    def one(position, blocks):
        steps = jax.random.uniform(jax.random.fold_in(jax.random.fold_in(rng, 6), position), (blocks,), jnp.float32, low / len(shards), high / len(shards))
        return jnp.repeat(jnp.exp(steps), extent[position] // blocks).reshape((-1,) + (1,) * (len(extent) - position - 1))

    factor_of = one(*shards[0])
    for cut in shards[1:]:
        factor_of = factor_of * one(*cut)
    return factor_of


def normal_values(rng, shape, deviation, limit, cuts=(), kind=jnp.bfloat16):
    result = deviation * jax.random.normal(rng, shape, jnp.float32)
    if cuts:
        result = result * level_of(rng, shape, cuts, -0.22, 0.18)
    return jnp.clip(result, -limit, limit).astype(kind)


def setup_inputs(seed: int = 0) -> dict:
    key_list = jax.random.split(jax.random.key(seed), 10)
    return {
        "hidden": normal_values(key_list[0], (ADAPTER_COUNT, RESP, MODEL_WIDTH), 1.0, 6.0, ((0, 4), (1, 8))),
        "response_base_queries": draw_response_base_queries(jax.random.fold_in(key_list[9], 71), 0),
        "attention_output_gradient": normal_values(key_list[2], (ADAPTER_COUNT, RESP, GROUP_FEATURES), 1.0, 6.0, ((0, 4), (1, 8))),
        "keys": draw_keys(jax.random.fold_in(key_list[9], 71), 0),
        "values": normal_values(key_list[4], (PROMPT, HD), 1.0, 6.0, ((0, 8),)),
        "adapter_down_weight": normal_values(key_list[5], (ADAPTER_COUNT, ADAPTER_RANK, MODEL_WIDTH), MODEL_WIDTH ** -0.5, 0.0625, ((0, 4),)),
        "adapter_up_weight": normal_values(key_list[6], (ADAPTER_COUNT, ADAPTER_RANK, GROUP_FEATURES), ADAPTER_RANK ** -0.5, 1.5, ((0, 4),)),
        "lengths": with_ends(jax.random.randint(key_list[7], (ADAPTER_COUNT,), RESP // 2, RESP + 1), jax.random.fold_in(key_list[7], 1), RESP // 2, RESP).astype(jnp.int32),
        "offsets": draw_offsets(jax.random.fold_in(key_list[9], 71), 0),
    }


adapter_scale = 2.0
masked_score = -1.0e30


def block_grads(query_blk, grad_blk, place_blk, key_win, value_win, first_pos):
    adapt_n, row_n, _ = query_blk.shape
    head_dim = key_win.shape[1]
    factor = head_dim ** -0.5
    query_heads = query_blk.reshape(adapt_n, row_n, GROUP, head_dim).astype(jnp.float32)
    grad_heads = grad_blk.reshape(adapt_n, row_n, GROUP, head_dim).astype(jnp.float32)
    key_pos = first_pos + jnp.arange(key_win.shape[0], dtype=jnp.int32)
    allowed = (key_pos[None, None, :] >= 0) & (key_pos[None, None, :] <= place_blk[:, :, None]) & (key_pos[None, None, :] > place_blk[:, :, None] - SPAN)
    allowed = allowed[:, :, None, :]
    scores = jnp.einsum("arhd,kd->arhk", query_heads, key_win.astype(jnp.float32)) * factor
    scores = jnp.where(allowed, scores, masked_score)
    peak_val = jnp.max(scores, axis=-1, keepdims=True)
    raised = jnp.exp(scores - peak_val)
    attn_prob = raised / jnp.sum(raised, axis=-1, keepdims=True)
    dprob = jnp.einsum("arhd,kd->arhk", grad_heads, value_win.astype(jnp.float32))
    delta = jnp.sum(attn_prob * dprob, axis=-1, keepdims=True)
    dscore = (attn_prob * (dprob - delta)).astype(jnp.bfloat16).astype(jnp.float32)
    prob_low = attn_prob.astype(jnp.bfloat16).astype(jnp.float32)
    value_part = jnp.einsum("arhk,arhd->kd", prob_low, grad_heads)
    key_part = jnp.einsum("arhk,arhd->kd", dscore, query_heads) * factor
    query_part = jnp.einsum("arhk,kd->arhd", dscore, key_win.astype(jnp.float32)) * factor
    return query_part.reshape(adapt_n, row_n, GROUP * head_dim), key_part, value_part


def reference(hidden, response_base_queries, attention_output_gradient, keys, values, adapter_down_weight, adapter_up_weight, lengths, offsets):
    def reduced_features_for(entry_tuple):
        input_matrix, a_mat, b_mat, base_matrix = entry_tuple
        reduced_matrix = jnp.dot(input_matrix, a_mat.T, preferred_element_type=jnp.float32).astype(jnp.bfloat16)
        upper_limit = jnp.dot(reduced_matrix, b_mat, preferred_element_type=jnp.float32)
        return reduced_matrix, (base_matrix.astype(jnp.float32) + adapter_scale * upper_limit).astype(jnp.bfloat16)

    reduced_features, query_rows = lax.map(reduced_features_for, (hidden, adapter_down_weight, adapter_up_weight, response_base_queries))
    row_index = jnp.arange(RESP, dtype=jnp.int32)
    live_rows = row_index[None, :] < lengths[:, None]
    grad_use = jnp.where(live_rows[:, :, None], attention_output_gradient, jnp.zeros_like(attention_output_gradient))
    query_blocks = query_rows.reshape(ADAPTER_COUNT, N_SEQ, RESP_DEV, GROUP_FEATURES).transpose(1, 0, 2, 3)
    grad_blocks = grad_use.reshape(ADAPTER_COUNT, N_SEQ, RESP_DEV, GROUP_FEATURES).transpose(1, 0, 2, 3)
    place_blocks = offsets.reshape(ADAPTER_COUNT, N_SEQ, RESP_DEV).transpose(1, 0, 2)
    leading = jnp.zeros((3 * PROMPT_SPAN, HD), jnp.bfloat16)
    keys_pad = jnp.concatenate([leading, keys], axis=0)
    values_pad = jnp.concatenate([leading, values], axis=0)
    zero_acc = jnp.zeros((PROMPT + 3 * PROMPT_SPAN, HD), jnp.float32)

    def scan_step(carry, entry_tuple):
        key_running_sum, value_running_sum = carry
        block_id, query_blk, grad_blk, place_blk = entry_tuple
        begin = (block_id * PROMPT_SPAN).astype(jnp.int32)
        key_win = lax.dynamic_slice(keys_pad, (begin, jnp.int32(0)), (4 * PROMPT_SPAN, HD))
        value_win = lax.dynamic_slice(values_pad, (begin, jnp.int32(0)), (4 * PROMPT_SPAN, HD))
        query_part, key_part, value_part = block_grads(query_blk, grad_blk, place_blk, key_win, value_win, begin - 3 * PROMPT_SPAN)
        key_old = lax.dynamic_slice(key_running_sum, (begin, jnp.int32(0)), (4 * PROMPT_SPAN, HD))
        value_old = lax.dynamic_slice(value_running_sum, (begin, jnp.int32(0)), (4 * PROMPT_SPAN, HD))
        key_running_sum = lax.dynamic_update_slice(key_running_sum, key_old + key_part, (begin, jnp.int32(0)))
        value_running_sum = lax.dynamic_update_slice(value_running_sum, value_old + value_part, (begin, jnp.int32(0)))
        return (key_running_sum, value_running_sum), query_part

    block_ids = jnp.arange(N_SEQ, dtype=jnp.int32)
    (key_running_sum, value_running_sum), query_parts = lax.scan(scan_step, (zero_acc, zero_acc), (block_ids, query_blocks, grad_blocks, place_blocks))
    query_gradient = query_parts.transpose(1, 0, 2, 3).reshape(ADAPTER_COUNT, RESP, GROUP_FEATURES).astype(jnp.bfloat16)

    def adapter_gradients(entry_tuple):
        input_matrix, reduced_matrix, query_grad_matrix, b_mat = entry_tuple
        up_gradient = adapter_scale * jnp.dot(reduced_matrix.T, query_grad_matrix, preferred_element_type=jnp.float32)
        reduced_gradient = jnp.dot(query_grad_matrix, b_mat.T, preferred_element_type=jnp.float32).astype(jnp.bfloat16)
        down_gradient = adapter_scale * jnp.dot(reduced_gradient.T, input_matrix, preferred_element_type=jnp.float32)
        return down_gradient, up_gradient

    adapter_down_gradient, adapter_up_gradient = lax.map(adapter_gradients, (hidden, reduced_features, query_gradient, adapter_up_weight))
    return adapter_down_gradient, adapter_up_gradient, key_running_sum[3 * PROMPT_SPAN:], value_running_sum[3 * PROMPT_SPAN:]
```

```python
import functools

import jax
import jax.numpy as jnp
from jax import lax
from jax.experimental import pallas as pl
from jax.experimental.pallas import tpu as pltpu
from jax.sharding import PartitionSpec as P

adapter_scale = 2.0
masked_score = -1e30
MESH = pl.DeviceIdType.MESH
VMEM = pltpu.VMEM


def to_seq(index):
    return dict(device_id={"seq": index}, device_id_type=MESH)


def to_adapter(index):
    return dict(device_id={"adapter": index}, device_id_type=MESH)


def remote(src, dst, send_sem, recv_sem, target):
    return pltpu.make_async_remote_copy(
        src_ref=src, dst_ref=dst, send_sem=send_sem, recv_sem=recv_sem, **target
    )


def dot(a, b, dims):
    return lax.dot_general(a, b, (dims, ((), ())), preferred_element_type=jnp.float32)


def attend_kernel(
    n, nz, heads, chunk,
    len_ref, hidden_hbm, base_hbm, grad_hbm, down_w, up_w, offset_ref, keys_ref, values_ref,
    down_out, up_out, prompt_out,
    low_ref, dq_ref, part, hidden, base, grad, gq_all, k_all, v_all, kt, s_ref, dp_ref, peaks, totals, inners,
    weight, delta, place_ref, acc, dq_acc, load_sem, send_sem, recv_sem,
    down, up, pair_a, pair_b, back_two, back_three, summed, total, z_in, down_in, up_in, up_mine,
    pair_send, pair_recv, back_send, back_recv, z_send, z_recv, d_send, d_recv, u_send, u_recv,
    ag_send, ag_recv,
):
    s = lax.axis_index("seq")
    core = s % 2
    partner = s + 1 - 2 * core
    adapt_n, rows, _ = base.shape
    stretch, hd = keys_ref.shape
    tiles, wide, _ = gq_all.shape
    per = tiles // adapt_n
    factor = hd**-0.5
    pieces = stretch // chunk
    loads = [
        pltpu.make_async_copy(a, b, load_sem.at[i])
        for i, (a, b) in enumerate(((hidden_hbm, hidden), (base_hbm, base), (grad_hbm, grad)))
    ]
    for c in loads:
        c.start()
    full = (k_all, v_all)
    own = (keys_ref, values_ref)

    def copy(i, src, slot, which, target):
        return remote(src, full[i].at[slot], send_sem.at[which, i], recv_sem.at[slot, i], to_seq(target))

    two_on = [copy(i, own[i], 2, 0, s + 2) for i in range(2)]
    three_on = [copy(i, own[i], 3, 1, s + 3) for i in range(2)]
    next_on = [copy(i, own[i], 1, 1, s + 1) for i in range(2)]
    hand_up = [copy(i, full[i].at[2], 3, 2, s + 1) for i in range(2)]
    hand_down = [copy(i, full[i].at[2], 1, 2, s - 1) for i in range(2)]

    def arrived(slot, i):
        @pl.when(s >= slot)
        def _():
            remote(
                full[i].at[slot], full[i].at[slot], send_sem.at[0, i], recv_sem.at[slot, i], to_seq(partner)
            ).wait_recv()

    z = lax.axis_index("adapter")
    has_three_in = (core == 1) & (s + 3 < n)

    @pl.when(s + 2 >= n)
    def _():
        back_two[...] = jnp.zeros_like(back_two)

    @pl.when(jnp.logical_not(has_three_in))
    def _():
        back_three[...] = jnp.zeros_like(back_three)

    @pl.when(core == 1)
    def _():
        pair_b[...] = jnp.zeros_like(pair_b)

    barrier = pltpu.get_barrier_semaphore()
    for i in range(1, n):
        pl.semaphore_signal(barrier, inc=1, **to_seq((s + i) % n))
    for i in range(1, nz):
        pl.semaphore_signal(barrier, inc=1, **to_adapter((z + i) % nz))
    pl.semaphore_wait(barrier, n - 1 + nz - 1)

    has_two_on = s + 2 < n
    has_three_on = (core == 1) & (s + 3 < n)
    for i in range(2):

        @pl.when(has_two_on)
        def _():
            two_on[i].start()

        @pl.when(has_three_on)
        def _():
            three_on[i].start()

        @pl.when(core == 0)
        def _():
            next_on[i].start()

    k_all[0] = keys_ref[...]
    v_all[0] = values_ref[...]
    for slot in (1, 2, 3):

        @pl.when(s < slot)
        def _():
            k_all[slot] = jnp.zeros(k_all.shape[1:], k_all.dtype)
            v_all[slot] = jnp.zeros(v_all.shape[1:], v_all.dtype)

    for c in loads:
        c.wait()
    for a in range(adapt_n):
        low = dot(hidden[a], down_w[a], ((1,), (1,))).astype(jnp.bfloat16)
        low_ref[a] = low
        place = jnp.concatenate([offset_ref[a]] * heads, axis=1) - s * stretch
        for t in range(per):
            place_ref[a * per + t] = place
        raised = dot(low, up_w[a], ((1,), (0,)))
        query = (base[a].astype(jnp.float32) + adapter_scale * raised).astype(jnp.bfloat16)
        live = s * rows + lax.broadcasted_iota(jnp.int32, (rows, 1), 0) < len_ref[a]
        g = jnp.where(live, grad[a], jnp.zeros_like(grad[a]))
        for h in range(per * heads):
            t, at_row = a * per + h // heads, (h % heads) * rows
            gq_all[t, at_row : at_row + rows, :hd] = g[:, h * hd : (h + 1) * hd]
            gq_all[t, at_row : at_row + rows, hd:] = query[:, h * hd : (h + 1) * hd]

    def hand(i):
        @pl.when(s >= 2)
        def _():
            @pl.when(core == 0)
            def _():
                hand_up[i].start()

            @pl.when(core == 1)
            def _():
                hand_down[i].start()

    def at(piece):
        return slice(piece * chunk, (piece + 1) * chunk)

    def before(piece, place):
        pos = piece * chunk + lax.broadcasted_iota(jnp.int32, (chunk, wide), 0)
        return pos <= place

    spots = {0: 0, 3: 1, 1: 2, 2: 3}

    def turned(d):
        kt[:, spots[d] * stretch : (spots[d] + 1) * stretch] = k_all[d].T

    def product(source, d, piece, other):
        return dot(source[d, at(piece), :], other, ((1,), (1,)))

    far_bias = jnp.where(s >= 3, 0.0, masked_score)

    @pl.loop(0, tiles)
    def _(t):
        q = gq_all[t, :, hd:]
        g = gq_all[t, :, :hd]
        for piece in range(pieces):
            s_ref[t, at(piece), :] = product(k_all, 0, piece, q) * factor
            dp_ref[t, at(piece), :] = product(v_all, 0, piece, g)

    def scores_of(d):
        @pl.loop(0, tiles)
        def _(t):
            q = gq_all[t, :, hd:]
            peak = jnp.full((1, wide), masked_score, jnp.float32)
            for piece in range(pieces):
                score = product(k_all, d or 3, piece, q) * factor
                if d == 0:
                    near = before(piece, place_ref[t])
                    score = jnp.where(near, s_ref[t, at(piece), :], score + far_bias)
                s_ref[t, at(d * pieces + piece), :] = score
                peak = jnp.maximum(peak, jnp.max(score, axis=0, keepdims=True))
            peaks[d, t] = peak

    def raise_of(d):
        @pl.loop(0, tiles)
        def _(t):
            g = gq_all[t, :, :hd]
            peak = peaks[d, t]
            total = jnp.zeros((1, wide), jnp.float32)
            inner = jnp.zeros((1, wide), jnp.float32)
            for piece in range(pieces):
                spot = at(d * pieces + piece)
                e = jnp.exp(s_ref[t, spot, :] - peak)
                dp = product(v_all, d or 3, piece, g)
                if d == 0:
                    dp = jnp.where(before(piece, place_ref[t]), dp_ref[t, spot, :], dp)
                s_ref[t, spot, :] = e
                dp_ref[t, spot, :] = dp
                total = total + jnp.sum(e, axis=0, keepdims=True)
                inner = inner + jnp.sum(e * dp, axis=0, keepdims=True)
            totals[d, t] = total
            inners[d, t] = inner

    arrived(2, 0)
    hand(0)
    turned(2)
    scores_of(2)
    arrived(1, 0)
    turned(1)
    scores_of(1)
    arrived(2, 1)
    hand(1)
    raise_of(2)
    arrived(1, 1)
    raise_of(1)
    arrived(3, 0)
    turned(3)
    turned(0)
    scores_of(0)
    arrived(3, 1)
    raise_of(0)

    @pl.loop(0, tiles)
    def _(t):
        tops = [peaks[0, t]] + [jnp.where(s >= d, peaks[d, t], masked_score) for d in (1, 2)]
        peak = jnp.maximum(jnp.maximum(tops[0], tops[1]), tops[2])
        shares = [jnp.exp(top - peak) for top in tops]
        total = jnp.zeros((1, wide), jnp.float32)
        inner = jnp.zeros((1, wide), jnp.float32)
        for d, share in enumerate(shares):
            total = total + totals[d, t] * share
            inner = inner + inners[d, t] * share
        inverse = 1.0 / total
        for d, share in enumerate(shares):
            weight[d, t] = share * inverse
        delta[t] = inner * inverse

    def split(piece, t, d, value):
        if d:
            return [value.astype(jnp.bfloat16)]
        near = before(piece, place_ref[t])
        return [
            jnp.where(near, value, 0.0).astype(jnp.bfloat16),
            jnp.where(near, 0.0, value).astype(jnp.bfloat16),
        ]

    def gather_up(d, i):
        acc[...] = jnp.zeros_like(acc)
        blocks = (d,) if d else (0, 3)

        @pl.loop(0, tiles)
        def _(t):
            other = gq_all[t]
            share = weight[d, t]
            lows = [[] for _ in blocks]
            for piece in range(pieces):
                spot = at(d * pieces + piece)
                value = s_ref[t, spot, :] * share
                if i == 0:
                    value = value * (dp_ref[t, spot, :] - delta[t])
                for j, low in enumerate(split(piece, t, d, value)):
                    both = dot(low, other, ((1,), (0,)))
                    acc[j, at(piece), :] += both[:, :hd] if i else both[:, hd:]
                    lows[j].append(low)
            if i == 0:
                begin = spots[d] * stretch
                ds = jnp.concatenate(sum(lows, []), axis=0)
                dq = dot(kt[:, begin : begin + len(blocks) * stretch], ds, ((1,), (0,)))
                if d == 0:
                    dq_acc[t] = dq
                else:
                    dq_acc[t] += dq

        for j, block in enumerate(blocks):
            out = acc[j]
            part[block, i] = (out if i else out * factor).astype(jnp.bfloat16)

    width = down_out.shape[1]
    quarter = prompt_out.shape[1]
    has_far = (core == 0) & (s >= 3)

    def pair_copy(d, to, i, j):
        return remote(part.at[d, i], to.at[i], pair_send.at[j, i], pair_recv.at[j, i], to_seq(partner))

    zero_to_one = [pair_copy(1, pair_a, i, 0) for i in range(2)]
    one_to_zero = [pair_copy(3, pair_a, i, 0) for i in range(2)]
    near_back = [pair_copy(1, pair_b, i, 1) for i in range(2)]
    far_back = [
        remote(part.at[3, i], back_three.at[i], back_send.at[1, i], back_recv.at[1, i], to_seq(s - 3))
        for i in range(2)
    ]
    two_back = [
        remote(summed.at[i], back_two.at[i], back_send.at[0, i], back_recv.at[0, i], to_seq(s - 2))
        for i in range(2)
    ]
    downs, ups, gathers = [], [], []
    for i in range(1, n):
        peer = (s + i) % n
        columns = pl.ds(pl.multiple_of(peer * width, 128), width)
        downs.append(
            remote(down.at[:, columns], down_in.at[i - 1], d_send.at[i - 1], d_recv.at[i - 1], to_seq(peer))
        )
        ups.append(remote(up.at[peer], up_in.at[i - 1], u_send.at[i - 1], u_recv.at[i - 1], to_seq(peer)))
        gathers.append(remote(up_mine, up_out.at[s], ag_send.at[i - 1], ag_recv.at[i - 1], to_seq(peer)))

    def sum_pair(i):
        zero_to_one[i].wait_recv()
        summed[i] = (part[2, i].astype(jnp.float32) + pair_a[i].astype(jnp.float32)).astype(jnp.bfloat16)

        @pl.when(s >= 2)
        def _():
            two_back[i].start()

    spread = [[], []]

    def owner(i):
        @pl.when(core == 0)
        def _():
            near_back[i].wait_recv()

        @pl.when(s + 2 < n)
        def _():
            two_back[i].wait_recv()

        @pl.when(has_three_in)
        def _():
            far_back[i].wait_recv()

        total[i] = (
            part[0, i].astype(jnp.float32)
            + pair_b[i].astype(jnp.float32)
            + back_two[i].astype(jnp.float32)
            + back_three[i].astype(jnp.float32)
        ).astype(jnp.bfloat16)
        for j in range(1, nz):
            peer = (z + j) % nz
            c = remote(
                total.at[i, pl.ds(pl.multiple_of(peer * quarter, 16), quarter), :],
                z_in.at[j - 1, i], z_send.at[j - 1, i], z_recv.at[j - 1, i], to_adapter(peer),
            )
            c.start()
            spread[i].append(c)

    def prompt_sum(i):
        mine = total[i, pl.ds(pl.multiple_of(z * quarter, 16), quarter), :].astype(jnp.float32)
        for j, c in enumerate(spread[i]):
            c.wait_recv()
            mine = mine + z_in[j, i].astype(jnp.float32)
        prompt_out[i] = mine

    def far_out(i):
        @pl.when(core == 1)
        def _():
            one_to_zero[i].start()

        @pl.when(has_far)
        def _():
            far_back[i].start()

    def near_out(i):
        @pl.when(core == 0)
        def _():
            zero_to_one[i].start()

        @pl.when(core == 1)
        def _():
            near_back[i].start()

    def sum_on(which, i):
        @pl.when(core == which)
        def _():
            sum_pair(i)

    gather_up(0, 1)
    far_out(1)
    gather_up(2, 1)
    sum_on(0, 1)
    gather_up(1, 1)
    near_out(1)
    gather_up(0, 0)
    far_out(0)
    sum_on(1, 1)
    gather_up(2, 0)
    sum_on(0, 0)
    owner(1)
    gather_up(1, 0)
    near_out(0)

    @pl.loop(0, tiles)
    def _(t):
        dq_ref[t] = (dq_acc[t] * factor).T.astype(jnp.bfloat16)

    _, rank, feature_n = up_w.shape
    group = feature_n // hd
    shards, up_rows, _ = up.shape
    for a in range(adapt_n):
        small = jnp.zeros((rows, rank), jnp.float32)
        for h in range(group):
            place = a * group + h
            dq_h = dq_ref[place // heads, (place % heads) * rows : (place % heads + 1) * rows, :]
            up_h = dot(low_ref[a], dq_h, ((0,), (0,)))
            for r in range(0, rank, min(rank, up_rows)):
                spot = (h * adapt_n + a) * rank + r
                begin = spot % up_rows
                up[spot // up_rows, begin : begin + min(rank, up_rows), :] = up_h[r : r + min(rank, up_rows)]
            small = small + dot(dq_h, up_w[a, :, h * hd : (h + 1) * hd], ((1,), (1,)))
        down[a * rank : (a + 1) * rank, :] = dot(
            small.astype(jnp.bfloat16), hidden[a], ((0,), (0,))
        ).astype(jnp.bfloat16)
        if a == 0:
            sum_on(1, 0)
    for c in ups + downs:
        c.start()
    owner(0)
    mine = up[s]
    for i, c in enumerate(ups):
        c.wait_recv()
        mine = mine + up_in[i]
    up_mine[...] = mine
    for c in gathers:
        c.start()
    up_out[s] = mine
    mine = down[:, pl.ds(pl.multiple_of(s * width, 128), width)].astype(jnp.float32)
    for i, c in enumerate(downs):
        c.wait_recv()
        mine = mine + down_in[i].astype(jnp.float32)
    down_out[...] = mine
    prompt_sum(1)
    prompt_sum(0)
    for c in gathers:
        c.wait_recv()
    for c in downs + ups + gathers + spread[0] + spread[1] + zero_to_one:
        c.wait_send()
    for i in range(2):

        @pl.when(core == 1)
        def _():
            near_back[i].wait_send()

        @pl.when(has_far)
        def _():
            far_back[i].wait_send()

        @pl.when(s >= 2)
        def _():
            two_back[i].wait_send()

    for i in range(2):

        @pl.when(has_two_on)
        def _():
            two_on[i].wait_send()

        @pl.when(has_three_on)
        def _():
            three_on[i].wait_send()

        @pl.when(core == 0)
        def _():
            next_on[i].wait_send()

        @pl.when(s >= 2)
        def _():
            hand_up[i].wait_send()


def gradients(n, nz, hidden, base, grad, down_w, up_w, lengths, offsets, keys, values):
    adapt_n, row_n, feature_n = base.shape
    stretch, hd = keys.shape
    rank, model = down_w.shape[1:]
    ranks = adapt_n * rank
    heads = 4
    wide = heads * row_n
    tiles = adapt_n * feature_n // (hd * heads)
    chunk = 256 if stretch % 256 == 0 else stretch
    quarter = stretch // nz
    up_shape = (n, ranks * feature_n // (n * hd), hd)
    spec = pl.BlockSpec(memory_space=VMEM)
    anywhere = pl.BlockSpec(memory_space=pl.ANY)
    dma = pltpu.SemaphoreType.DMA
    bf16 = jnp.bfloat16
    f32 = jnp.float32
    block = VMEM((2, stretch, hd), bf16)
    stat = VMEM((3, tiles, 1, wide), f32)
    return pl.pallas_call(
        functools.partial(attend_kernel, n, nz, heads, chunk),
        out_shape=(
            jax.ShapeDtypeStruct((ranks, model // n), f32),
            jax.ShapeDtypeStruct(up_shape, f32),
            jax.ShapeDtypeStruct((2, quarter, hd), f32),
        ),
        in_specs=[pl.BlockSpec(memory_space=pltpu.SMEM)] + [anywhere] * 3 + [spec] * 5,
        out_specs=(spec, spec, spec),
        scratch_shapes=[
            VMEM((adapt_n, row_n, rank), bf16),
            VMEM((tiles, wide, hd), bf16),
            VMEM((4, 2, stretch, hd), bf16),
            VMEM(hidden.shape, bf16),
            VMEM(base.shape, bf16),
            VMEM(grad.shape, bf16),
            VMEM((tiles, wide, 2 * hd), bf16),
            VMEM((4, stretch, hd), bf16),
            VMEM((4, stretch, hd), bf16),
            VMEM((hd, 4 * stretch), bf16),
            VMEM((tiles, 3 * stretch, wide), f32),
            VMEM((tiles, 3 * stretch, wide), f32),
            stat, stat, stat, stat,
            VMEM((tiles, 1, wide), f32),
            VMEM((tiles, 1, wide), jnp.int32),
            VMEM((2, stretch, hd), f32),
            VMEM((tiles, hd, wide), f32),
            dma((3,)), dma((3, 2)), dma((4, 2)),
            VMEM((ranks, model), bf16),
            VMEM(up_shape, f32),
            block, block, block, block, block, block,
            VMEM((nz - 1, 2, quarter, hd), bf16),
            VMEM((n - 1, ranks, model // n), bf16),
            VMEM((n - 1,) + up_shape[1:], f32),
            VMEM(up_shape[1:], f32),
            dma((2, 2)), dma((2, 2)), dma((2, 2)), dma((2, 2)), dma((nz - 1, 2)), dma((nz - 1, 2)),
            dma((n - 1,)), dma((n - 1,)), dma((n - 1,)), dma((n - 1,)), dma((n - 1,)), dma((n - 1,)),
        ],
        compiler_params=pltpu.CompilerParams(
            collective_id=0, has_side_effects=True, vmem_limit_bytes=60 * 1024 * 1024
        ),
        name="gradients",
    )(lengths, hidden, base, grad, down_w, up_w, offsets[:, None, :], keys, values)


def finish_kernel(down_hbm, up_hbm, prompt_hbm, down_out, up_out, key_out, value_out, down, up, sems):
    adapt_n, rank, _ = down_out.shape
    _, up_rows, hd = up.shape
    pairs = ((up_hbm, up), (down_hbm, down), (prompt_hbm.at[0], key_out), (prompt_hbm.at[1], value_out))
    loads = [pltpu.make_async_copy(a, b, sems.at[i]) for i, (a, b) in enumerate(pairs)]
    for c in loads:
        c.start()
    for c in loads:
        c.wait()
    for a in range(adapt_n):
        down_out[a] = adapter_scale * down[a * rank : (a + 1) * rank, :]
        for h in range(up_out.shape[2] // hd):
            for r in range(0, rank, min(rank, up_rows)):
                at = (h * adapt_n + a) * rank + r
                begin = at % up_rows
                size = min(rank, up_rows)
                up_out[a, r : r + size, h * hd : (h + 1) * hd] = (
                    adapter_scale * up[at // up_rows, begin : begin + size, :]
                )


def finish(up_w, down, up, prompt):
    adapt_n, rank, feature_n = up_w.shape
    f32 = jnp.float32
    spec = pl.BlockSpec(memory_space=VMEM)
    side = jax.ShapeDtypeStruct(prompt.shape[1:], f32)
    return pl.pallas_call(
        finish_kernel,
        out_shape=(
            jax.ShapeDtypeStruct((adapt_n, rank, down.shape[1]), f32),
            jax.ShapeDtypeStruct(up_w.shape, f32),
            side,
            side,
        ),
        in_specs=[pl.BlockSpec(memory_space=pl.ANY)] * 3,
        out_specs=(spec,) * 4,
        scratch_shapes=[VMEM(down.shape, f32), VMEM(up.shape, f32), pltpu.SemaphoreType.DMA((4,))],
        name="finish",
    )(down, up, prompt)


def local(
    hidden,
    response_base_queries,
    attention_output_gradient,
    keys,
    values,
    adapter_down_weight,
    adapter_up_weight,
    lengths,
    offsets,
):
    n = lax.axis_size("seq")
    nz = lax.axis_size("adapter")
    sums = gradients(
        n,
        nz,
        hidden,
        response_base_queries,
        attention_output_gradient,
        adapter_down_weight,
        adapter_up_weight,
        lengths,
        offsets,
        keys,
        values,
    )
    return finish(adapter_up_weight, *sums)


def solution(mesh):
    return jax.shard_map(
        local,
        mesh=mesh,
        in_specs=(
            P("adapter", "seq", None),
            P("adapter", "seq", None),
            P("adapter", "seq", None),
            P("seq", None),
            P("seq", None),
            P("adapter", None, None),
            P("adapter", None, None),
            P("adapter"),
            P("adapter", "seq"),
        ),
        out_specs=(
            P("adapter", None, "seq"),
            P("adapter", None, None),
            P(("seq", "adapter"), None),
            P(("seq", "adapter"), None),
        ),
        check_vma=False,
    )
```

```python
import functools

import jax
import jax.numpy as jnp
from jax import lax
from jax.experimental import pallas as pl
from jax.experimental.pallas import tpu as pltpu
from jax.sharding import PartitionSpec as P

adapter_scale = 2.0
masked_score = -1e30
MESH = pl.DeviceIdType.MESH
VMEM = pltpu.VMEM


def to_seq(index):
    return dict(device_id={"seq": index}, device_id_type=MESH)


def to_adapter(index):
    return dict(device_id={"adapter": index}, device_id_type=MESH)


def remote(src, dst, send_sem, recv_sem, target):
    return pltpu.make_async_remote_copy(
        src_ref=src, dst_ref=dst, send_sem=send_sem, recv_sem=recv_sem, **target
    )


def dot(a, b, dims):
    return lax.dot_general(a, b, (dims, ((), ())), preferred_element_type=jnp.float32)


def attend_kernel(
    n, nz, heads, chunk,
    len_ref, hidden_hbm, base_hbm, grad_hbm, down_w, up_w, offset_ref, keys_ref, values_ref,
    down_out, up_out, prompt_out,
    low_ref, dq_ref, part, hidden, base, grad, gq_all, k_all, v_all, kt, s_ref, dp_ref, peaks, totals, inners,
    weight, delta, place_ref, acc, dq_acc, load_sem, send_sem, recv_sem,
    down, up, pair_a, pair_b, back_two, back_three, summed, total, z_in, down_in, up_in, up_mine,
    pair_send, pair_recv, back_send, back_recv, z_send, z_recv, d_send, d_recv, u_send, u_recv,
    ag_send, ag_recv,
):
    s = lax.axis_index("seq")
    core = s % 2
    partner = s + 1 - 2 * core
    adapt_n, rows, _ = base.shape
    stretch, hd = keys_ref.shape
    tiles, wide, _ = gq_all.shape
    per = tiles // adapt_n
    factor = hd**-0.5
    pieces = stretch // chunk
    loads = [
        pltpu.make_async_copy(a, b, load_sem.at[i])
        for i, (a, b) in enumerate(((hidden_hbm, hidden), (base_hbm, base), (grad_hbm, grad)))
    ]
    for c in loads:
        c.start()
    full = (k_all, v_all)
    own = (keys_ref, values_ref)

    def copy(i, src, slot, which, target):
        return remote(src, full[i].at[slot], send_sem.at[which, i], recv_sem.at[slot, i], to_seq(target))

    two_on = [copy(i, own[i], 2, 0, s + 2) for i in range(2)]
    three_on = [copy(i, own[i], 3, 1, s + 3) for i in range(2)]
    next_on = [copy(i, own[i], 1, 1, s + 1) for i in range(2)]
    hand_up = [copy(i, full[i].at[2], 3, 2, s + 1) for i in range(2)]
    hand_down = [copy(i, full[i].at[2], 1, 2, s - 1) for i in range(2)]

    def arrived(slot, i):
        @pl.when(s >= slot)
        def _():
            remote(
                full[i].at[slot], full[i].at[slot], send_sem.at[0, i], recv_sem.at[slot, i], to_seq(partner)
            ).wait_recv()

    z = lax.axis_index("adapter")
    has_three_in = (core == 1) & (s + 3 < n)

    @pl.when(s + 2 >= n)
    def _():
        back_two[...] = jnp.zeros_like(back_two)

    @pl.when(jnp.logical_not(has_three_in))
    def _():
        back_three[...] = jnp.zeros_like(back_three)

    @pl.when(core == 1)
    def _():
        pair_b[...] = jnp.zeros_like(pair_b)

    barrier = pltpu.get_barrier_semaphore()
    for i in range(1, n):
        pl.semaphore_signal(barrier, inc=1, **to_seq((s + i) % n))
    for i in range(1, nz):
        pl.semaphore_signal(barrier, inc=1, **to_adapter((z + i) % nz))
    pl.semaphore_wait(barrier, n - 1 + nz - 1)

    has_two_on = s + 2 < n
    has_three_on = (core == 1) & (s + 3 < n)
    for i in range(2):

        @pl.when(has_two_on)
        def _():
            two_on[i].start()

        @pl.when(has_three_on)
        def _():
            three_on[i].start()

        @pl.when(core == 0)
        def _():
            next_on[i].start()

    k_all[0] = keys_ref[...]
    v_all[0] = values_ref[...]
    for slot in (1, 2, 3):

        @pl.when(s < slot)
        def _():
            k_all[slot] = jnp.zeros(k_all.shape[1:], k_all.dtype)
            v_all[slot] = jnp.zeros(v_all.shape[1:], v_all.dtype)

    for c in loads:
        c.wait()
    for a in range(adapt_n):
        low = dot(hidden[a], down_w[a], ((1,), (1,))).astype(jnp.bfloat16)
        low_ref[a] = low
        place = jnp.concatenate([offset_ref[a]] * heads, axis=1) - s * stretch
        for t in range(per):
            place_ref[a * per + t] = place
        raised = dot(low, up_w[a], ((1,), (0,)))
        query = (base[a].astype(jnp.float32) + adapter_scale * raised).astype(jnp.bfloat16)
        live = s * rows + lax.broadcasted_iota(jnp.int32, (rows, 1), 0) < len_ref[a]
        g = jnp.where(live, grad[a], jnp.zeros_like(grad[a]))
        for h in range(per * heads):
            t, at_row = a * per + h // heads, (h % heads) * rows
            gq_all[t, at_row : at_row + rows, :hd] = g[:, h * hd : (h + 1) * hd]
            gq_all[t, at_row : at_row + rows, hd:] = query[:, h * hd : (h + 1) * hd]

    def hand(i):
        @pl.when(s >= 2)
        def _():
            @pl.when(core == 0)
            def _():
                hand_up[i].start()

            @pl.when(core == 1)
            def _():
                hand_down[i].start()

    def at(piece):
        return slice(piece * chunk, (piece + 1) * chunk)

    def before(piece, place):
        pos = piece * chunk + lax.broadcasted_iota(jnp.int32, (chunk, wide), 0)
        return pos <= place

    spots = {0: 0, 3: 1, 1: 2, 2: 3}

    def turned(d):
        kt[:, spots[d] * stretch : (spots[d] + 1) * stretch] = k_all[d].T

    def product(source, d, piece, other):
        return dot(source[d, at(piece), :], other, ((1,), (1,)))

    far_bias = jnp.where(s >= 3, 0.0, masked_score)

    @pl.loop(0, tiles)
    def _(t):
        q = gq_all[t, :, hd:]
        g = gq_all[t, :, :hd]
        for piece in range(pieces):
            s_ref[t, at(piece), :] = product(k_all, 0, piece, q) * factor
            dp_ref[t, at(piece), :] = product(v_all, 0, piece, g)

    def scores_of(d):
        @pl.loop(0, tiles)
        def _(t):
            q = gq_all[t, :, hd:]
            peak = jnp.full((1, wide), masked_score, jnp.float32)
            for piece in range(pieces):
                score = product(k_all, d or 3, piece, q) * factor
                if d == 0:
                    near = before(piece, place_ref[t])
                    score = jnp.where(near, s_ref[t, at(piece), :], score + far_bias)
                s_ref[t, at(d * pieces + piece), :] = score
                peak = jnp.maximum(peak, jnp.max(score, axis=0, keepdims=True))
            peaks[d, t] = peak

    def raise_of(d):
        @pl.loop(0, tiles)
        def _(t):
            g = gq_all[t, :, :hd]
            peak = peaks[d, t]
            total = jnp.zeros((1, wide), jnp.float32)
            inner = jnp.zeros((1, wide), jnp.float32)
            for piece in range(pieces):
                spot = at(d * pieces + piece)
                e = jnp.exp(s_ref[t, spot, :] - peak)
                dp = product(v_all, d or 3, piece, g)
                if d == 0:
                    dp = jnp.where(before(piece, place_ref[t]), dp_ref[t, spot, :], dp)
                s_ref[t, spot, :] = e
                dp_ref[t, spot, :] = dp
                total = total + jnp.sum(e, axis=0, keepdims=True)
                inner = inner + jnp.sum(e * dp, axis=0, keepdims=True)
            totals[d, t] = total
            inners[d, t] = inner

    arrived(2, 0)
    hand(0)
    turned(2)
    scores_of(2)
    arrived(1, 0)
    turned(1)
    scores_of(1)
    arrived(2, 1)
    hand(1)
    raise_of(2)
    arrived(1, 1)
    raise_of(1)
    arrived(3, 0)
    turned(3)
    turned(0)
    scores_of(0)
    arrived(3, 1)
    raise_of(0)

    @pl.loop(0, tiles)
    def _(t):
        tops = [peaks[0, t]] + [jnp.where(s >= d, peaks[d, t], masked_score) for d in (1, 2)]
        peak = jnp.maximum(jnp.maximum(tops[0], tops[1]), tops[2])
        shares = [jnp.exp(top - peak) for top in tops]
        total = jnp.zeros((1, wide), jnp.float32)
        inner = jnp.zeros((1, wide), jnp.float32)
        for d, share in enumerate(shares):
            total = total + totals[d, t] * share
            inner = inner + inners[d, t] * share
        inverse = 1.0 / total
        for d, share in enumerate(shares):
            weight[d, t] = share * inverse
        delta[t] = inner * inverse

    def rows_of(unit, piece):
        if isinstance(unit, int):
            return at(unit * pieces + piece)
        return pl.ds(pl.multiple_of(unit * stretch + piece * chunk, chunk), chunk)

    def gather_up(block, i, first=0, last=tiles):
        static = isinstance(block, int)
        unit = 0 if static else block
        if first == 0:
            acc[...] = jnp.zeros_like(acc)

        @pl.loop(first, last)
        def _(t):
            other = gq_all[t]
            share = weight[unit, t]
            lows = []
            for piece in range(pieces):
                spot = rows_of(unit, piece)
                value = s_ref[t, spot, :] * share
                if i == 0:
                    value = value * (dp_ref[t, spot, :] - delta[t])
                if static:
                    near = before(piece, place_ref[t])
                    value = jnp.where(near, 0.0, value) if block else jnp.where(near, value, 0.0)
                low = value.astype(jnp.bfloat16)
                both = dot(low, other, ((1,), (0,)))
                acc[at(piece), :] += both[:, :hd] if i else both[:, hd:]
                lows.append(low)
            if i == 0:
                if static:
                    turned_block = kt[:, spots[block] * stretch : (spots[block] + 1) * stretch]
                else:
                    turned_block = kt[:, pl.ds(pl.multiple_of((block + 1) * stretch, stretch), stretch)]
                dq = dot(turned_block, jnp.concatenate(lows, axis=0), ((1,), (0,)))
                if static and block == 3:
                    dq_acc[t] = dq
                else:
                    dq_acc[t] += dq

        if last == tiles:
            out = acc[...]
            part[block, i] = (out if i else out * factor).astype(jnp.bfloat16)

    width = down_out.shape[1]
    quarter = prompt_out.shape[1]
    has_far = (core == 0) & (s >= 3)

    def pair_copy(d, to, i, j):
        return remote(part.at[d, i], to.at[i], pair_send.at[j, i], pair_recv.at[j, i], to_seq(partner))

    zero_to_one = [pair_copy(1, pair_a, i, 0) for i in range(2)]
    one_to_zero = [pair_copy(3, pair_a, i, 0) for i in range(2)]
    near_back = [pair_copy(1, pair_b, i, 1) for i in range(2)]
    far_back = [
        remote(part.at[3, i], back_three.at[i], back_send.at[1, i], back_recv.at[1, i], to_seq(s - 3))
        for i in range(2)
    ]
    two_back = [
        remote(summed.at[i], back_two.at[i], back_send.at[0, i], back_recv.at[0, i], to_seq(s - 2))
        for i in range(2)
    ]
    downs, ups, gathers = [], [], []
    for i in range(1, n):
        peer = (s + i) % n
        columns = pl.ds(pl.multiple_of(peer * width, 128), width)
        downs.append(
            remote(down.at[:, columns], down_in.at[i - 1], d_send.at[i - 1], d_recv.at[i - 1], to_seq(peer))
        )
        ups.append(remote(up.at[peer], up_in.at[i - 1], u_send.at[i - 1], u_recv.at[i - 1], to_seq(peer)))
        gathers.append(remote(up_mine, up_out.at[s], ag_send.at[i - 1], ag_recv.at[i - 1], to_seq(peer)))

    def sum_pair(i):
        zero_to_one[i].wait_recv()
        summed[i] = (part[2, i].astype(jnp.float32) + pair_a[i].astype(jnp.float32)).astype(jnp.bfloat16)

        @pl.when(s >= 2)
        def _():
            two_back[i].start()

    spread = [[], []]

    def owner(i):
        @pl.when(core == 0)
        def _():
            near_back[i].wait_recv()

        @pl.when(s + 2 < n)
        def _():
            two_back[i].wait_recv()

        @pl.when(has_three_in)
        def _():
            far_back[i].wait_recv()

        total[i] = (
            part[0, i].astype(jnp.float32)
            + pair_b[i].astype(jnp.float32)
            + back_two[i].astype(jnp.float32)
            + back_three[i].astype(jnp.float32)
        ).astype(jnp.bfloat16)
        for j in range(1, nz):
            peer = (z + j) % nz
            c = remote(
                total.at[i, pl.ds(pl.multiple_of(peer * quarter, 16), quarter), :],
                z_in.at[j - 1, i], z_send.at[j - 1, i], z_recv.at[j - 1, i], to_adapter(peer),
            )
            c.start()
            spread[i].append(c)

    def prompt_sum(i):
        mine = total[i, pl.ds(pl.multiple_of(z * quarter, 16), quarter), :].astype(jnp.float32)
        for j, c in enumerate(spread[i]):
            c.wait_recv()
            mine = mine + z_in[j, i].astype(jnp.float32)
        prompt_out[i] = mine

    def far_out(i):
        @pl.when(core == 1)
        def _():
            one_to_zero[i].start()

        @pl.when(has_far)
        def _():
            far_back[i].start()

    def sum_on(which, i):
        @pl.when(core == which)
        def _():
            sum_pair(i)

    second = 1 + core
    third = 2 - core
    middle = tiles // 2

    def second_out(i):
        gather_up(second, i)

        @pl.when(core == 0)
        def _():
            zero_to_one[i].start()

    def third_out(i):
        gather_up(third, i, 0, middle)
        sum_on(1, i)
        gather_up(third, i, middle, tiles)
        sum_on(0, i)

        @pl.when(core == 1)
        def _():
            near_back[i].start()

    gather_up(3, 1)
    far_out(1)
    second_out(1)
    third_out(1)
    gather_up(3, 0)
    far_out(0)
    gather_up(0, 1)
    second_out(0)
    owner(1)
    third_out(0)
    gather_up(0, 0)

    @pl.loop(0, tiles)
    def _(t):
        dq_ref[t] = (dq_acc[t] * factor).T.astype(jnp.bfloat16)

    _, rank, feature_n = up_w.shape
    group = feature_n // hd
    shards, up_rows, _ = up.shape
    smalls = []
    for a in range(adapt_n):
        small = jnp.zeros((rows, rank), jnp.float32)
        for h in range(group):
            place = a * group + h
            dq_h = dq_ref[place // heads, (place % heads) * rows : (place % heads + 1) * rows, :]
            up_h = dot(low_ref[a], dq_h, ((0,), (0,)))
            for r in range(0, rank, min(rank, up_rows)):
                spot = (h * adapt_n + a) * rank + r
                begin = spot % up_rows
                up[spot // up_rows, begin : begin + min(rank, up_rows), :] = up_h[r : r + min(rank, up_rows)]
            small = small + dot(dq_h, up_w[a, :, h * hd : (h + 1) * hd], ((1,), (1,)))
        smalls.append(small.astype(jnp.bfloat16))
    for c in ups:
        c.start()
    for a in range(adapt_n):
        down[a * rank : (a + 1) * rank, :] = dot(smalls[a], hidden[a], ((0,), (0,))).astype(jnp.bfloat16)
    mine = up[s]
    for i, c in enumerate(ups):
        c.wait_recv()
        mine = mine + up_in[i]
    up_mine[...] = mine
    for c in gathers + downs:
        c.start()
    up_out[s] = mine
    owner(0)
    mine = down[:, pl.ds(pl.multiple_of(s * width, 128), width)].astype(jnp.float32)
    for i, c in enumerate(downs):
        c.wait_recv()
        mine = mine + down_in[i].astype(jnp.float32)
    down_out[...] = mine
    prompt_sum(1)
    prompt_sum(0)
    for c in gathers:
        c.wait_recv()
    for c in downs + ups + gathers + spread[0] + spread[1] + zero_to_one:
        c.wait_send()
    for i in range(2):

        @pl.when(core == 1)
        def _():
            near_back[i].wait_send()

        @pl.when(has_far)
        def _():
            far_back[i].wait_send()

        @pl.when(s >= 2)
        def _():
            two_back[i].wait_send()

    for i in range(2):

        @pl.when(has_two_on)
        def _():
            two_on[i].wait_send()

        @pl.when(has_three_on)
        def _():
            three_on[i].wait_send()

        @pl.when(core == 0)
        def _():
            next_on[i].wait_send()

        @pl.when(s >= 2)
        def _():
            hand_up[i].wait_send()


def gradients(n, nz, hidden, base, grad, down_w, up_w, lengths, offsets, keys, values):
    adapt_n, row_n, feature_n = base.shape
    stretch, hd = keys.shape
    rank, model = down_w.shape[1:]
    ranks = adapt_n * rank
    heads = 4
    wide = heads * row_n
    tiles = adapt_n * feature_n // (hd * heads)
    chunk = 256 if stretch % 256 == 0 else stretch
    quarter = stretch // nz
    up_shape = (n, ranks * feature_n // (n * hd), hd)
    spec = pl.BlockSpec(memory_space=VMEM)
    anywhere = pl.BlockSpec(memory_space=pl.ANY)
    dma = pltpu.SemaphoreType.DMA
    bf16 = jnp.bfloat16
    f32 = jnp.float32
    block = VMEM((2, stretch, hd), bf16)
    stat = VMEM((3, tiles, 1, wide), f32)
    return pl.pallas_call(
        functools.partial(attend_kernel, n, nz, heads, chunk),
        out_shape=(
            jax.ShapeDtypeStruct((ranks, model // n), f32),
            jax.ShapeDtypeStruct(up_shape, f32),
            jax.ShapeDtypeStruct((2, quarter, hd), f32),
        ),
        in_specs=[pl.BlockSpec(memory_space=pltpu.SMEM)] + [anywhere] * 3 + [spec] * 5,
        out_specs=(spec, spec, spec),
        scratch_shapes=[
            VMEM((adapt_n, row_n, rank), bf16),
            VMEM((tiles, wide, hd), bf16),
            VMEM((4, 2, stretch, hd), bf16),
            VMEM(hidden.shape, bf16),
            VMEM(base.shape, bf16),
            VMEM(grad.shape, bf16),
            VMEM((tiles, wide, 2 * hd), bf16),
            VMEM((4, stretch, hd), bf16),
            VMEM((4, stretch, hd), bf16),
            VMEM((hd, 4 * stretch), bf16),
            VMEM((tiles, 3 * stretch, wide), f32),
            VMEM((tiles, 3 * stretch, wide), f32),
            stat, stat, stat, stat,
            VMEM((tiles, 1, wide), f32),
            VMEM((tiles, 1, wide), jnp.int32),
            VMEM((stretch, hd), f32),
            VMEM((tiles, hd, wide), f32),
            dma((3,)), dma((3, 2)), dma((4, 2)),
            VMEM((ranks, model), bf16),
            VMEM(up_shape, f32),
            block, block, block, block, block, block,
            VMEM((nz - 1, 2, quarter, hd), bf16),
            VMEM((n - 1, ranks, model // n), bf16),
            VMEM((n - 1,) + up_shape[1:], f32),
            VMEM(up_shape[1:], f32),
            dma((2, 2)), dma((2, 2)), dma((2, 2)), dma((2, 2)), dma((nz - 1, 2)), dma((nz - 1, 2)),
            dma((n - 1,)), dma((n - 1,)), dma((n - 1,)), dma((n - 1,)), dma((n - 1,)), dma((n - 1,)),
        ],
        compiler_params=pltpu.CompilerParams(
            collective_id=0, has_side_effects=True, vmem_limit_bytes=60 * 1024 * 1024
        ),
        name="gradients",
    )(lengths, hidden, base, grad, down_w, up_w, offsets[:, None, :], keys, values)


def finish_kernel(down_hbm, up_hbm, prompt_hbm, down_out, up_out, key_out, value_out, down, up, sems):
    adapt_n, rank, _ = down_out.shape
    _, up_rows, hd = up.shape
    pairs = ((up_hbm, up), (down_hbm, down), (prompt_hbm.at[0], key_out), (prompt_hbm.at[1], value_out))
    loads = [pltpu.make_async_copy(a, b, sems.at[i]) for i, (a, b) in enumerate(pairs)]
    for c in loads:
        c.start()
    for c in loads:
        c.wait()
    for a in range(adapt_n):
        down_out[a] = adapter_scale * down[a * rank : (a + 1) * rank, :]
        for h in range(up_out.shape[2] // hd):
            for r in range(0, rank, min(rank, up_rows)):
                at = (h * adapt_n + a) * rank + r
                begin = at % up_rows
                size = min(rank, up_rows)
                up_out[a, r : r + size, h * hd : (h + 1) * hd] = (
                    adapter_scale * up[at // up_rows, begin : begin + size, :]
                )


def finish(up_w, down, up, prompt):
    adapt_n, rank, feature_n = up_w.shape
    f32 = jnp.float32
    spec = pl.BlockSpec(memory_space=VMEM)
    side = jax.ShapeDtypeStruct(prompt.shape[1:], f32)
    return pl.pallas_call(
        finish_kernel,
        out_shape=(
            jax.ShapeDtypeStruct((adapt_n, rank, down.shape[1]), f32),
            jax.ShapeDtypeStruct(up_w.shape, f32),
            side,
            side,
        ),
        in_specs=[pl.BlockSpec(memory_space=pl.ANY)] * 3,
        out_specs=(spec,) * 4,
        scratch_shapes=[VMEM(down.shape, f32), VMEM(up.shape, f32), pltpu.SemaphoreType.DMA((4,))],
        name="finish",
    )(down, up, prompt)


def local(
    hidden,
    response_base_queries,
    attention_output_gradient,
    keys,
    values,
    adapter_down_weight,
    adapter_up_weight,
    lengths,
    offsets,
):
    n = lax.axis_size("seq")
    nz = lax.axis_size("adapter")
    sums = gradients(
        n,
        nz,
        hidden,
        response_base_queries,
        attention_output_gradient,
        adapter_down_weight,
        adapter_up_weight,
        lengths,
        offsets,
        keys,
        values,
    )
    return finish(adapter_up_weight, *sums)


def solution(mesh):
    return jax.shard_map(
        local,
        mesh=mesh,
        in_specs=(
            P("adapter", "seq", None),
            P("adapter", "seq", None),
            P("adapter", "seq", None),
            P("seq", None),
            P("seq", None),
            P("adapter", None, None),
            P("adapter", None, None),
            P("adapter"),
            P("adapter", "seq"),
        ),
        out_specs=(
            P("adapter", None, "seq"),
            P("adapter", None, None),
            P(("seq", "adapter"), None),
            P(("seq", "adapter"), None),
        ),
        check_vma=False,
    )
```

```python
import functools

import jax
import jax.numpy as jnp
from jax import lax
from jax.experimental import pallas as pl
from jax.experimental.pallas import tpu as pltpu
from jax.sharding import PartitionSpec as P

adapter_scale = 2.0
masked_score = -1e30
MESH = pl.DeviceIdType.MESH
VMEM = pltpu.VMEM


def to_seq(index):
    return dict(device_id={"seq": index}, device_id_type=MESH)


def to_adapter(index):
    return dict(device_id={"adapter": index}, device_id_type=MESH)


def remote(src, dst, send_sem, recv_sem, target):
    return pltpu.make_async_remote_copy(
        src_ref=src, dst_ref=dst, send_sem=send_sem, recv_sem=recv_sem, **target
    )


def dot(a, b, dims):
    return lax.dot_general(a, b, (dims, ((), ())), preferred_element_type=jnp.float32)


def attend_kernel(
    n, nz, heads, chunk,
    len_ref, hidden_hbm, base_hbm, grad_hbm, down_w, up_w, offset_ref, keys_ref, values_ref,
    down_out, up_out, prompt_out,
    low_ref, dq_ref, part, hidden, base, grad, gq_all, k_all, v_all, kt, s_ref, dp_ref, peaks, totals, inners,
    weight, delta, place_ref, acc, dq_acc, load_sem, send_sem, recv_sem,
    down, up, pair_a, pair_b, back_two, back_three, summed, total, z_in, down_pair, down_chip, down_in,
    up_pair, up_all, pair_send, pair_recv, back_send, back_recv, z_send, z_recv, d_send, d_recv, u_send, u_recv,
    swap_send, swap_recv,
):
    s = lax.axis_index("seq")
    core = s % 2
    partner = s + 1 - 2 * core
    adapt_n, rows, _ = base.shape
    stretch, hd = keys_ref.shape
    tiles, wide, _ = gq_all.shape
    per = tiles // adapt_n
    factor = hd**-0.5
    pieces = stretch // chunk
    loads = [
        pltpu.make_async_copy(a, b, load_sem.at[i])
        for i, (a, b) in enumerate(((hidden_hbm, hidden), (base_hbm, base), (grad_hbm, grad)))
    ]
    for c in loads:
        c.start()
    full = (k_all, v_all)
    own = (keys_ref, values_ref)

    def copy(i, src, slot, which, target):
        return remote(src, full[i].at[slot], send_sem.at[which, i], recv_sem.at[slot, i], to_seq(target))

    two_on = [copy(i, own[i], 2, 0, s + 2) for i in range(2)]
    three_on = [copy(i, own[i], 3, 1, s + 3) for i in range(2)]
    next_on = [copy(i, own[i], 1, 1, s + 1) for i in range(2)]
    hand_up = [copy(i, full[i].at[2], 3, 2, s + 1) for i in range(2)]
    hand_down = [copy(i, full[i].at[2], 1, 2, s - 1) for i in range(2)]

    def arrived(slot, i):
        @pl.when(s >= slot)
        def _():
            remote(
                full[i].at[slot], full[i].at[slot], send_sem.at[0, i], recv_sem.at[slot, i], to_seq(partner)
            ).wait_recv()

    z = lax.axis_index("adapter")
    has_three_in = (core == 1) & (s + 3 < n)

    @pl.when(s + 2 >= n)
    def _():
        back_two[...] = jnp.zeros_like(back_two)

    @pl.when(jnp.logical_not(has_three_in))
    def _():
        back_three[...] = jnp.zeros_like(back_three)

    @pl.when(core == 1)
    def _():
        pair_b[...] = jnp.zeros_like(pair_b)

    barrier = pltpu.get_barrier_semaphore()
    for i in range(1, n):
        pl.semaphore_signal(barrier, inc=1, **to_seq((s + i) % n))
    for i in range(1, nz):
        pl.semaphore_signal(barrier, inc=1, **to_adapter((z + i) % nz))
    pl.semaphore_wait(barrier, n - 1 + nz - 1)

    has_two_on = s + 2 < n
    has_three_on = (core == 1) & (s + 3 < n)
    for i in range(2):

        @pl.when(has_two_on)
        def _():
            two_on[i].start()

        @pl.when(has_three_on)
        def _():
            three_on[i].start()

        @pl.when(core == 0)
        def _():
            next_on[i].start()

    k_all[0] = keys_ref[...]
    v_all[0] = values_ref[...]
    for slot in (1, 2, 3):

        @pl.when(s < slot)
        def _():
            k_all[slot] = jnp.zeros(k_all.shape[1:], k_all.dtype)
            v_all[slot] = jnp.zeros(v_all.shape[1:], v_all.dtype)

    for c in loads:
        c.wait()
    for a in range(adapt_n):
        low = dot(hidden[a], down_w[a], ((1,), (1,))).astype(jnp.bfloat16)
        low_ref[a] = low
        place = jnp.concatenate([offset_ref[a]] * heads, axis=1) - s * stretch
        for t in range(per):
            place_ref[a * per + t] = place
        raised = dot(low, up_w[a], ((1,), (0,)))
        query = (base[a].astype(jnp.float32) + adapter_scale * raised).astype(jnp.bfloat16)
        live = s * rows + lax.broadcasted_iota(jnp.int32, (rows, 1), 0) < len_ref[a]
        g = jnp.where(live, grad[a], jnp.zeros_like(grad[a]))
        for h in range(per * heads):
            t, at_row = a * per + h // heads, (h % heads) * rows
            gq_all[t, at_row : at_row + rows, :hd] = g[:, h * hd : (h + 1) * hd]
            gq_all[t, at_row : at_row + rows, hd:] = query[:, h * hd : (h + 1) * hd]

    def hand(i):
        @pl.when(s >= 2)
        def _():
            @pl.when(core == 0)
            def _():
                hand_up[i].start()

            @pl.when(core == 1)
            def _():
                hand_down[i].start()

    def at(piece):
        return slice(piece * chunk, (piece + 1) * chunk)

    def before(piece, place):
        pos = piece * chunk + lax.broadcasted_iota(jnp.int32, (chunk, wide), 0)
        return pos <= place

    spots = {0: 0, 3: 1, 1: 2, 2: 3}

    def turned(d):
        kt[:, spots[d] * stretch : (spots[d] + 1) * stretch] = k_all[d].T

    def product(source, d, piece, other):
        return dot(source[d, at(piece), :], other, ((1,), (1,)))

    far_bias = jnp.where(s >= 3, 0.0, masked_score)

    @pl.loop(0, tiles)
    def _(t):
        q = gq_all[t, :, hd:]
        g = gq_all[t, :, :hd]
        for piece in range(pieces):
            s_ref[t, at(piece), :] = product(k_all, 0, piece, q) * factor
            dp_ref[t, at(piece), :] = product(v_all, 0, piece, g)

    def scores_of(d):
        @pl.loop(0, tiles)
        def _(t):
            q = gq_all[t, :, hd:]
            peak = jnp.full((1, wide), masked_score, jnp.float32)
            for piece in range(pieces):
                score = product(k_all, d or 3, piece, q) * factor
                if d == 0:
                    near = before(piece, place_ref[t])
                    score = jnp.where(near, s_ref[t, at(piece), :], score + far_bias)
                s_ref[t, at(d * pieces + piece), :] = score
                peak = jnp.maximum(peak, jnp.max(score, axis=0, keepdims=True))
            peaks[d, t] = peak

    def raise_of(d):
        @pl.loop(0, tiles)
        def _(t):
            g = gq_all[t, :, :hd]
            peak = peaks[d, t]
            total = jnp.zeros((1, wide), jnp.float32)
            inner = jnp.zeros((1, wide), jnp.float32)
            for piece in range(pieces):
                spot = at(d * pieces + piece)
                e = jnp.exp(s_ref[t, spot, :] - peak)
                dp = product(v_all, d or 3, piece, g)
                if d == 0:
                    dp = jnp.where(before(piece, place_ref[t]), dp_ref[t, spot, :], dp)
                s_ref[t, spot, :] = e
                dp_ref[t, spot, :] = dp
                total = total + jnp.sum(e, axis=0, keepdims=True)
                inner = inner + jnp.sum(e * dp, axis=0, keepdims=True)
            totals[d, t] = total
            inners[d, t] = inner

    arrived(2, 0)
    hand(0)
    turned(2)
    scores_of(2)
    arrived(1, 0)
    turned(1)
    scores_of(1)
    arrived(2, 1)
    hand(1)
    raise_of(2)
    arrived(1, 1)
    raise_of(1)
    arrived(3, 0)
    turned(3)
    turned(0)
    scores_of(0)
    arrived(3, 1)
    raise_of(0)

    @pl.loop(0, tiles)
    def _(t):
        tops = [peaks[0, t]] + [jnp.where(s >= d, peaks[d, t], masked_score) for d in (1, 2)]
        peak = jnp.maximum(jnp.maximum(tops[0], tops[1]), tops[2])
        shares = [jnp.exp(top - peak) for top in tops]
        total = jnp.zeros((1, wide), jnp.float32)
        inner = jnp.zeros((1, wide), jnp.float32)
        for d, share in enumerate(shares):
            total = total + totals[d, t] * share
            inner = inner + inners[d, t] * share
        inverse = 1.0 / total
        for d, share in enumerate(shares):
            weight[d, t] = share * inverse
        delta[t] = inner * inverse

    def rows_of(unit, piece):
        if isinstance(unit, int):
            return at(unit * pieces + piece)
        return pl.ds(pl.multiple_of(unit * stretch + piece * chunk, chunk), chunk)

    def gather_up(block, i, first=0, last=tiles):
        static = isinstance(block, int)
        unit = 0 if static else block
        if first == 0:
            acc[...] = jnp.zeros_like(acc)

        @pl.loop(first, last)
        def _(t):
            other = gq_all[t]
            share = weight[unit, t]
            lows = []
            for piece in range(pieces):
                spot = rows_of(unit, piece)
                value = s_ref[t, spot, :] * share
                if i == 0:
                    value = value * (dp_ref[t, spot, :] - delta[t])
                if static:
                    near = before(piece, place_ref[t])
                    value = jnp.where(near, 0.0, value) if block else jnp.where(near, value, 0.0)
                low = value.astype(jnp.bfloat16)
                both = dot(low, other, ((1,), (0,)))
                acc[at(piece), :] += both[:, :hd] if i else both[:, hd:]
                lows.append(low)
            if i == 0:
                if static:
                    turned_block = kt[:, spots[block] * stretch : (spots[block] + 1) * stretch]
                else:
                    turned_block = kt[:, pl.ds(pl.multiple_of((block + 1) * stretch, stretch), stretch)]
                dq = dot(turned_block, jnp.concatenate(lows, axis=0), ((1,), (0,)))
                if static and block == 3:
                    dq_acc[t] = dq
                else:
                    dq_acc[t] += dq

        if last == tiles:
            out = acc[...]
            part[block, i] = (out if i else out * factor).astype(jnp.bfloat16)

    quarter = prompt_out.shape[1]
    has_far = (core == 0) & (s >= 3)

    def pair_copy(d, to, i, j):
        return remote(part.at[d, i], to.at[i], pair_send.at[j, i], pair_recv.at[j, i], to_seq(partner))

    zero_to_one = [pair_copy(1, pair_a, i, 0) for i in range(2)]
    one_to_zero = [pair_copy(3, pair_a, i, 0) for i in range(2)]
    near_back = [pair_copy(1, pair_b, i, 1) for i in range(2)]
    far_back = [
        remote(part.at[3, i], back_three.at[i], back_send.at[1, i], back_recv.at[1, i], to_seq(s - 3))
        for i in range(2)
    ]
    two_back = [
        remote(summed.at[i], back_two.at[i], back_send.at[0, i], back_recv.at[0, i], to_seq(s - 2))
        for i in range(2)
    ]
    chips = n // 2
    chip = s // 2
    down_swap = remote(down.at[1 - core], down_pair, swap_send.at[0], swap_recv.at[0], to_seq(partner))
    up_swap = remote(up.at[1 - core], up_pair, swap_send.at[1], swap_recv.at[1], to_seq(partner))
    up_back = remote(up_out.at[core], up_out.at[core], swap_send.at[2], swap_recv.at[2], to_seq(partner))
    downs, ups = [], []
    for i in range(1, chips):
        peer = (chip + i) % chips
        target = to_seq(2 * peer + core)
        downs.append(remote(down_chip.at[peer], down_in.at[i - 1], d_send.at[i - 1], d_recv.at[i - 1], target))
        ups.append(remote(up_all.at[chip], up_all.at[chip], u_send.at[i - 1], u_recv.at[i - 1], target))

    def sum_pair(i):
        zero_to_one[i].wait_recv()
        summed[i] = (part[2, i].astype(jnp.float32) + pair_a[i].astype(jnp.float32)).astype(jnp.bfloat16)

        @pl.when(s >= 2)
        def _():
            two_back[i].start()

    spread = [[], []]

    def owner(i):
        @pl.when(core == 0)
        def _():
            near_back[i].wait_recv()

        @pl.when(s + 2 < n)
        def _():
            two_back[i].wait_recv()

        @pl.when(has_three_in)
        def _():
            far_back[i].wait_recv()

        total[i] = (
            part[0, i].astype(jnp.float32)
            + pair_b[i].astype(jnp.float32)
            + back_two[i].astype(jnp.float32)
            + back_three[i].astype(jnp.float32)
        ).astype(jnp.bfloat16)
        for j in range(1, nz):
            peer = (z + j) % nz
            c = remote(
                total.at[i, pl.ds(pl.multiple_of(peer * quarter, 16), quarter), :],
                z_in.at[j - 1, i], z_send.at[j - 1, i], z_recv.at[j - 1, i], to_adapter(peer),
            )
            c.start()
            spread[i].append(c)

    def prompt_sum(i):
        mine = total[i, pl.ds(pl.multiple_of(z * quarter, 16), quarter), :].astype(jnp.float32)
        for j, c in enumerate(spread[i]):
            c.wait_recv()
            mine = mine + z_in[j, i].astype(jnp.float32)
        prompt_out[i] = mine

    def far_out(i):
        @pl.when(core == 1)
        def _():
            one_to_zero[i].start()

        @pl.when(has_far)
        def _():
            far_back[i].start()

    def sum_on(which, i):
        @pl.when(core == which)
        def _():
            sum_pair(i)

    second = 1 + core
    third = 2 - core
    middle = tiles // 2

    def second_out(i):
        gather_up(second, i)

        @pl.when(core == 0)
        def _():
            zero_to_one[i].start()

    def third_out(i):
        gather_up(third, i, 0, middle)
        sum_on(1, i)
        gather_up(third, i, middle, tiles)
        sum_on(0, i)

        @pl.when(core == 1)
        def _():
            near_back[i].start()

    gather_up(3, 1)
    far_out(1)
    second_out(1)
    third_out(1)
    gather_up(3, 0)
    far_out(0)
    gather_up(0, 1)
    second_out(0)
    owner(1)
    third_out(0)
    gather_up(0, 0)

    @pl.loop(0, tiles)
    def _(t):
        dq_ref[t] = (dq_acc[t] * factor).T.astype(jnp.bfloat16)

    _, rank, feature_n = up_w.shape
    group = feature_n // hd
    half = feature_n // 2
    width = down_out.shape[1]
    smalls = []
    for a in range(adapt_n):
        small = jnp.zeros((rows, rank), jnp.float32)
        for h in range(group):
            place = a * group + h
            dq_h = dq_ref[place // heads, (place % heads) * rows : (place % heads + 1) * rows, :]
            up_h = dot(low_ref[a], dq_h, ((0,), (0,)))
            begin = h * hd % half
            up[h * hd // half, a * rank : (a + 1) * rank, begin : begin + hd] = up_h.astype(jnp.bfloat16)
            small = small + dot(dq_h, up_w[a, :, h * hd : (h + 1) * hd], ((1,), (1,)))
        smalls.append(small.astype(jnp.bfloat16))
    up_swap.start()
    for a in range(adapt_n):
        out = dot(smalls[a], hidden[a], ((0,), (0,))).astype(jnp.bfloat16)
        for j in range(n):
            down[j % 2, j // 2, a * rank : (a + 1) * rank, :] = out[:, j * width : (j + 1) * width]
    down_swap.start()
    up_swap.wait_recv()
    up_all[chip] = (up[core].astype(jnp.float32) + up_pair[...].astype(jnp.float32)).astype(jnp.bfloat16)
    for c in ups:
        c.start()
    down_swap.wait_recv()
    for j in range(chips):
        both = down[core, j].astype(jnp.float32) + down_pair[j].astype(jnp.float32)
        down_chip[j] = both.astype(jnp.bfloat16)
    for c in downs:
        c.start()
    owner(0)
    for c in ups:
        c.wait_recv()
    mine = up_all[0].astype(jnp.float32)
    for j in range(1, chips):
        mine = mine + up_all[j].astype(jnp.float32)
    up_out[core] = mine
    up_back.start()
    mine = down[core, chip].astype(jnp.float32) + down_pair[chip].astype(jnp.float32)
    for i, c in enumerate(downs):
        c.wait_recv()
        mine = mine + down_in[i].astype(jnp.float32)
    down_out[...] = mine
    prompt_sum(1)
    prompt_sum(0)
    up_back.wait_recv()
    for c in downs + ups + spread[0] + spread[1] + zero_to_one + [up_swap, down_swap, up_back]:
        c.wait_send()
    for i in range(2):

        @pl.when(core == 1)
        def _():
            near_back[i].wait_send()

        @pl.when(has_far)
        def _():
            far_back[i].wait_send()

        @pl.when(s >= 2)
        def _():
            two_back[i].wait_send()

    for i in range(2):

        @pl.when(has_two_on)
        def _():
            two_on[i].wait_send()

        @pl.when(has_three_on)
        def _():
            three_on[i].wait_send()

        @pl.when(core == 0)
        def _():
            next_on[i].wait_send()

        @pl.when(s >= 2)
        def _():
            hand_up[i].wait_send()


def gradients(n, nz, hidden, base, grad, down_w, up_w, lengths, offsets, keys, values):
    adapt_n, row_n, feature_n = base.shape
    stretch, hd = keys.shape
    rank, model = down_w.shape[1:]
    ranks = adapt_n * rank
    heads = 4
    wide = heads * row_n
    tiles = adapt_n * feature_n // (hd * heads)
    chunk = 256 if stretch % 256 == 0 else stretch
    quarter = stretch // nz
    up_shape = (2, ranks, feature_n // 2)
    down_shape = (n // 2, ranks, model // n)
    spec = pl.BlockSpec(memory_space=VMEM)
    anywhere = pl.BlockSpec(memory_space=pl.ANY)
    dma = pltpu.SemaphoreType.DMA
    bf16 = jnp.bfloat16
    f32 = jnp.float32
    block = VMEM((2, stretch, hd), bf16)
    stat = VMEM((3, tiles, 1, wide), f32)
    return pl.pallas_call(
        functools.partial(attend_kernel, n, nz, heads, chunk),
        out_shape=(
            jax.ShapeDtypeStruct((ranks, model // n), f32),
            jax.ShapeDtypeStruct(up_shape, f32),
            jax.ShapeDtypeStruct((2, quarter, hd), f32),
        ),
        in_specs=[pl.BlockSpec(memory_space=pltpu.SMEM)] + [anywhere] * 3 + [spec] * 5,
        out_specs=(spec, spec, spec),
        scratch_shapes=[
            VMEM((adapt_n, row_n, rank), bf16),
            VMEM((tiles, wide, hd), bf16),
            VMEM((4, 2, stretch, hd), bf16),
            VMEM(hidden.shape, bf16),
            VMEM(base.shape, bf16),
            VMEM(grad.shape, bf16),
            VMEM((tiles, wide, 2 * hd), bf16),
            VMEM((4, stretch, hd), bf16),
            VMEM((4, stretch, hd), bf16),
            VMEM((hd, 4 * stretch), bf16),
            VMEM((tiles, 3 * stretch, wide), f32),
            VMEM((tiles, 3 * stretch, wide), f32),
            stat, stat, stat, stat,
            VMEM((tiles, 1, wide), f32),
            VMEM((tiles, 1, wide), jnp.int32),
            VMEM((stretch, hd), f32),
            VMEM((tiles, hd, wide), f32),
            dma((3,)), dma((3, 2)), dma((4, 2)),
            VMEM((2,) + down_shape, bf16),
            VMEM(up_shape, bf16),
            block, block, block, block, block, block,
            VMEM((nz - 1, 2, quarter, hd), bf16),
            VMEM(down_shape, bf16),
            VMEM(down_shape, bf16),
            VMEM((n // 2 - 1,) + down_shape[1:], bf16),
            VMEM(up_shape[1:], bf16),
            VMEM((n // 2,) + up_shape[1:], bf16),
            dma((2, 2)), dma((2, 2)), dma((2, 2)), dma((2, 2)), dma((nz - 1, 2)), dma((nz - 1, 2)),
            dma((n // 2 - 1,)), dma((n // 2 - 1,)), dma((n // 2 - 1,)), dma((n // 2 - 1,)), dma((3,)), dma((3,)),
        ],
        compiler_params=pltpu.CompilerParams(
            collective_id=0, has_side_effects=True, vmem_limit_bytes=60 * 1024 * 1024
        ),
        name="gradients",
    )(lengths, hidden, base, grad, down_w, up_w, offsets[:, None, :], keys, values)


def finish_kernel(down_hbm, up_hbm, prompt_hbm, down_out, up_out, key_out, value_out, down, up, sems):
    adapt_n, rank, _ = down_out.shape
    half = up.shape[2]
    pairs = ((up_hbm, up), (down_hbm, down), (prompt_hbm.at[0], key_out), (prompt_hbm.at[1], value_out))
    loads = [pltpu.make_async_copy(a, b, sems.at[i]) for i, (a, b) in enumerate(pairs)]
    for c in loads:
        c.start()
    for c in loads:
        c.wait()
    for a in range(adapt_n):
        down_out[a] = adapter_scale * down[a * rank : (a + 1) * rank, :]
        for j in range(2):
            up_out[a, :, j * half : (j + 1) * half] = adapter_scale * up[j, a * rank : (a + 1) * rank, :]


def finish(up_w, down, up, prompt):
    adapt_n, rank, feature_n = up_w.shape
    f32 = jnp.float32
    spec = pl.BlockSpec(memory_space=VMEM)
    side = jax.ShapeDtypeStruct(prompt.shape[1:], f32)
    return pl.pallas_call(
        finish_kernel,
        out_shape=(
            jax.ShapeDtypeStruct((adapt_n, rank, down.shape[1]), f32),
            jax.ShapeDtypeStruct(up_w.shape, f32),
            side,
            side,
        ),
        in_specs=[pl.BlockSpec(memory_space=pl.ANY)] * 3,
        out_specs=(spec,) * 4,
        scratch_shapes=[VMEM(down.shape, f32), VMEM(up.shape, f32), pltpu.SemaphoreType.DMA((4,))],
        name="finish",
    )(down, up, prompt)


def local(
    hidden,
    response_base_queries,
    attention_output_gradient,
    keys,
    values,
    adapter_down_weight,
    adapter_up_weight,
    lengths,
    offsets,
):
    n = lax.axis_size("seq")
    nz = lax.axis_size("adapter")
    sums = gradients(
        n,
        nz,
        hidden,
        response_base_queries,
        attention_output_gradient,
        adapter_down_weight,
        adapter_up_weight,
        lengths,
        offsets,
        keys,
        values,
    )
    return finish(adapter_up_weight, *sums)


def solution(mesh):
    return jax.shard_map(
        local,
        mesh=mesh,
        in_specs=(
            P("adapter", "seq", None),
            P("adapter", "seq", None),
            P("adapter", "seq", None),
            P("seq", None),
            P("seq", None),
            P("adapter", None, None),
            P("adapter", None, None),
            P("adapter"),
            P("adapter", "seq"),
        ),
        out_specs=(
            P("adapter", None, "seq"),
            P("adapter", None, None),
            P(("seq", "adapter"), None),
            P(("seq", "adapter"), None),
        ),
        check_vma=False,
    )
```

```python
import functools

import jax
import jax.numpy as jnp
from jax import lax
from jax.experimental import pallas as pl
from jax.experimental.pallas import tpu as pltpu
from jax.sharding import PartitionSpec as P

adapter_scale = 2.0
masked_score = -1e30
MESH = pl.DeviceIdType.MESH
VMEM = pltpu.VMEM


def to_seq(index):
    return dict(device_id={"seq": index}, device_id_type=MESH)


def to_adapter(index):
    return dict(device_id={"adapter": index}, device_id_type=MESH)


def remote(src, dst, send_sem, recv_sem, target):
    return pltpu.make_async_remote_copy(
        src_ref=src, dst_ref=dst, send_sem=send_sem, recv_sem=recv_sem, **target
    )


def dot(a, b, dims):
    return lax.dot_general(a, b, (dims, ((), ())), preferred_element_type=jnp.float32)


def attend_kernel(
    n, nz, heads, chunk,
    len_hbm, hidden_hbm, base_hbm, grad_hbm, down_hbm, up_hbm, offset_hbm, keys_hbm, values_hbm,
    down_result, up_result, prompt_result,
    len_ref, down_w, up_w, offset_ref, down_out, up_out, prompt_out, low_ref, dq_ref, part, hidden, base, grad, gq_all, g_turned, q_turned, k_all, v_all, kt, s_ref, dp_ref, peaks, totals, inners,
    weight, delta, place_ref, acc, dq_acc, load_sem, out_sem, send_sem, recv_sem,
    down, up, pair_a, pair_b, back_two, back_three, summed, total, z_in, down_pair, down_chip, down_in,
    up_pair, up_all, pair_send, pair_recv, back_send, back_recv, z_send, z_recv, d_send, d_recv, u_send, u_recv,
    swap_send, swap_recv,
):
    s = lax.axis_index("seq")
    z = lax.axis_index("adapter")
    barrier = pltpu.get_barrier_semaphore()
    for i in range(1, n):
        pl.semaphore_signal(barrier, inc=1, **to_seq((s + i) % n))
    for i in range(1, nz):
        pl.semaphore_signal(barrier, inc=1, **to_adapter((z + i) % nz))
    core = s % 2
    partner = s + 1 - 2 * core
    adapt_n, rows, _ = base.shape
    _, stretch, hd = k_all.shape
    tiles, wide, _ = gq_all.shape
    per = tiles // adapt_n
    factor = hd**-0.5
    pieces = stretch // chunk
    pairs = (
        (down_hbm, down_w), (hidden_hbm, hidden), (len_hbm, len_ref), (offset_hbm, offset_ref), (up_hbm, up_w),
        (base_hbm, base), (grad_hbm, grad), (keys_hbm, k_all.at[0]), (values_hbm, v_all.at[0]),
    )
    loads = [pltpu.make_async_copy(a, b, load_sem.at[i]) for i, (a, b) in enumerate(pairs)]
    for c in loads:
        c.start()
    full = (k_all, v_all)
    own = (keys_hbm, values_hbm)

    def copy(i, src, slot, which, target):
        return remote(src, full[i].at[slot], send_sem.at[which, i], recv_sem.at[slot, i], to_seq(target))

    two_on = [copy(i, own[i], 2, 0, s + 2) for i in range(2)]
    three_on = [copy(i, own[i], 3, 1, s + 3) for i in range(2)]
    next_on = [copy(i, own[i], 1, 1, s + 1) for i in range(2)]
    hand_up = [copy(i, full[i].at[2], 3, 2, s + 1) for i in range(2)]
    hand_down = [copy(i, full[i].at[2], 1, 2, s - 1) for i in range(2)]

    def arrived(slot, i):
        @pl.when(s >= slot)
        def _():
            remote(
                full[i].at[slot], full[i].at[slot], send_sem.at[0, i], recv_sem.at[slot, i], to_seq(partner)
            ).wait_recv()

    has_three_in = (core == 1) & (s + 3 < n)
    pl.semaphore_wait(barrier, n - 1 + nz - 1)

    has_two_on = s + 2 < n
    has_three_on = (core == 1) & (s + 3 < n)
    for i in range(2):

        @pl.when(has_two_on)
        def _():
            two_on[i].start()

        @pl.when(has_three_on)
        def _():
            three_on[i].start()

        @pl.when(core == 0)
        def _():
            next_on[i].start()

    @pl.when(s + 2 >= n)
    def _():
        back_two[...] = jnp.zeros_like(back_two)

    @pl.when(jnp.logical_not(has_three_in))
    def _():
        back_three[...] = jnp.zeros_like(back_three)

    @pl.when(core == 1)
    def _():
        pair_b[...] = jnp.zeros_like(pair_b)

    for slot in (1, 2, 3):

        @pl.when(s < slot)
        def _():
            k_all[slot] = jnp.zeros(k_all.shape[1:], k_all.dtype)
            v_all[slot] = jnp.zeros(v_all.shape[1:], v_all.dtype)

    for c in loads:
        c.wait()
    for a in range(adapt_n):
        low = dot(hidden[a], down_w[a], ((1,), (1,))).astype(jnp.bfloat16)
        low_ref[a] = low
        place = jnp.concatenate([offset_ref[a]] * heads, axis=1) - s * stretch
        for t in range(per):
            place_ref[a * per + t] = place
        raised = dot(low, up_w[a], ((1,), (0,)))
        query = (base[a].astype(jnp.float32) + adapter_scale * raised).astype(jnp.bfloat16)
        live = s * rows + lax.broadcasted_iota(jnp.int32, (rows, 1), 0) < len_ref[a]
        g = jnp.where(live, grad[a], jnp.zeros_like(grad[a]))
        for h in range(per * heads):
            t, at_row = a * per + h // heads, (h % heads) * rows
            gq_all[t, at_row : at_row + rows, :hd] = g[:, h * hd : (h + 1) * hd]
            gq_all[t, at_row : at_row + rows, hd:] = query[:, h * hd : (h + 1) * hd]
            g_turned[t, :, at_row : at_row + rows] = g[:, h * hd : (h + 1) * hd].T
            q_turned[t, :, at_row : at_row + rows] = query[:, h * hd : (h + 1) * hd].T

    def hand(i):
        @pl.when(s >= 2)
        def _():
            @pl.when(core == 0)
            def _():
                hand_up[i].start()

            @pl.when(core == 1)
            def _():
                hand_down[i].start()

    def at(piece):
        return slice(piece * chunk, (piece + 1) * chunk)

    def before(piece, place):
        pos = piece * chunk + lax.broadcasted_iota(jnp.int32, (chunk, wide), 0)
        return pos <= place

    spots = {0: 0, 3: 1, 1: 2, 2: 3}

    def turned(d):
        kt[:, spots[d] * stretch : (spots[d] + 1) * stretch] = k_all[d].T

    def product(source, d, piece, other):
        return dot(source[d, at(piece), :], other, ((1,), (0,)))

    far_bias = jnp.where(s >= 3, 0.0, masked_score)

    @pl.loop(0, tiles)
    def _(t):
        q = q_turned[t]
        g = g_turned[t]
        for piece in range(pieces):
            s_ref[t, at(piece), :] = product(k_all, 0, piece, q) * factor
            dp_ref[t, at(piece), :] = product(v_all, 0, piece, g)

    def scores_of(d):
        @pl.loop(0, tiles)
        def _(t):
            q = q_turned[t]
            peak = jnp.full((1, wide), masked_score, jnp.float32)
            for piece in range(pieces):
                score = product(k_all, d or 3, piece, q) * factor
                if d == 0:
                    near = before(piece, place_ref[t])
                    score = jnp.where(near, s_ref[t, at(piece), :], score + far_bias)
                s_ref[t, at(d * pieces + piece), :] = score
                peak = jnp.maximum(peak, jnp.max(score, axis=0, keepdims=True))
            peaks[d, t] = peak

    def raise_of(d):
        @pl.loop(0, tiles)
        def _(t):
            g = g_turned[t]
            peak = peaks[d, t]
            total = jnp.zeros((1, wide), jnp.float32)
            inner = jnp.zeros((1, wide), jnp.float32)
            for piece in range(pieces):
                spot = at(d * pieces + piece)
                e = jnp.exp(s_ref[t, spot, :] - peak)
                dp = product(v_all, d or 3, piece, g)
                if d == 0:
                    dp = jnp.where(before(piece, place_ref[t]), dp_ref[t, spot, :], dp)
                s_ref[t, spot, :] = e
                dp_ref[t, spot, :] = dp
                total = total + jnp.sum(e, axis=0, keepdims=True)
                inner = inner + jnp.sum(e * dp, axis=0, keepdims=True)
            totals[d, t] = total
            inners[d, t] = inner

    arrived(2, 0)
    hand(0)
    turned(2)
    scores_of(2)
    arrived(1, 0)
    turned(1)
    scores_of(1)
    arrived(2, 1)
    hand(1)
    raise_of(2)
    arrived(1, 1)
    raise_of(1)
    arrived(3, 0)
    turned(3)
    turned(0)
    scores_of(0)
    arrived(3, 1)
    raise_of(0)

    @pl.loop(0, tiles)
    def _(t):
        tops = [peaks[0, t]] + [jnp.where(s >= d, peaks[d, t], masked_score) for d in (1, 2)]
        peak = jnp.maximum(jnp.maximum(tops[0], tops[1]), tops[2])
        shares = [jnp.exp(top - peak) for top in tops]
        total = jnp.zeros((1, wide), jnp.float32)
        inner = jnp.zeros((1, wide), jnp.float32)
        for d, share in enumerate(shares):
            total = total + totals[d, t] * share
            inner = inner + inners[d, t] * share
        inverse = 1.0 / total
        for d, share in enumerate(shares):
            weight[d, t] = share * inverse
        delta[t] = inner * inverse

    def rows_of(unit, piece):
        if isinstance(unit, int):
            return at(unit * pieces + piece)
        return pl.ds(pl.multiple_of(unit * stretch + piece * chunk, chunk), chunk)

    def gather_up(block, i, first=0, last=tiles):
        static = isinstance(block, int)
        unit = 0 if static else block
        if first == 0:
            acc[...] = jnp.zeros_like(acc)

        @pl.loop(first, last)
        def _(t):
            other = gq_all[t]
            share = weight[unit, t]
            lows = []
            for piece in range(pieces):
                spot = rows_of(unit, piece)
                value = s_ref[t, spot, :] * share
                if i == 0:
                    value = value * (dp_ref[t, spot, :] - delta[t])
                if static:
                    near = before(piece, place_ref[t])
                    value = jnp.where(near, 0.0, value) if block else jnp.where(near, value, 0.0)
                low = value.astype(jnp.bfloat16)
                both = dot(low, other, ((1,), (0,)))
                acc[at(piece), :] += both[:, :hd] if i else both[:, hd:]
                lows.append(low)
            if i == 0:
                if static:
                    turned_block = kt[:, spots[block] * stretch : (spots[block] + 1) * stretch]
                else:
                    turned_block = kt[:, pl.ds(pl.multiple_of((block + 1) * stretch, stretch), stretch)]
                dq = dot(turned_block, jnp.concatenate(lows, axis=0), ((1,), (0,)))
                if static and block == 3:
                    dq_acc[t] = dq
                else:
                    dq_acc[t] += dq

        if last == tiles:
            out = acc[...]
            part[block, i] = (out if i else out * factor).astype(jnp.bfloat16)

    quarter = prompt_out.shape[1]
    has_far = (core == 0) & (s >= 3)

    def pair_copy(d, to, i, j):
        return remote(part.at[d, i], to.at[i], pair_send.at[j, i], pair_recv.at[j, i], to_seq(partner))

    zero_to_one = [pair_copy(1, pair_a, i, 0) for i in range(2)]
    one_to_zero = [pair_copy(3, pair_a, i, 0) for i in range(2)]
    near_back = [pair_copy(1, pair_b, i, 1) for i in range(2)]
    far_back = [
        remote(part.at[3, i], back_three.at[i], back_send.at[1, i], back_recv.at[1, i], to_seq(s - 3))
        for i in range(2)
    ]
    two_back = [
        remote(summed.at[i], back_two.at[i], back_send.at[0, i], back_recv.at[0, i], to_seq(s - 2))
        for i in range(2)
    ]
    chips = n // 2
    chip = s // 2
    down_swap = remote(down.at[1 - core], down_pair, swap_send.at[0], swap_recv.at[0], to_seq(partner))
    up_swap = remote(up.at[1 - core], up_pair, swap_send.at[1], swap_recv.at[1], to_seq(partner))
    up_back = remote(up_out.at[core], up_out.at[core], swap_send.at[2], swap_recv.at[2], to_seq(partner))
    downs, ups = [], []
    for i in range(1, chips):
        peer = (chip + i) % chips
        target = to_seq(2 * peer + core)
        downs.append(remote(down_chip.at[peer], down_in.at[i - 1], d_send.at[i - 1], d_recv.at[i - 1], target))
        ups.append(remote(up_all.at[chip], up_all.at[chip], u_send.at[i - 1], u_recv.at[i - 1], target))

    def sum_pair(i):
        zero_to_one[i].wait_recv()
        summed[i] = (part[2, i].astype(jnp.float32) + pair_a[i].astype(jnp.float32)).astype(jnp.bfloat16)

        @pl.when(s >= 2)
        def _():
            two_back[i].start()

    spread = [[], []]

    def owner(i):
        @pl.when(core == 0)
        def _():
            near_back[i].wait_recv()

        @pl.when(s + 2 < n)
        def _():
            two_back[i].wait_recv()

        @pl.when(has_three_in)
        def _():
            far_back[i].wait_recv()

        total[i] = (
            part[0, i].astype(jnp.float32)
            + pair_b[i].astype(jnp.float32)
            + back_two[i].astype(jnp.float32)
            + back_three[i].astype(jnp.float32)
        ).astype(jnp.bfloat16)
        for j in range(1, nz):
            peer = (z + j) % nz
            c = remote(
                total.at[i, pl.ds(pl.multiple_of(peer * quarter, 16), quarter), :],
                z_in.at[j - 1, i], z_send.at[j - 1, i], z_recv.at[j - 1, i], to_adapter(peer),
            )
            c.start()
            spread[i].append(c)

    def prompt_sum(i):
        mine = total[i, pl.ds(pl.multiple_of(z * quarter, 16), quarter), :].astype(jnp.float32)
        for j, c in enumerate(spread[i]):
            c.wait_recv()
            mine = mine + z_in[j, i].astype(jnp.float32)
        prompt_out[i] = mine

    def far_out(i):
        @pl.when(core == 1)
        def _():
            one_to_zero[i].start()

        @pl.when(has_far)
        def _():
            far_back[i].start()

    def sum_on(which, i):
        @pl.when(core == which)
        def _():
            sum_pair(i)

    second = 1 + core
    third = 2 - core
    middle = tiles // 2

    def second_out(i):
        gather_up(second, i)

        @pl.when(core == 0)
        def _():
            zero_to_one[i].start()

    def third_out(i):
        gather_up(third, i, 0, middle)
        sum_on(1, i)
        gather_up(third, i, middle, tiles)
        sum_on(0, i)

        @pl.when(core == 1)
        def _():
            near_back[i].start()

    gather_up(3, 1)
    far_out(1)
    second_out(1)
    third_out(1)
    gather_up(3, 0)
    far_out(0)
    gather_up(0, 1)
    second_out(0)
    owner(1)
    third_out(0)
    gather_up(0, 0)

    @pl.loop(0, tiles)
    def _(t):
        dq_ref[t] = (dq_acc[t] * factor).T.astype(jnp.bfloat16)

    _, rank, feature_n = up_w.shape
    group = feature_n // hd
    half = feature_n // 2
    width = down_out.shape[1]
    smalls = []
    for a in range(adapt_n):
        small = jnp.zeros((rows, rank), jnp.float32)
        for h in range(group):
            place = a * group + h
            dq_h = dq_ref[place // heads, (place % heads) * rows : (place % heads + 1) * rows, :]
            up_h = dot(low_ref[a], dq_h, ((0,), (0,)))
            begin = h * hd % half
            up[h * hd // half, a * rank : (a + 1) * rank, begin : begin + hd] = up_h.astype(jnp.bfloat16)
            small = small + dot(dq_h, up_w[a, :, h * hd : (h + 1) * hd], ((1,), (1,)))
        smalls.append(small.astype(jnp.bfloat16))
    up_swap.start()
    for a in range(adapt_n):
        out = dot(smalls[a], hidden[a], ((0,), (0,))).astype(jnp.bfloat16)
        for j in range(n):
            down[j % 2, j // 2, a * rank : (a + 1) * rank, :] = out[:, j * width : (j + 1) * width]
    down_swap.start()
    up_swap.wait_recv()
    up_all[chip] = (up[core].astype(jnp.float32) + up_pair[...].astype(jnp.float32)).astype(jnp.bfloat16)
    for c in ups:
        c.start()
    down_swap.wait_recv()
    for j in range(chips):
        both = down[core, j].astype(jnp.float32) + down_pair[j].astype(jnp.float32)
        down_chip[j] = both.astype(jnp.bfloat16)
    for c in downs:
        c.start()
    owner(0)
    for c in ups:
        c.wait_recv()
    mine = up_all[0].astype(jnp.float32)
    for j in range(1, chips):
        mine = mine + up_all[j].astype(jnp.float32)
    up_out[core] = mine
    up_back.start()
    mine = down[core, chip].astype(jnp.float32) + down_pair[chip].astype(jnp.float32)
    for i, c in enumerate(downs):
        c.wait_recv()
        mine = mine + down_in[i].astype(jnp.float32)
    down_out[...] = mine
    results = [
        pltpu.make_async_copy(down_out, down_result, out_sem.at[0]),
        pltpu.make_async_copy(up_out, up_result, out_sem.at[1]),
        pltpu.make_async_copy(prompt_out.at[0], prompt_result.at[0], out_sem.at[2]),
        pltpu.make_async_copy(prompt_out.at[1], prompt_result.at[1], out_sem.at[3]),
    ]
    results[0].start()
    prompt_sum(1)
    results[3].start()
    prompt_sum(0)
    results[2].start()
    up_back.wait_recv()
    results[1].start()
    for c in results:
        c.wait()
    for c in downs + ups + spread[0] + spread[1] + zero_to_one + [up_swap, down_swap, up_back]:
        c.wait_send()
    for i in range(2):

        @pl.when(core == 1)
        def _():
            near_back[i].wait_send()

        @pl.when(has_far)
        def _():
            far_back[i].wait_send()

        @pl.when(s >= 2)
        def _():
            two_back[i].wait_send()

    for i in range(2):

        @pl.when(has_two_on)
        def _():
            two_on[i].wait_send()

        @pl.when(has_three_on)
        def _():
            three_on[i].wait_send()

        @pl.when(core == 0)
        def _():
            next_on[i].wait_send()

        @pl.when(s >= 2)
        def _():
            hand_up[i].wait_send()


def gradients(n, nz, hidden, base, grad, down_w, up_w, lengths, offsets, keys, values):
    adapt_n, row_n, feature_n = base.shape
    stretch, hd = keys.shape
    rank, model = down_w.shape[1:]
    ranks = adapt_n * rank
    heads = 4
    wide = heads * row_n
    tiles = adapt_n * feature_n // (hd * heads)
    chunk = stretch
    quarter = stretch // nz
    up_shape = (2, ranks, feature_n // 2)
    down_shape = (n // 2, ranks, model // n)
    anywhere = pl.BlockSpec(memory_space=pl.ANY)
    dma = pltpu.SemaphoreType.DMA
    bf16 = jnp.bfloat16
    f32 = jnp.float32
    block = VMEM((2, stretch, hd), bf16)
    stat = VMEM((3, tiles, 1, wide), f32)
    return pl.pallas_call(
        functools.partial(attend_kernel, n, nz, heads, chunk),
        out_shape=(
            jax.ShapeDtypeStruct((ranks, model // n), f32),
            jax.ShapeDtypeStruct(up_shape, f32),
            jax.ShapeDtypeStruct((2, quarter, hd), f32),
        ),
        in_specs=[anywhere] * 9,
        out_specs=(anywhere,) * 3,
        scratch_shapes=[
            pltpu.SMEM(lengths.shape, jnp.int32),
            VMEM(down_w.shape, bf16),
            VMEM(up_w.shape, bf16),
            VMEM((adapt_n, 1, row_n), jnp.int32),
            VMEM((ranks, model // n), f32),
            VMEM(up_shape, f32),
            VMEM((2, quarter, hd), f32),
            VMEM((adapt_n, row_n, rank), bf16),
            VMEM((tiles, wide, hd), bf16),
            VMEM((4, 2, stretch, hd), bf16),
            VMEM(hidden.shape, bf16),
            VMEM(base.shape, bf16),
            VMEM(grad.shape, bf16),
            VMEM((tiles, wide, 2 * hd), bf16),
            VMEM((tiles, hd, wide), bf16),
            VMEM((tiles, hd, wide), bf16),
            VMEM((4, stretch, hd), bf16),
            VMEM((4, stretch, hd), bf16),
            VMEM((hd, 4 * stretch), bf16),
            VMEM((tiles, 3 * stretch, wide), f32),
            VMEM((tiles, 3 * stretch, wide), f32),
            stat, stat, stat, stat,
            VMEM((tiles, 1, wide), f32),
            VMEM((tiles, 1, wide), jnp.int32),
            VMEM((stretch, hd), f32),
            VMEM((tiles, hd, wide), f32),
            dma((9,)), dma((4,)), dma((3, 2)), dma((4, 2)),
            VMEM((2,) + down_shape, bf16),
            VMEM(up_shape, bf16),
            block, block, block, block, block, block,
            VMEM((nz - 1, 2, quarter, hd), bf16),
            VMEM(down_shape, bf16),
            VMEM(down_shape, bf16),
            VMEM((n // 2 - 1,) + down_shape[1:], bf16),
            VMEM(up_shape[1:], bf16),
            VMEM((n // 2,) + up_shape[1:], bf16),
            dma((2, 2)), dma((2, 2)), dma((2, 2)), dma((2, 2)), dma((nz - 1, 2)), dma((nz - 1, 2)),
            dma((n // 2 - 1,)), dma((n // 2 - 1,)), dma((n // 2 - 1,)), dma((n // 2 - 1,)), dma((3,)), dma((3,)),
        ],
        compiler_params=pltpu.CompilerParams(
            collective_id=0, has_side_effects=True, vmem_limit_bytes=60 * 1024 * 1024
        ),
        name="gradients",
    )(lengths, hidden, base, grad, down_w, up_w, offsets[:, None, :], keys, values)


def finish_kernel(down_hbm, up_hbm, prompt_hbm, down_out, up_out, key_out, value_out, down, up, sems):
    adapt_n, rank, _ = down_out.shape
    half = up.shape[2]
    pairs = ((up_hbm, up), (down_hbm, down), (prompt_hbm.at[0], key_out), (prompt_hbm.at[1], value_out))
    loads = [pltpu.make_async_copy(a, b, sems.at[i]) for i, (a, b) in enumerate(pairs)]
    for c in loads:
        c.start()
    for c in loads:
        c.wait()
    for a in range(adapt_n):
        down_out[a] = adapter_scale * down[a * rank : (a + 1) * rank, :]
        for j in range(2):
            up_out[a, :, j * half : (j + 1) * half] = adapter_scale * up[j, a * rank : (a + 1) * rank, :]


def finish(up_w, down, up, prompt):
    adapt_n, rank, feature_n = up_w.shape
    f32 = jnp.float32
    spec = pl.BlockSpec(memory_space=VMEM)
    side = jax.ShapeDtypeStruct(prompt.shape[1:], f32)
    return pl.pallas_call(
        finish_kernel,
        out_shape=(
            jax.ShapeDtypeStruct((adapt_n, rank, down.shape[1]), f32),
            jax.ShapeDtypeStruct(up_w.shape, f32),
            side,
            side,
        ),
        in_specs=[pl.BlockSpec(memory_space=pl.ANY)] * 3,
        out_specs=(spec,) * 4,
        scratch_shapes=[VMEM(down.shape, f32), VMEM(up.shape, f32), pltpu.SemaphoreType.DMA((4,))],
        name="finish",
    )(down, up, prompt)


def local(
    hidden,
    response_base_queries,
    attention_output_gradient,
    keys,
    values,
    adapter_down_weight,
    adapter_up_weight,
    lengths,
    offsets,
):
    n = lax.axis_size("seq")
    nz = lax.axis_size("adapter")
    sums = gradients(
        n,
        nz,
        hidden,
        response_base_queries,
        attention_output_gradient,
        adapter_down_weight,
        adapter_up_weight,
        lengths,
        offsets,
        keys,
        values,
    )
    return finish(adapter_up_weight, *sums)


def solution(mesh):
    return jax.shard_map(
        local,
        mesh=mesh,
        in_specs=(
            P("adapter", "seq", None),
            P("adapter", "seq", None),
            P("adapter", "seq", None),
            P("seq", None),
            P("seq", None),
            P("adapter", None, None),
            P("adapter", None, None),
            P("adapter"),
            P("adapter", "seq"),
        ),
        out_specs=(
            P("adapter", None, "seq"),
            P("adapter", None, None),
            P(("seq", "adapter"), None),
            P(("seq", "adapter"), None),
        ),
        check_vma=False,
    )
```

```python
import functools

import jax
import jax.numpy as jnp
from jax import lax
from jax.experimental import pallas as pl
from jax.experimental.pallas import tpu as pltpu
from jax.sharding import PartitionSpec as P

adapter_scale = 2.0
at_once = 2
masked_score = -1e30
MESH = pl.DeviceIdType.MESH
VMEM = pltpu.VMEM


def to_seq(index):
    return dict(device_id={"seq": index}, device_id_type=MESH)


def to_adapter(index):
    return dict(device_id={"adapter": index}, device_id_type=MESH)


def remote(src, dst, send_sem, recv_sem, target):
    return pltpu.make_async_remote_copy(
        src_ref=src, dst_ref=dst, send_sem=send_sem, recv_sem=recv_sem, **target
    )


def dot(a, b, dims):
    return lax.dot_general(a, b, (dims, ((), ())), preferred_element_type=jnp.float32)


def attend_kernel(
    n, nz, heads, chunk,
    len_hbm, hidden_hbm, base_hbm, grad_hbm, down_hbm, up_hbm, offset_hbm, keys_hbm, values_hbm,
    down_result, up_result, prompt_result,
    len_ref, down_w, up_w, offset_ref, down_out, up_out, prompt_out, low_ref, dq_ref, part, hidden, base, grad, gq_all, g_turned, q_turned, k_all, v_all, kt, s_ref, dp_ref, peaks, totals, inners,
    weight, delta, place_ref, acc, dq_acc, load_sem, out_sem, send_sem, recv_sem,
    down, up, pair_a, pair_b, back_two, back_three, summed, total, z_in, down_pair, down_chip, down_in,
    up_pair, up_all, pair_send, pair_recv, back_send, back_recv, z_send, z_recv, d_send, d_recv, u_send, u_recv,
    swap_send, swap_recv,
):
    s = lax.axis_index("seq")
    z = lax.axis_index("adapter")
    barrier = pltpu.get_barrier_semaphore()
    for i in range(1, n):
        pl.semaphore_signal(barrier, inc=1, **to_seq((s + i) % n))
    for i in range(1, nz):
        pl.semaphore_signal(barrier, inc=1, **to_adapter((z + i) % nz))
    core = s % 2
    partner = s + 1 - 2 * core
    adapt_n, rows, _ = base.shape
    _, stretch, hd = k_all.shape
    tiles, wide, _ = gq_all.shape
    per = tiles // adapt_n
    factor = hd**-0.5
    pieces = stretch // chunk
    pairs = (
        (down_hbm, down_w), (hidden_hbm, hidden), (len_hbm, len_ref), (offset_hbm, offset_ref), (up_hbm, up_w),
        (base_hbm, base), (grad_hbm, grad), (keys_hbm, k_all.at[0]), (values_hbm, v_all.at[0]),
    )
    loads = [pltpu.make_async_copy(a, b, load_sem.at[i]) for i, (a, b) in enumerate(pairs)]
    for c in loads:
        c.start()
    full = (k_all, v_all)
    own = (keys_hbm, values_hbm)

    def copy(i, src, slot, which, target):
        return remote(src, full[i].at[slot], send_sem.at[which, i], recv_sem.at[slot, i], to_seq(target))

    two_on = [copy(i, own[i], 2, 0, s + 2) for i in range(2)]
    three_on = [copy(i, own[i], 3, 1, s + 3) for i in range(2)]
    next_on = [copy(i, own[i], 1, 1, s + 1) for i in range(2)]
    hand_up = [copy(i, full[i].at[2], 3, 2, s + 1) for i in range(2)]
    hand_down = [copy(i, full[i].at[2], 1, 2, s - 1) for i in range(2)]

    def arrived(slot, i):
        @pl.when(s >= slot)
        def _():
            remote(
                full[i].at[slot], full[i].at[slot], send_sem.at[0, i], recv_sem.at[slot, i], to_seq(partner)
            ).wait_recv()

    has_three_in = (core == 1) & (s + 3 < n)
    pl.semaphore_wait(barrier, n - 1 + nz - 1)

    has_two_on = s + 2 < n
    has_three_on = (core == 1) & (s + 3 < n)
    for i in range(2):

        @pl.when(has_two_on)
        def _():
            two_on[i].start()

        @pl.when(has_three_on)
        def _():
            three_on[i].start()

        @pl.when(core == 0)
        def _():
            next_on[i].start()

    @pl.when(s + 2 >= n)
    def _():
        back_two[...] = jnp.zeros_like(back_two)

    @pl.when(jnp.logical_not(has_three_in))
    def _():
        back_three[...] = jnp.zeros_like(back_three)

    @pl.when(core == 1)
    def _():
        pair_b[...] = jnp.zeros_like(pair_b)

    for slot in (1, 2, 3):

        @pl.when(s < slot)
        def _():
            k_all[slot] = jnp.zeros(k_all.shape[1:], k_all.dtype)
            v_all[slot] = jnp.zeros(v_all.shape[1:], v_all.dtype)

    for c in loads:
        c.wait()
    for a in range(adapt_n):
        low = dot(hidden[a], down_w[a], ((1,), (1,))).astype(jnp.bfloat16)
        low_ref[a] = low
        place = jnp.concatenate([offset_ref[a]] * heads, axis=1) - s * stretch
        for t in range(per):
            place_ref[a * per + t] = place
        raised = dot(low, up_w[a], ((1,), (0,)))
        query = (base[a].astype(jnp.float32) + adapter_scale * raised).astype(jnp.bfloat16)
        live = s * rows + lax.broadcasted_iota(jnp.int32, (rows, 1), 0) < len_ref[a]
        g = jnp.where(live, grad[a], jnp.zeros_like(grad[a]))
        for h in range(per * heads):
            t, at_row = a * per + h // heads, (h % heads) * rows
            gq_all[t, at_row : at_row + rows, :hd] = g[:, h * hd : (h + 1) * hd]
            gq_all[t, at_row : at_row + rows, hd:] = query[:, h * hd : (h + 1) * hd]
            g_turned[t, :, at_row : at_row + rows] = g[:, h * hd : (h + 1) * hd].T
            q_turned[t, :, at_row : at_row + rows] = query[:, h * hd : (h + 1) * hd].T

    def hand(i):
        @pl.when(s >= 2)
        def _():
            @pl.when(core == 0)
            def _():
                hand_up[i].start()

            @pl.when(core == 1)
            def _():
                hand_down[i].start()

    def at(piece):
        return slice(piece * chunk, (piece + 1) * chunk)

    def each(first, last):
        step = at_once if (last - first) % at_once == 0 else 1

        def run(body):
            if last - first == step:
                for j in range(first, last):
                    body(j)
                return

            @pl.loop(first, last, step=step)
            def _(t):
                for j in range(step):
                    body(t + j)

        return run

    def before(piece, place):
        pos = piece * chunk + lax.broadcasted_iota(jnp.int32, (chunk, wide), 0)
        return pos <= place

    spots = {0: 0, 3: 1, 1: 2, 2: 3}

    def turned(d):
        kt[:, spots[d] * stretch : (spots[d] + 1) * stretch] = k_all[d].T

    def product(source, d, piece, other):
        return dot(source[d, at(piece), :], other, ((1,), (0,)))

    far_bias = jnp.where(s >= 3, 0.0, masked_score)

    @each(0, tiles)
    def _(t):
        q = q_turned[t]
        g = g_turned[t]
        for piece in range(pieces):
            s_ref[t, at(piece), :] = product(k_all, 0, piece, q) * factor
            dp_ref[t, at(piece), :] = product(v_all, 0, piece, g)

    def scores_of(d):
        @each(0, tiles)
        def _(t):
            q = q_turned[t]
            peak = jnp.full((1, wide), masked_score, jnp.float32)
            for piece in range(pieces):
                score = product(k_all, d or 3, piece, q) * factor
                if d == 0:
                    near = before(piece, place_ref[t])
                    score = jnp.where(near, s_ref[t, at(piece), :], score + far_bias)
                s_ref[t, at(d * pieces + piece), :] = score
                peak = jnp.maximum(peak, jnp.max(score, axis=0, keepdims=True))
            peaks[d, t] = peak

    def raise_of(d):
        @each(0, tiles)
        def _(t):
            g = g_turned[t]
            peak = peaks[d, t]
            total = jnp.zeros((1, wide), jnp.float32)
            inner = jnp.zeros((1, wide), jnp.float32)
            for piece in range(pieces):
                spot = at(d * pieces + piece)
                e = jnp.exp(s_ref[t, spot, :] - peak)
                dp = product(v_all, d or 3, piece, g)
                if d == 0:
                    dp = jnp.where(before(piece, place_ref[t]), dp_ref[t, spot, :], dp)
                s_ref[t, spot, :] = e
                dp_ref[t, spot, :] = dp
                total = total + jnp.sum(e, axis=0, keepdims=True)
                inner = inner + jnp.sum(e * dp, axis=0, keepdims=True)
            totals[d, t] = total
            inners[d, t] = inner

    arrived(2, 0)
    hand(0)
    turned(2)
    scores_of(2)
    arrived(1, 0)
    turned(1)
    scores_of(1)
    arrived(2, 1)
    hand(1)
    raise_of(2)
    arrived(1, 1)
    raise_of(1)
    arrived(3, 0)
    turned(3)
    turned(0)
    scores_of(0)
    arrived(3, 1)
    raise_of(0)

    @each(0, tiles)
    def _(t):
        tops = [peaks[0, t]] + [jnp.where(s >= d, peaks[d, t], masked_score) for d in (1, 2)]
        peak = jnp.maximum(jnp.maximum(tops[0], tops[1]), tops[2])
        shares = [jnp.exp(top - peak) for top in tops]
        total = jnp.zeros((1, wide), jnp.float32)
        inner = jnp.zeros((1, wide), jnp.float32)
        for d, share in enumerate(shares):
            total = total + totals[d, t] * share
            inner = inner + inners[d, t] * share
        inverse = 1.0 / total
        for d, share in enumerate(shares):
            weight[d, t] = share * inverse
        delta[t] = inner * inverse

    def rows_of(unit, piece):
        if isinstance(unit, int):
            return at(unit * pieces + piece)
        return pl.ds(pl.multiple_of(unit * stretch + piece * chunk, chunk), chunk)

    def gather_up(block, i, first=0, last=tiles):
        static = isinstance(block, int)
        unit = 0 if static else block
        if first == 0:
            acc[...] = jnp.zeros_like(acc)

        @each(first, last)
        def _(t):
            other = gq_all[t]
            share = weight[unit, t]
            lows = []
            for piece in range(pieces):
                spot = rows_of(unit, piece)
                value = s_ref[t, spot, :] * share
                if i == 0:
                    value = value * (dp_ref[t, spot, :] - delta[t])
                if static:
                    near = before(piece, place_ref[t])
                    value = jnp.where(near, 0.0, value) if block else jnp.where(near, value, 0.0)
                low = value.astype(jnp.bfloat16)
                both = dot(low, other, ((1,), (0,)))
                acc[at(piece), :] += both[:, :hd] if i else both[:, hd:]
                lows.append(low)
            if i == 0:
                if static:
                    turned_block = kt[:, spots[block] * stretch : (spots[block] + 1) * stretch]
                else:
                    turned_block = kt[:, pl.ds(pl.multiple_of((block + 1) * stretch, stretch), stretch)]
                dq = dot(turned_block, jnp.concatenate(lows, axis=0), ((1,), (0,)))
                if static and block == 3:
                    dq_acc[t] = dq
                else:
                    dq_acc[t] += dq

        if last == tiles:
            out = acc[...]
            part[block, i] = (out if i else out * factor).astype(jnp.bfloat16)

    quarter = prompt_out.shape[1]
    has_far = (core == 0) & (s >= 3)

    def pair_copy(d, to, i, j):
        return remote(part.at[d, i], to.at[i], pair_send.at[j, i], pair_recv.at[j, i], to_seq(partner))

    zero_to_one = [pair_copy(1, pair_a, i, 0) for i in range(2)]
    one_to_zero = [pair_copy(3, pair_a, i, 0) for i in range(2)]
    near_back = [pair_copy(1, pair_b, i, 1) for i in range(2)]
    far_back = [
        remote(part.at[3, i], back_three.at[i], back_send.at[1, i], back_recv.at[1, i], to_seq(s - 3))
        for i in range(2)
    ]
    two_back = [
        remote(summed.at[i], back_two.at[i], back_send.at[0, i], back_recv.at[0, i], to_seq(s - 2))
        for i in range(2)
    ]
    chips = n // 2
    chip = s // 2
    down_swap = remote(down.at[1 - core], down_pair, swap_send.at[0], swap_recv.at[0], to_seq(partner))
    up_swap = remote(up.at[1 - core], up_pair, swap_send.at[1], swap_recv.at[1], to_seq(partner))
    up_back = remote(up_out.at[core], up_out.at[core], swap_send.at[2], swap_recv.at[2], to_seq(partner))
    downs, ups = [], []
    for i in range(1, chips):
        peer = (chip + i) % chips
        target = to_seq(2 * peer + core)
        downs.append(remote(down_chip.at[peer], down_in.at[i - 1], d_send.at[i - 1], d_recv.at[i - 1], target))
        ups.append(remote(up_all.at[chip], up_all.at[chip], u_send.at[i - 1], u_recv.at[i - 1], target))

    def sum_pair(i):
        zero_to_one[i].wait_recv()
        summed[i] = (part[2, i].astype(jnp.float32) + pair_a[i].astype(jnp.float32)).astype(jnp.bfloat16)

        @pl.when(s >= 2)
        def _():
            two_back[i].start()

    spread = [[], []]

    def owner(i):
        @pl.when(core == 0)
        def _():
            near_back[i].wait_recv()

        @pl.when(s + 2 < n)
        def _():
            two_back[i].wait_recv()

        @pl.when(has_three_in)
        def _():
            far_back[i].wait_recv()

        total[i] = (
            part[0, i].astype(jnp.float32)
            + pair_b[i].astype(jnp.float32)
            + back_two[i].astype(jnp.float32)
            + back_three[i].astype(jnp.float32)
        ).astype(jnp.bfloat16)
        for j in range(1, nz):
            peer = (z + j) % nz
            c = remote(
                total.at[i, pl.ds(pl.multiple_of(peer * quarter, 16), quarter), :],
                z_in.at[j - 1, i], z_send.at[j - 1, i], z_recv.at[j - 1, i], to_adapter(peer),
            )
            c.start()
            spread[i].append(c)

    def prompt_sum(i):
        mine = total[i, pl.ds(pl.multiple_of(z * quarter, 16), quarter), :].astype(jnp.float32)
        for j, c in enumerate(spread[i]):
            c.wait_recv()
            mine = mine + z_in[j, i].astype(jnp.float32)
        prompt_out[i] = mine

    def far_out(i):
        @pl.when(core == 1)
        def _():
            one_to_zero[i].start()

        @pl.when(has_far)
        def _():
            far_back[i].start()

    def sum_on(which, i):
        @pl.when(core == which)
        def _():
            sum_pair(i)

    second = 1 + core
    third = 2 - core
    middle = tiles // 2

    def second_out(i):
        gather_up(second, i)

        @pl.when(core == 0)
        def _():
            zero_to_one[i].start()

    def third_out(i):
        gather_up(third, i, 0, middle)
        sum_on(1, i)
        gather_up(third, i, middle, tiles)
        sum_on(0, i)

        @pl.when(core == 1)
        def _():
            near_back[i].start()

    gather_up(3, 1)
    far_out(1)
    second_out(1)
    third_out(1)
    gather_up(3, 0)
    far_out(0)
    gather_up(0, 1)
    second_out(0)
    owner(1)
    third_out(0)
    gather_up(0, 0)

    @each(0, tiles)
    def _(t):
        dq_ref[t] = (dq_acc[t] * factor).T.astype(jnp.bfloat16)

    _, rank, feature_n = up_w.shape
    group = feature_n // hd
    half = feature_n // 2
    width = down_out.shape[1]
    smalls = []
    for a in range(adapt_n):
        small = jnp.zeros((rows, rank), jnp.float32)
        for h in range(group):
            place = a * group + h
            dq_h = dq_ref[place // heads, (place % heads) * rows : (place % heads + 1) * rows, :]
            up_h = dot(low_ref[a], dq_h, ((0,), (0,)))
            begin = h * hd % half
            up[h * hd // half, a * rank : (a + 1) * rank, begin : begin + hd] = up_h.astype(jnp.bfloat16)
            small = small + dot(dq_h, up_w[a, :, h * hd : (h + 1) * hd], ((1,), (1,)))
        smalls.append(small.astype(jnp.bfloat16))
    up_swap.start()
    for a in range(adapt_n):
        out = dot(smalls[a], hidden[a], ((0,), (0,))).astype(jnp.bfloat16)
        for j in range(n):
            down[j % 2, j // 2, a * rank : (a + 1) * rank, :] = out[:, j * width : (j + 1) * width]
    down_swap.start()
    up_swap.wait_recv()
    up_all[chip] = (up[core].astype(jnp.float32) + up_pair[...].astype(jnp.float32)).astype(jnp.bfloat16)
    for c in ups:
        c.start()
    down_swap.wait_recv()
    for j in range(chips):
        both = down[core, j].astype(jnp.float32) + down_pair[j].astype(jnp.float32)
        down_chip[j] = both.astype(jnp.bfloat16)
    for c in downs:
        c.start()
    owner(0)
    for c in ups:
        c.wait_recv()
    mine = up_all[0].astype(jnp.float32)
    for j in range(1, chips):
        mine = mine + up_all[j].astype(jnp.float32)
    up_out[core] = mine
    up_back.start()
    mine = down[core, chip].astype(jnp.float32) + down_pair[chip].astype(jnp.float32)
    for i, c in enumerate(downs):
        c.wait_recv()
        mine = mine + down_in[i].astype(jnp.float32)
    down_out[...] = mine
    results = [
        pltpu.make_async_copy(down_out, down_result, out_sem.at[0]),
        pltpu.make_async_copy(up_out, up_result, out_sem.at[1]),
        pltpu.make_async_copy(prompt_out.at[0], prompt_result.at[0], out_sem.at[2]),
        pltpu.make_async_copy(prompt_out.at[1], prompt_result.at[1], out_sem.at[3]),
    ]
    results[0].start()
    prompt_sum(1)
    results[3].start()
    prompt_sum(0)
    results[2].start()
    up_back.wait_recv()
    results[1].start()
    for c in results:
        c.wait()
    for c in downs + ups + spread[0] + spread[1] + zero_to_one + [up_swap, down_swap, up_back]:
        c.wait_send()
    for i in range(2):

        @pl.when(core == 1)
        def _():
            near_back[i].wait_send()

        @pl.when(has_far)
        def _():
            far_back[i].wait_send()

        @pl.when(s >= 2)
        def _():
            two_back[i].wait_send()

    for i in range(2):

        @pl.when(has_two_on)
        def _():
            two_on[i].wait_send()

        @pl.when(has_three_on)
        def _():
            three_on[i].wait_send()

        @pl.when(core == 0)
        def _():
            next_on[i].wait_send()

        @pl.when(s >= 2)
        def _():
            hand_up[i].wait_send()


def gradients(n, nz, hidden, base, grad, down_w, up_w, lengths, offsets, keys, values):
    adapt_n, row_n, feature_n = base.shape
    stretch, hd = keys.shape
    rank, model = down_w.shape[1:]
    ranks = adapt_n * rank
    heads = 4
    wide = heads * row_n
    tiles = adapt_n * feature_n // (hd * heads)
    chunk = stretch
    quarter = stretch // nz
    up_shape = (2, ranks, feature_n // 2)
    down_shape = (n // 2, ranks, model // n)
    anywhere = pl.BlockSpec(memory_space=pl.ANY)
    dma = pltpu.SemaphoreType.DMA
    bf16 = jnp.bfloat16
    f32 = jnp.float32
    block = VMEM((2, stretch, hd), bf16)
    stat = VMEM((3, tiles, 1, wide), f32)
    return pl.pallas_call(
        functools.partial(attend_kernel, n, nz, heads, chunk),
        out_shape=(
            jax.ShapeDtypeStruct((ranks, model // n), f32),
            jax.ShapeDtypeStruct(up_shape, f32),
            jax.ShapeDtypeStruct((2, quarter, hd), f32),
        ),
        in_specs=[anywhere] * 9,
        out_specs=(anywhere,) * 3,
        scratch_shapes=[
            pltpu.SMEM(lengths.shape, jnp.int32),
            VMEM(down_w.shape, bf16),
            VMEM(up_w.shape, bf16),
            VMEM((adapt_n, 1, row_n), jnp.int32),
            VMEM((ranks, model // n), f32),
            VMEM(up_shape, f32),
            VMEM((2, quarter, hd), f32),
            VMEM((adapt_n, row_n, rank), bf16),
            VMEM((tiles, wide, hd), bf16),
            VMEM((4, 2, stretch, hd), bf16),
            VMEM(hidden.shape, bf16),
            VMEM(base.shape, bf16),
            VMEM(grad.shape, bf16),
            VMEM((tiles, wide, 2 * hd), bf16),
            VMEM((tiles, hd, wide), bf16),
            VMEM((tiles, hd, wide), bf16),
            VMEM((4, stretch, hd), bf16),
            VMEM((4, stretch, hd), bf16),
            VMEM((hd, 4 * stretch), bf16),
            VMEM((tiles, 3 * stretch, wide), f32),
            VMEM((tiles, 3 * stretch, wide), f32),
            stat, stat, stat, stat,
            VMEM((tiles, 1, wide), f32),
            VMEM((tiles, 1, wide), jnp.int32),
            VMEM((stretch, hd), f32),
            VMEM((tiles, hd, wide), f32),
            dma((9,)), dma((4,)), dma((3, 2)), dma((4, 2)),
            VMEM((2,) + down_shape, bf16),
            VMEM(up_shape, bf16),
            block, block, block, block, block, block,
            VMEM((nz - 1, 2, quarter, hd), bf16),
            VMEM(down_shape, bf16),
            VMEM(down_shape, bf16),
            VMEM((n // 2 - 1,) + down_shape[1:], bf16),
            VMEM(up_shape[1:], bf16),
            VMEM((n // 2,) + up_shape[1:], bf16),
            dma((2, 2)), dma((2, 2)), dma((2, 2)), dma((2, 2)), dma((nz - 1, 2)), dma((nz - 1, 2)),
            dma((n // 2 - 1,)), dma((n // 2 - 1,)), dma((n // 2 - 1,)), dma((n // 2 - 1,)), dma((3,)), dma((3,)),
        ],
        compiler_params=pltpu.CompilerParams(
            collective_id=0, has_side_effects=True, vmem_limit_bytes=60 * 1024 * 1024
        ),
        name="gradients",
    )(lengths, hidden, base, grad, down_w, up_w, offsets[:, None, :], keys, values)


def finish_kernel(down_hbm, up_hbm, prompt_hbm, down_out, up_out, key_out, value_out, down, up, sems):
    adapt_n, rank, _ = down_out.shape
    half = up.shape[2]
    pairs = ((up_hbm, up), (down_hbm, down), (prompt_hbm.at[0], key_out), (prompt_hbm.at[1], value_out))
    loads = [pltpu.make_async_copy(a, b, sems.at[i]) for i, (a, b) in enumerate(pairs)]
    for c in loads:
        c.start()
    for c in loads:
        c.wait()
    for a in range(adapt_n):
        down_out[a] = adapter_scale * down[a * rank : (a + 1) * rank, :]
        for j in range(2):
            up_out[a, :, j * half : (j + 1) * half] = adapter_scale * up[j, a * rank : (a + 1) * rank, :]


def finish(up_w, down, up, prompt):
    adapt_n, rank, feature_n = up_w.shape
    f32 = jnp.float32
    spec = pl.BlockSpec(memory_space=VMEM)
    side = jax.ShapeDtypeStruct(prompt.shape[1:], f32)
    return pl.pallas_call(
        finish_kernel,
        out_shape=(
            jax.ShapeDtypeStruct((adapt_n, rank, down.shape[1]), f32),
            jax.ShapeDtypeStruct(up_w.shape, f32),
            side,
            side,
        ),
        in_specs=[pl.BlockSpec(memory_space=pl.ANY)] * 3,
        out_specs=(spec,) * 4,
        scratch_shapes=[VMEM(down.shape, f32), VMEM(up.shape, f32), pltpu.SemaphoreType.DMA((4,))],
        name="finish",
    )(down, up, prompt)


def local(
    hidden,
    response_base_queries,
    attention_output_gradient,
    keys,
    values,
    adapter_down_weight,
    adapter_up_weight,
    lengths,
    offsets,
):
    n = lax.axis_size("seq")
    nz = lax.axis_size("adapter")
    sums = gradients(
        n,
        nz,
        hidden,
        response_base_queries,
        attention_output_gradient,
        adapter_down_weight,
        adapter_up_weight,
        lengths,
        offsets,
        keys,
        values,
    )
    return finish(adapter_up_weight, *sums)


def solution(mesh):
    return jax.shard_map(
        local,
        mesh=mesh,
        in_specs=(
            P("adapter", "seq", None),
            P("adapter", "seq", None),
            P("adapter", "seq", None),
            P("seq", None),
            P("seq", None),
            P("adapter", None, None),
            P("adapter", None, None),
            P("adapter"),
            P("adapter", "seq"),
        ),
        out_specs=(
            P("adapter", None, "seq"),
            P("adapter", None, None),
            P(("seq", "adapter"), None),
            P(("seq", "adapter"), None),
        ),
        check_vma=False,
    )
```

```python
import functools

import jax
import jax.numpy as jnp
from jax import lax
from jax.experimental import pallas as pl
from jax.experimental.pallas import tpu as pltpu
from jax.sharding import PartitionSpec as P

adapter_scale = 2.0
at_once = 2
masked_score = -1e30
MESH = pl.DeviceIdType.MESH
VMEM = pltpu.VMEM


def to_seq(index):
    return dict(device_id={"seq": index}, device_id_type=MESH)


def to_adapter(index):
    return dict(device_id={"adapter": index}, device_id_type=MESH)


def remote(src, dst, send_sem, recv_sem, target):
    return pltpu.make_async_remote_copy(
        src_ref=src, dst_ref=dst, send_sem=send_sem, recv_sem=recv_sem, **target
    )


def dot(a, b, dims):
    return lax.dot_general(a, b, (dims, ((), ())), preferred_element_type=jnp.float32)


def attend_kernel(
    n, nz, heads, chunk,
    len_hbm, hidden_hbm, base_hbm, grad_hbm, down_hbm, up_hbm, offset_hbm, keys_hbm, values_hbm,
    down_result, up_result, prompt_result,
    len_ref, down_w, up_w, offset_ref, down_out, up_out, prompt_out, low_ref, dq_ref, part, hidden, base, grad, gq_all, g_turned, q_turned, k_all, v_all, kt, s_ref, dp_ref, peaks, totals, inners,
    weight, delta, place_ref, acc, dq_acc, load_sem, out_sem, send_sem, recv_sem,
    down, up, pair_a, pair_b, back_two, back_three, summed, total, z_in, down_pair, down_chip, down_in,
    up_pair, up_all, pair_send, pair_recv, back_send, back_recv, z_send, z_recv, d_send, d_recv, u_send, u_recv,
    swap_send, swap_recv,
):
    s = lax.axis_index("seq")
    z = lax.axis_index("adapter")
    barrier = pltpu.get_barrier_semaphore()
    for i in range(1, n):
        pl.semaphore_signal(barrier, inc=1, **to_seq((s + i) % n))
    for i in range(1, nz):
        pl.semaphore_signal(barrier, inc=1, **to_adapter((z + i) % nz))
    core = s % 2
    partner = s + 1 - 2 * core
    adapt_n, rows, _ = base.shape
    _, stretch, hd = k_all.shape
    tiles, wide, _ = gq_all.shape
    per = tiles // adapt_n
    factor = hd**-0.5
    pieces = stretch // chunk
    pairs = (
        (down_hbm, down_w), (hidden_hbm, hidden), (len_hbm, len_ref), (offset_hbm, offset_ref), (up_hbm, up_w),
        (base_hbm, base), (grad_hbm, grad), (keys_hbm, k_all.at[0]), (values_hbm, v_all.at[0]),
    )
    loads = [pltpu.make_async_copy(a, b, load_sem.at[i]) for i, (a, b) in enumerate(pairs)]
    for c in loads:
        c.start()
    full = (k_all, v_all)
    own = (keys_hbm, values_hbm)

    def copy(i, src, slot, which, target):
        return remote(src, full[i].at[slot], send_sem.at[which, i], recv_sem.at[slot, i], to_seq(target))

    two_on = [copy(i, own[i], 2, 0, s + 2) for i in range(2)]
    three_on = [copy(i, own[i], 3, 1, s + 3) for i in range(2)]
    next_on = [copy(i, own[i], 1, 1, s + 1) for i in range(2)]
    hand_up = [copy(i, full[i].at[2], 3, 2, s + 1) for i in range(2)]
    hand_down = [copy(i, full[i].at[2], 1, 2, s - 1) for i in range(2)]

    def arrived(slot, i):
        @pl.when(s >= slot)
        def _():
            remote(
                full[i].at[slot], full[i].at[slot], send_sem.at[0, i], recv_sem.at[slot, i], to_seq(partner)
            ).wait_recv()

    has_three_in = (core == 1) & (s + 3 < n)
    pl.semaphore_wait(barrier, n - 1 + nz - 1)

    has_two_on = s + 2 < n
    has_three_on = (core == 1) & (s + 3 < n)
    for i in range(2):

        @pl.when(has_two_on)
        def _():
            two_on[i].start()

        @pl.when(has_three_on)
        def _():
            three_on[i].start()

        @pl.when(core == 0)
        def _():
            next_on[i].start()

    @pl.when(s + 2 >= n)
    def _():
        back_two[...] = jnp.zeros_like(back_two)

    @pl.when(jnp.logical_not(has_three_in))
    def _():
        back_three[...] = jnp.zeros_like(back_three)

    @pl.when(core == 1)
    def _():
        pair_b[...] = jnp.zeros_like(pair_b)

    for slot in (1, 2, 3):

        @pl.when(s < slot)
        def _():
            k_all[slot] = jnp.zeros(k_all.shape[1:], k_all.dtype)
            v_all[slot] = jnp.zeros(v_all.shape[1:], v_all.dtype)

    for c in loads:
        c.wait()
    for a in range(adapt_n):
        low = dot(hidden[a], down_w[a], ((1,), (1,))).astype(jnp.bfloat16)
        low_ref[a] = low
        place = jnp.concatenate([offset_ref[a]] * heads, axis=1) - s * stretch
        for t in range(per):
            place_ref[a * per + t] = place
        raised = dot(low, up_w[a], ((1,), (0,)))
        query = (base[a].astype(jnp.float32) + adapter_scale * raised).astype(jnp.bfloat16)
        live = s * rows + lax.broadcasted_iota(jnp.int32, (rows, 1), 0) < len_ref[a]
        g = jnp.where(live, grad[a], jnp.zeros_like(grad[a]))
        for h in range(per * heads):
            t, at_row = a * per + h // heads, (h % heads) * rows
            gq_all[t, at_row : at_row + rows, :hd] = g[:, h * hd : (h + 1) * hd]
            gq_all[t, at_row : at_row + rows, hd:] = query[:, h * hd : (h + 1) * hd]
            g_turned[t, :, at_row : at_row + rows] = g[:, h * hd : (h + 1) * hd].T
            q_turned[t, :, at_row : at_row + rows] = query[:, h * hd : (h + 1) * hd].T

    def hand(i):
        @pl.when(s >= 2)
        def _():
            @pl.when(core == 0)
            def _():
                hand_up[i].start()

            @pl.when(core == 1)
            def _():
                hand_down[i].start()

    def at(piece):
        return slice(piece * chunk, (piece + 1) * chunk)

    def each(first, last):
        step = at_once if (last - first) % at_once == 0 else 1

        def run(body):
            if last - first == step:
                for j in range(first, last):
                    body(j)
                return

            @pl.loop(first, last, step=step)
            def _(t):
                for j in range(step):
                    body(t + j)

        return run

    def before(piece, place):
        pos = piece * chunk + lax.broadcasted_iota(jnp.int32, (chunk, wide), 0)
        return pos <= place

    spots = {0: 0, 3: 1, 1: 2, 2: 3}

    def turned(d):
        kt[:, spots[d] * stretch : (spots[d] + 1) * stretch] = k_all[d].T

    def product(source, d, piece, other):
        return dot(source[d, at(piece), :], other, ((1,), (0,)))

    far_bias = jnp.where(s >= 3, 0.0, masked_score)

    @each(0, tiles)
    def _(t):
        q = q_turned[t]
        g = g_turned[t]
        for piece in range(pieces):
            s_ref[t, at(piece), :] = product(k_all, 0, piece, q) * factor
            dp_ref[t, at(piece), :] = product(v_all, 0, piece, g)

    def scores_of(d):
        @each(0, tiles)
        def _(t):
            q = q_turned[t]
            peak = jnp.full((1, wide), masked_score, jnp.float32)
            for piece in range(pieces):
                score = product(k_all, d or 3, piece, q) * factor
                if d == 0:
                    near = before(piece, place_ref[t])
                    score = jnp.where(near, s_ref[t, at(piece), :], score + far_bias)
                s_ref[t, at(d * pieces + piece), :] = score
                peak = jnp.maximum(peak, jnp.max(score, axis=0, keepdims=True))
            peaks[d, t] = peak

    def raise_of(d):
        @each(0, tiles)
        def _(t):
            g = g_turned[t]
            peak = peaks[d, t]
            total = jnp.zeros((1, wide), jnp.float32)
            inner = jnp.zeros((1, wide), jnp.float32)
            for piece in range(pieces):
                spot = at(d * pieces + piece)
                e = jnp.exp(s_ref[t, spot, :] - peak)
                dp = product(v_all, d or 3, piece, g)
                if d == 0:
                    dp = jnp.where(before(piece, place_ref[t]), dp_ref[t, spot, :], dp)
                s_ref[t, spot, :] = e
                dp_ref[t, spot, :] = dp
                total = total + jnp.sum(e, axis=0, keepdims=True)
                inner = inner + jnp.sum(e * dp, axis=0, keepdims=True)
            totals[d, t] = total
            inners[d, t] = inner

    arrived(2, 0)
    hand(0)
    turned(2)
    scores_of(2)
    arrived(1, 0)
    turned(1)
    scores_of(1)
    arrived(2, 1)
    hand(1)
    raise_of(2)
    arrived(1, 1)
    raise_of(1)
    arrived(3, 0)
    turned(3)
    turned(0)
    scores_of(0)
    arrived(3, 1)
    raise_of(0)

    @each(0, tiles)
    def _(t):
        tops = [peaks[0, t]] + [jnp.where(s >= d, peaks[d, t], masked_score) for d in (1, 2)]
        peak = jnp.maximum(jnp.maximum(tops[0], tops[1]), tops[2])
        shares = [jnp.exp(top - peak) for top in tops]
        total = jnp.zeros((1, wide), jnp.float32)
        inner = jnp.zeros((1, wide), jnp.float32)
        for d, share in enumerate(shares):
            total = total + totals[d, t] * share
            inner = inner + inners[d, t] * share
        inverse = 1.0 / total
        for d, share in enumerate(shares):
            weight[d, t] = share * inverse
        delta[t] = inner * inverse

    def rows_of(unit, piece):
        if isinstance(unit, int):
            return at(unit * pieces + piece)
        return pl.ds(pl.multiple_of(unit * stretch + piece * chunk, chunk), chunk)

    def gather_up(block, i, first=0, last=tiles):
        static = isinstance(block, int)
        unit = 0 if static else block
        if first == 0:
            acc[...] = jnp.zeros_like(acc)

        @each(first, last)
        def _(t):
            other = gq_all[t]
            share = weight[unit, t]
            lows = []
            for piece in range(pieces):
                spot = rows_of(unit, piece)
                if i == 0 and static and block == 0:
                    value = dp_ref[t, spot, :]
                else:
                    value = s_ref[t, spot, :] * share
                    if i == 0:
                        value = value * (dp_ref[t, spot, :] - delta[t])
                    if i == 0 and static:
                        dp_ref[t, spot, :] = value
                if static:
                    near = before(piece, place_ref[t])
                    value = jnp.where(near, 0.0, value) if block else jnp.where(near, value, 0.0)
                low = value.astype(jnp.bfloat16)
                both = dot(low, other, ((1,), (0,)))
                acc[at(piece), :] += both[:, :hd] if i else both[:, hd:]
                lows.append(low)
            if i == 0:
                if static:
                    turned_block = kt[:, spots[block] * stretch : (spots[block] + 1) * stretch]
                else:
                    turned_block = kt[:, pl.ds(pl.multiple_of((block + 1) * stretch, stretch), stretch)]
                dq = dot(turned_block, jnp.concatenate(lows, axis=0), ((1,), (0,)))
                if static and block == 3:
                    dq_acc[t] = dq
                else:
                    dq_acc[t] += dq

        if last == tiles:
            out = acc[...]
            part[block, i] = (out if i else out * factor).astype(jnp.bfloat16)

    quarter = prompt_out.shape[1]
    has_far = (core == 0) & (s >= 3)

    def pair_copy(d, to, i, j):
        return remote(part.at[d, i], to.at[i], pair_send.at[j, i], pair_recv.at[j, i], to_seq(partner))

    zero_to_one = [pair_copy(1, pair_a, i, 0) for i in range(2)]
    one_to_zero = [pair_copy(3, pair_a, i, 0) for i in range(2)]
    near_back = [pair_copy(1, pair_b, i, 1) for i in range(2)]
    far_back = [
        remote(part.at[3, i], back_three.at[i], back_send.at[1, i], back_recv.at[1, i], to_seq(s - 3))
        for i in range(2)
    ]
    two_back = [
        remote(summed.at[i], back_two.at[i], back_send.at[0, i], back_recv.at[0, i], to_seq(s - 2))
        for i in range(2)
    ]
    chips = n // 2
    chip = s // 2
    down_swap = remote(down.at[1 - core], down_pair, swap_send.at[0], swap_recv.at[0], to_seq(partner))
    up_swap = remote(up.at[1 - core], up_pair, swap_send.at[1], swap_recv.at[1], to_seq(partner))
    up_back = remote(up_out.at[core], up_out.at[core], swap_send.at[2], swap_recv.at[2], to_seq(partner))
    downs, ups = [], []
    for i in range(1, chips):
        peer = (chip + i) % chips
        target = to_seq(2 * peer + core)
        downs.append(remote(down_chip.at[peer], down_in.at[i - 1], d_send.at[i - 1], d_recv.at[i - 1], target))
        ups.append(remote(up_all.at[chip], up_all.at[chip], u_send.at[i - 1], u_recv.at[i - 1], target))

    def sum_pair(i):
        zero_to_one[i].wait_recv()
        summed[i] = (part[2, i].astype(jnp.float32) + pair_a[i].astype(jnp.float32)).astype(jnp.bfloat16)

        @pl.when(s >= 2)
        def _():
            two_back[i].start()

    spread = [[], []]

    def owner(i):
        @pl.when(core == 0)
        def _():
            near_back[i].wait_recv()

        @pl.when(s + 2 < n)
        def _():
            two_back[i].wait_recv()

        @pl.when(has_three_in)
        def _():
            far_back[i].wait_recv()

        total[i] = (
            part[0, i].astype(jnp.float32)
            + pair_b[i].astype(jnp.float32)
            + back_two[i].astype(jnp.float32)
            + back_three[i].astype(jnp.float32)
        ).astype(jnp.bfloat16)
        for j in range(1, nz):
            peer = (z + j) % nz
            c = remote(
                total.at[i, pl.ds(pl.multiple_of(peer * quarter, 16), quarter), :],
                z_in.at[j - 1, i], z_send.at[j - 1, i], z_recv.at[j - 1, i], to_adapter(peer),
            )
            c.start()
            spread[i].append(c)

    def prompt_sum(i):
        mine = total[i, pl.ds(pl.multiple_of(z * quarter, 16), quarter), :].astype(jnp.float32)
        for j, c in enumerate(spread[i]):
            c.wait_recv()
            mine = mine + z_in[j, i].astype(jnp.float32)
        prompt_out[i] = mine

    def far_out(i):
        @pl.when(core == 1)
        def _():
            one_to_zero[i].start()

        @pl.when(has_far)
        def _():
            far_back[i].start()

    def sum_on(which, i):
        @pl.when(core == which)
        def _():
            sum_pair(i)

    second = 1 + core
    third = 2 - core
    middle = tiles // 2

    def second_out(i):
        gather_up(second, i)

        @pl.when(core == 0)
        def _():
            zero_to_one[i].start()

    def third_out(i):
        gather_up(third, i, 0, middle)
        sum_on(1, i)
        gather_up(third, i, middle, tiles)
        sum_on(0, i)

        @pl.when(core == 1)
        def _():
            near_back[i].start()

    gather_up(3, 1)
    far_out(1)
    second_out(1)
    third_out(1)
    gather_up(3, 0)
    far_out(0)
    gather_up(0, 1)
    second_out(0)
    owner(1)
    third_out(0)
    gather_up(0, 0)

    @each(0, tiles)
    def _(t):
        dq_ref[t] = (dq_acc[t] * factor).T.astype(jnp.bfloat16)

    _, rank, feature_n = up_w.shape
    group = feature_n // hd
    half = feature_n // 2
    width = down_out.shape[1]
    smalls = []
    for a in range(adapt_n):
        small = jnp.zeros((rows, rank), jnp.float32)
        for h in range(group):
            place = a * group + h
            dq_h = dq_ref[place // heads, (place % heads) * rows : (place % heads + 1) * rows, :]
            up_h = dot(low_ref[a], dq_h, ((0,), (0,)))
            begin = h * hd % half
            up[h * hd // half, a * rank : (a + 1) * rank, begin : begin + hd] = up_h.astype(jnp.bfloat16)
            small = small + dot(dq_h, up_w[a, :, h * hd : (h + 1) * hd], ((1,), (1,)))
        smalls.append(small.astype(jnp.bfloat16))
    up_swap.start()
    for a in range(adapt_n):
        out = dot(smalls[a], hidden[a], ((0,), (0,))).astype(jnp.bfloat16)
        for j in range(n):
            down[j % 2, j // 2, a * rank : (a + 1) * rank, :] = out[:, j * width : (j + 1) * width]
    down_swap.start()
    up_swap.wait_recv()
    up_all[chip] = (up[core].astype(jnp.float32) + up_pair[...].astype(jnp.float32)).astype(jnp.bfloat16)
    for c in ups:
        c.start()
    owner(0)
    down_swap.wait_recv()
    for j in range(chips):
        both = down[core, j].astype(jnp.float32) + down_pair[j].astype(jnp.float32)
        down_chip[j] = both.astype(jnp.bfloat16)
    for c in downs:
        c.start()
    for c in ups:
        c.wait_recv()
    mine = up_all[0].astype(jnp.float32)
    for j in range(1, chips):
        mine = mine + up_all[j].astype(jnp.float32)
    up_out[core] = mine
    up_back.start()
    mine = down[core, chip].astype(jnp.float32) + down_pair[chip].astype(jnp.float32)
    for i, c in enumerate(downs):
        c.wait_recv()
        mine = mine + down_in[i].astype(jnp.float32)
    down_out[...] = mine
    results = [
        pltpu.make_async_copy(down_out, down_result, out_sem.at[0]),
        pltpu.make_async_copy(up_out, up_result, out_sem.at[1]),
        pltpu.make_async_copy(prompt_out.at[0], prompt_result.at[0], out_sem.at[2]),
        pltpu.make_async_copy(prompt_out.at[1], prompt_result.at[1], out_sem.at[3]),
    ]
    results[0].start()
    prompt_sum(1)
    results[3].start()
    prompt_sum(0)
    results[2].start()
    up_back.wait_recv()
    results[1].start()
    for c in results:
        c.wait()
    for c in downs + ups + spread[0] + spread[1] + zero_to_one + [up_swap, down_swap, up_back]:
        c.wait_send()
    for i in range(2):

        @pl.when(core == 1)
        def _():
            near_back[i].wait_send()

        @pl.when(has_far)
        def _():
            far_back[i].wait_send()

        @pl.when(s >= 2)
        def _():
            two_back[i].wait_send()

    for i in range(2):

        @pl.when(has_two_on)
        def _():
            two_on[i].wait_send()

        @pl.when(has_three_on)
        def _():
            three_on[i].wait_send()

        @pl.when(core == 0)
        def _():
            next_on[i].wait_send()

        @pl.when(s >= 2)
        def _():
            hand_up[i].wait_send()


def gradients(n, nz, hidden, base, grad, down_w, up_w, lengths, offsets, keys, values):
    adapt_n, row_n, feature_n = base.shape
    stretch, hd = keys.shape
    rank, model = down_w.shape[1:]
    ranks = adapt_n * rank
    heads = 4
    wide = heads * row_n
    tiles = adapt_n * feature_n // (hd * heads)
    chunk = stretch
    quarter = stretch // nz
    up_shape = (2, ranks, feature_n // 2)
    down_shape = (n // 2, ranks, model // n)
    anywhere = pl.BlockSpec(memory_space=pl.ANY)
    dma = pltpu.SemaphoreType.DMA
    bf16 = jnp.bfloat16
    f32 = jnp.float32
    block = VMEM((2, stretch, hd), bf16)
    stat = VMEM((3, tiles, 1, wide), f32)
    return pl.pallas_call(
        functools.partial(attend_kernel, n, nz, heads, chunk),
        out_shape=(
            jax.ShapeDtypeStruct((ranks, model // n), f32),
            jax.ShapeDtypeStruct(up_shape, f32),
            jax.ShapeDtypeStruct((2, quarter, hd), f32),
        ),
        in_specs=[anywhere] * 9,
        out_specs=(anywhere,) * 3,
        scratch_shapes=[
            pltpu.SMEM(lengths.shape, jnp.int32),
            VMEM(down_w.shape, bf16),
            VMEM(up_w.shape, bf16),
            VMEM((adapt_n, 1, row_n), jnp.int32),
            VMEM((ranks, model // n), f32),
            VMEM(up_shape, f32),
            VMEM((2, quarter, hd), f32),
            VMEM((adapt_n, row_n, rank), bf16),
            VMEM((tiles, wide, hd), bf16),
            VMEM((4, 2, stretch, hd), bf16),
            VMEM(hidden.shape, bf16),
            VMEM(base.shape, bf16),
            VMEM(grad.shape, bf16),
            VMEM((tiles, wide, 2 * hd), bf16),
            VMEM((tiles, hd, wide), bf16),
            VMEM((tiles, hd, wide), bf16),
            VMEM((4, stretch, hd), bf16),
            VMEM((4, stretch, hd), bf16),
            VMEM((hd, 4 * stretch), bf16),
            VMEM((tiles, 3 * stretch, wide), f32),
            VMEM((tiles, 3 * stretch, wide), f32),
            stat, stat, stat, stat,
            VMEM((tiles, 1, wide), f32),
            VMEM((tiles, 1, wide), jnp.int32),
            VMEM((stretch, hd), f32),
            VMEM((tiles, hd, wide), f32),
            dma((9,)), dma((4,)), dma((3, 2)), dma((4, 2)),
            VMEM((2,) + down_shape, bf16),
            VMEM(up_shape, bf16),
            block, block, block, block, block, block,
            VMEM((nz - 1, 2, quarter, hd), bf16),
            VMEM(down_shape, bf16),
            VMEM(down_shape, bf16),
            VMEM((n // 2 - 1,) + down_shape[1:], bf16),
            VMEM(up_shape[1:], bf16),
            VMEM((n // 2,) + up_shape[1:], bf16),
            dma((2, 2)), dma((2, 2)), dma((2, 2)), dma((2, 2)), dma((nz - 1, 2)), dma((nz - 1, 2)),
            dma((n // 2 - 1,)), dma((n // 2 - 1,)), dma((n // 2 - 1,)), dma((n // 2 - 1,)), dma((3,)), dma((3,)),
        ],
        compiler_params=pltpu.CompilerParams(
            collective_id=0, has_side_effects=True, vmem_limit_bytes=60 * 1024 * 1024
        ),
        name="gradients",
    )(lengths, hidden, base, grad, down_w, up_w, offsets[:, None, :], keys, values)


def finish_kernel(down_hbm, up_hbm, prompt_hbm, down_out, up_out, key_out, value_out, down, up, sems):
    adapt_n, rank, _ = down_out.shape
    half = up.shape[2]
    pairs = ((up_hbm, up), (down_hbm, down), (prompt_hbm.at[0], key_out), (prompt_hbm.at[1], value_out))
    loads = [pltpu.make_async_copy(a, b, sems.at[i]) for i, (a, b) in enumerate(pairs)]
    for c in loads:
        c.start()
    for c in loads:
        c.wait()
    for a in range(adapt_n):
        down_out[a] = adapter_scale * down[a * rank : (a + 1) * rank, :]
        for j in range(2):
            up_out[a, :, j * half : (j + 1) * half] = adapter_scale * up[j, a * rank : (a + 1) * rank, :]


def finish(up_w, down, up, prompt):
    adapt_n, rank, feature_n = up_w.shape
    f32 = jnp.float32
    spec = pl.BlockSpec(memory_space=VMEM)
    side = jax.ShapeDtypeStruct(prompt.shape[1:], f32)
    return pl.pallas_call(
        finish_kernel,
        out_shape=(
            jax.ShapeDtypeStruct((adapt_n, rank, down.shape[1]), f32),
            jax.ShapeDtypeStruct(up_w.shape, f32),
            side,
            side,
        ),
        in_specs=[pl.BlockSpec(memory_space=pl.ANY)] * 3,
        out_specs=(spec,) * 4,
        scratch_shapes=[VMEM(down.shape, f32), VMEM(up.shape, f32), pltpu.SemaphoreType.DMA((4,))],
        name="finish",
    )(down, up, prompt)


def local(
    hidden,
    response_base_queries,
    attention_output_gradient,
    keys,
    values,
    adapter_down_weight,
    adapter_up_weight,
    lengths,
    offsets,
):
    n = lax.axis_size("seq")
    nz = lax.axis_size("adapter")
    sums = gradients(
        n,
        nz,
        hidden,
        response_base_queries,
        attention_output_gradient,
        adapter_down_weight,
        adapter_up_weight,
        lengths,
        offsets,
        keys,
        values,
    )
    return finish(adapter_up_weight, *sums)


def solution(mesh):
    return jax.shard_map(
        local,
        mesh=mesh,
        in_specs=(
            P("adapter", "seq", None),
            P("adapter", "seq", None),
            P("adapter", "seq", None),
            P("seq", None),
            P("seq", None),
            P("adapter", None, None),
            P("adapter", None, None),
            P("adapter"),
            P("adapter", "seq"),
        ),
        out_specs=(
            P("adapter", None, "seq"),
            P("adapter", None, None),
            P(("seq", "adapter"), None),
            P(("seq", "adapter"), None),
        ),
        check_vma=False,
    )
```

```python
import functools
import math

import jax
import jax.numpy as jnp
from jax import lax
from jax.experimental import pallas as pl
from jax.experimental.pallas import tpu as pltpu
from jax.sharding import PartitionSpec as P

adapter_scale = 2.0
at_once = 2
masked_score = -1e30
MESH = pl.DeviceIdType.MESH
VMEM = pltpu.VMEM


def to_seq(index):
    return dict(device_id={"seq": index}, device_id_type=MESH)


def to_adapter(index):
    return dict(device_id={"adapter": index}, device_id_type=MESH)


def remote(src, dst, send_sem, recv_sem, target):
    return pltpu.make_async_remote_copy(
        src_ref=src, dst_ref=dst, send_sem=send_sem, recv_sem=recv_sem, **target
    )


def dot(a, b, dims):
    return lax.dot_general(a, b, (dims, ((), ())), preferred_element_type=jnp.float32)


def attend_kernel(
    n, nz, heads, chunk,
    len_hbm, hidden_hbm, base_hbm, grad_hbm, down_hbm, up_hbm, offset_hbm, keys_hbm, values_hbm,
    down_result, up_result, prompt_result,
    len_ref, down_w, up_w, offset_ref, down_out, up_out, prompt_out, low_ref, dq_ref, part, hidden, base, grad, gq_all, g_turned, q_turned, k_all, v_all, kt, s_ref, dp_ref, peaks, totals, inners,
    weight, delta, place_ref, acc, dq_acc, load_sem, out_sem, send_sem, recv_sem,
    down, up, pair_a, pair_b, back_two, back_three, summed, total, z_in, down_pair, down_chip, down_in,
    up_pair, up_all, pair_send, pair_recv, back_send, back_recv, z_send, z_recv, d_send, d_recv, u_send, u_recv,
    swap_send, swap_recv,
):
    s = lax.axis_index("seq")
    z = lax.axis_index("adapter")
    barrier = pltpu.get_barrier_semaphore()
    for i in range(1, n):
        pl.semaphore_signal(barrier, inc=1, **to_seq((s + i) % n))
    for i in range(1, nz):
        pl.semaphore_signal(barrier, inc=1, **to_adapter((z + i) % nz))
    core = s % 2
    partner = s + 1 - 2 * core
    adapt_n, rows, _ = base.shape
    _, stretch, hd = k_all.shape
    tiles, wide, _ = gq_all.shape
    per = tiles // adapt_n
    factor = hd**-0.5
    slope = factor * math.log2(math.e)
    pieces = stretch // chunk
    pairs = (
        (down_hbm, down_w), (hidden_hbm, hidden), (len_hbm, len_ref), (offset_hbm, offset_ref), (up_hbm, up_w),
        (base_hbm, base), (grad_hbm, grad), (keys_hbm, k_all.at[0]), (values_hbm, v_all.at[0]),
    )
    loads = [pltpu.make_async_copy(a, b, load_sem.at[i]) for i, (a, b) in enumerate(pairs)]
    for c in loads:
        c.start()
    full = (k_all, v_all)
    own = (keys_hbm, values_hbm)

    def copy(i, src, slot, which, target):
        return remote(src, full[i].at[slot], send_sem.at[which, i], recv_sem.at[slot, i], to_seq(target))

    two_on = [copy(i, own[i], 2, 0, s + 2) for i in range(2)]
    three_on = [copy(i, own[i], 3, 1, s + 3) for i in range(2)]
    next_on = [copy(i, own[i], 1, 1, s + 1) for i in range(2)]
    hand_up = [copy(i, full[i].at[2], 3, 2, s + 1) for i in range(2)]
    hand_down = [copy(i, full[i].at[2], 1, 2, s - 1) for i in range(2)]

    def arrived(slot, i):
        @pl.when(s >= slot)
        def _():
            remote(
                full[i].at[slot], full[i].at[slot], send_sem.at[0, i], recv_sem.at[slot, i], to_seq(partner)
            ).wait_recv()

    has_three_in = (core == 1) & (s + 3 < n)
    pl.semaphore_wait(barrier, n - 1 + nz - 1)

    has_two_on = s + 2 < n
    has_three_on = (core == 1) & (s + 3 < n)
    for i in range(2):

        @pl.when(has_two_on)
        def _():
            two_on[i].start()

        @pl.when(has_three_on)
        def _():
            three_on[i].start()

        @pl.when(core == 0)
        def _():
            next_on[i].start()

    @pl.when(s + 2 >= n)
    def _():
        back_two[...] = jnp.zeros_like(back_two)

    @pl.when(jnp.logical_not(has_three_in))
    def _():
        back_three[...] = jnp.zeros_like(back_three)

    @pl.when(core == 1)
    def _():
        pair_b[...] = jnp.zeros_like(pair_b)

    for slot in (1, 2, 3):

        @pl.when(s < slot)
        def _():
            k_all[slot] = jnp.zeros(k_all.shape[1:], k_all.dtype)
            v_all[slot] = jnp.zeros(v_all.shape[1:], v_all.dtype)

    for c in loads:
        c.wait()
    for a in range(adapt_n):
        low = dot(hidden[a], down_w[a], ((1,), (1,))).astype(jnp.bfloat16)
        low_ref[a] = low
        place = jnp.concatenate([offset_ref[a]] * heads, axis=1) - s * stretch
        for t in range(per):
            place_ref[a * per + t] = place
        raised = dot(low, up_w[a], ((1,), (0,)))
        query = (base[a].astype(jnp.float32) + adapter_scale * raised).astype(jnp.bfloat16)
        live = s * rows + lax.broadcasted_iota(jnp.int32, (rows, 1), 0) < len_ref[a]
        g = jnp.where(live, grad[a], jnp.zeros_like(grad[a]))
        for h in range(per * heads):
            t, at_row = a * per + h // heads, (h % heads) * rows
            gq_all[t, at_row : at_row + rows, :hd] = g[:, h * hd : (h + 1) * hd]
            gq_all[t, at_row : at_row + rows, hd:] = query[:, h * hd : (h + 1) * hd]
            g_turned[t, :, at_row : at_row + rows] = g[:, h * hd : (h + 1) * hd].T
            q_turned[t, :, at_row : at_row + rows] = query[:, h * hd : (h + 1) * hd].T

    def hand(i):
        @pl.when(s >= 2)
        def _():
            @pl.when(core == 0)
            def _():
                hand_up[i].start()

            @pl.when(core == 1)
            def _():
                hand_down[i].start()

    def at(piece):
        return slice(piece * chunk, (piece + 1) * chunk)

    def each(first, last):
        step = at_once if (last - first) % at_once == 0 else 1

        def run(body):
            if last - first == step:
                for j in range(first, last):
                    body(j)
                return

            @pl.loop(first, last, step=step)
            def _(t):
                for j in range(step):
                    body(t + j)

        return run

    def before(piece, place):
        pos = piece * chunk + lax.broadcasted_iota(jnp.int32, (chunk, wide), 0)
        return pos <= place

    spots = {0: 0, 3: 1, 1: 2, 2: 3}

    def turned(d):
        kt[:, spots[d] * stretch : (spots[d] + 1) * stretch] = k_all[d].T

    def product(source, d, piece, other):
        return dot(source[d, at(piece), :], other, ((1,), (0,)))

    far_bias = jnp.where(s >= 3, 0.0, masked_score)

    @each(0, tiles)
    def _(t):
        q = q_turned[t]
        g = g_turned[t]
        for piece in range(pieces):
            s_ref[t, at(piece), :] = product(k_all, 0, piece, q)
            dp_ref[t, at(piece), :] = product(v_all, 0, piece, g)

    def scores_of(d):
        @each(0, tiles)
        def _(t):
            q = q_turned[t]
            peak = jnp.full((1, wide), masked_score, jnp.float32)
            for piece in range(pieces):
                score = product(k_all, d or 3, piece, q)
                if d == 0:
                    near = before(piece, place_ref[t])
                    score = jnp.where(near, s_ref[t, at(piece), :], score + far_bias)
                s_ref[t, at(d * pieces + piece), :] = score
                peak = jnp.maximum(peak, jnp.max(score, axis=0, keepdims=True))
            peaks[d, t] = peak

    def raise_of(d):
        @each(0, tiles)
        def _(t):
            g = g_turned[t]
            peak = peaks[d, t]
            total = jnp.zeros((1, wide), jnp.float32)
            inner = jnp.zeros((1, wide), jnp.float32)
            for piece in range(pieces):
                spot = at(d * pieces + piece)
                e = jnp.exp2((s_ref[t, spot, :] - peak) * slope)
                dp = product(v_all, d or 3, piece, g)
                if d == 0:
                    dp = jnp.where(before(piece, place_ref[t]), dp_ref[t, spot, :], dp)
                s_ref[t, spot, :] = e
                dp_ref[t, spot, :] = dp
                total = total + jnp.sum(e, axis=0, keepdims=True)
                inner = inner + jnp.sum(e * dp, axis=0, keepdims=True)
            totals[d, t] = total
            inners[d, t] = inner

    arrived(2, 0)
    hand(0)
    turned(2)
    scores_of(2)
    arrived(1, 0)
    turned(1)
    scores_of(1)
    arrived(2, 1)
    hand(1)
    raise_of(2)
    arrived(1, 1)
    raise_of(1)
    arrived(3, 0)
    turned(3)
    turned(0)
    scores_of(0)
    arrived(3, 1)
    raise_of(0)

    @each(0, tiles)
    def _(t):
        tops = [peaks[0, t]] + [jnp.where(s >= d, peaks[d, t], masked_score) for d in (1, 2)]
        peak = jnp.maximum(jnp.maximum(tops[0], tops[1]), tops[2])
        shares = [jnp.exp2((top - peak) * slope) for top in tops]
        total = jnp.zeros((1, wide), jnp.float32)
        inner = jnp.zeros((1, wide), jnp.float32)
        for d, share in enumerate(shares):
            total = total + totals[d, t] * share
            inner = inner + inners[d, t] * share
        inverse = 1.0 / total
        for d, share in enumerate(shares):
            weight[d, t] = share * inverse
        delta[t] = inner * inverse

    def rows_of(unit, piece):
        if isinstance(unit, int):
            return at(unit * pieces + piece)
        return pl.ds(pl.multiple_of(unit * stretch + piece * chunk, chunk), chunk)

    def gather_up(block, i, first=0, last=tiles):
        static = isinstance(block, int)
        unit = 0 if static else block
        if first == 0:
            acc[...] = jnp.zeros_like(acc)

        @each(first, last)
        def _(t):
            other = gq_all[t]
            share = weight[unit, t]
            lows = []
            for piece in range(pieces):
                spot = rows_of(unit, piece)
                if i == 0 and static and block == 0:
                    value = dp_ref[t, spot, :]
                else:
                    value = s_ref[t, spot, :] * share
                    if i == 0:
                        value = value * (dp_ref[t, spot, :] - delta[t])
                    if i == 0 and static:
                        dp_ref[t, spot, :] = value
                if static:
                    near = before(piece, place_ref[t])
                    value = jnp.where(near, 0.0, value) if block else jnp.where(near, value, 0.0)
                low = value.astype(jnp.bfloat16)
                both = dot(low, other, ((1,), (0,)))
                acc[at(piece), :] += both[:, :hd] if i else both[:, hd:]
                lows.append(low)
            if i == 0:
                if static:
                    turned_block = kt[:, spots[block] * stretch : (spots[block] + 1) * stretch]
                else:
                    turned_block = kt[:, pl.ds(pl.multiple_of((block + 1) * stretch, stretch), stretch)]
                dq = dot(turned_block, jnp.concatenate(lows, axis=0), ((1,), (0,)))
                if static and block == 3:
                    dq_acc[t] = dq
                else:
                    dq_acc[t] += dq

        if last == tiles:
            out = acc[...]
            part[block, i] = (out if i else out * factor).astype(jnp.bfloat16)

    quarter = prompt_out.shape[1]
    has_far = (core == 0) & (s >= 3)

    def pair_copy(d, to, i, j):
        return remote(part.at[d, i], to.at[i], pair_send.at[j, i], pair_recv.at[j, i], to_seq(partner))

    zero_to_one = [pair_copy(1, pair_a, i, 0) for i in range(2)]
    one_to_zero = [pair_copy(3, pair_a, i, 0) for i in range(2)]
    near_back = [pair_copy(1, pair_b, i, 1) for i in range(2)]
    far_back = [
        remote(part.at[3, i], back_three.at[i], back_send.at[1, i], back_recv.at[1, i], to_seq(s - 3))
        for i in range(2)
    ]
    two_back = [
        remote(summed.at[i], back_two.at[i], back_send.at[0, i], back_recv.at[0, i], to_seq(s - 2))
        for i in range(2)
    ]
    chips = n // 2
    chip = s // 2
    down_swap = remote(down.at[1 - core], down_pair, swap_send.at[0], swap_recv.at[0], to_seq(partner))
    up_swap = remote(up.at[1 - core], up_pair, swap_send.at[1], swap_recv.at[1], to_seq(partner))
    up_back = remote(up_out.at[core], up_out.at[core], swap_send.at[2], swap_recv.at[2], to_seq(partner))
    downs, ups = [], []
    for i in range(1, chips):
        peer = (chip + i) % chips
        target = to_seq(2 * peer + core)
        downs.append(remote(down_chip.at[peer], down_in.at[i - 1], d_send.at[i - 1], d_recv.at[i - 1], target))
        ups.append(remote(up_all.at[chip], up_all.at[chip], u_send.at[i - 1], u_recv.at[i - 1], target))

    def sum_pair(i):
        zero_to_one[i].wait_recv()
        summed[i] = (part[2, i].astype(jnp.float32) + pair_a[i].astype(jnp.float32)).astype(jnp.bfloat16)

        @pl.when(s >= 2)
        def _():
            two_back[i].start()

    spread = [[], []]

    def owner(i):
        @pl.when(core == 0)
        def _():
            near_back[i].wait_recv()

        @pl.when(s + 2 < n)
        def _():
            two_back[i].wait_recv()

        @pl.when(has_three_in)
        def _():
            far_back[i].wait_recv()

        total[i] = (
            part[0, i].astype(jnp.float32)
            + pair_b[i].astype(jnp.float32)
            + back_two[i].astype(jnp.float32)
            + back_three[i].astype(jnp.float32)
        ).astype(jnp.bfloat16)
        for j in range(1, nz):
            peer = (z + j) % nz
            c = remote(
                total.at[i, pl.ds(pl.multiple_of(peer * quarter, 16), quarter), :],
                z_in.at[j - 1, i], z_send.at[j - 1, i], z_recv.at[j - 1, i], to_adapter(peer),
            )
            c.start()
            spread[i].append(c)

    def prompt_sum(i):
        mine = total[i, pl.ds(pl.multiple_of(z * quarter, 16), quarter), :].astype(jnp.float32)
        for j, c in enumerate(spread[i]):
            c.wait_recv()
            mine = mine + z_in[j, i].astype(jnp.float32)
        prompt_out[i] = mine

    def far_out(i):
        @pl.when(core == 1)
        def _():
            one_to_zero[i].start()

        @pl.when(has_far)
        def _():
            far_back[i].start()

    def sum_on(which, i):
        @pl.when(core == which)
        def _():
            sum_pair(i)

    second = 1 + core
    third = 2 - core
    middle = tiles // 2

    def second_out(i):
        gather_up(second, i)

        @pl.when(core == 0)
        def _():
            zero_to_one[i].start()

    def third_out(i):
        gather_up(third, i, 0, middle)
        sum_on(1, i)
        gather_up(third, i, middle, tiles)
        sum_on(0, i)

        @pl.when(core == 1)
        def _():
            near_back[i].start()

    gather_up(3, 1)
    far_out(1)
    second_out(1)
    third_out(1)
    gather_up(3, 0)
    far_out(0)
    gather_up(0, 1)
    second_out(0)
    owner(1)
    third_out(0)
    gather_up(0, 0)

    @each(0, tiles)
    def _(t):
        dq_ref[t] = (dq_acc[t] * factor).T.astype(jnp.bfloat16)

    _, rank, feature_n = up_w.shape
    group = feature_n // hd
    half = feature_n // 2
    width = down_out.shape[1]
    smalls = []
    for a in range(adapt_n):
        small = jnp.zeros((rows, rank), jnp.float32)
        for h in range(group):
            place = a * group + h
            dq_h = dq_ref[place // heads, (place % heads) * rows : (place % heads + 1) * rows, :]
            up_h = dot(low_ref[a], dq_h, ((0,), (0,)))
            begin = h * hd % half
            up[h * hd // half, a * rank : (a + 1) * rank, begin : begin + hd] = up_h.astype(jnp.bfloat16)
            small = small + dot(dq_h, up_w[a, :, h * hd : (h + 1) * hd], ((1,), (1,)))
        smalls.append(small.astype(jnp.bfloat16))
    up_swap.start()
    for a in range(adapt_n):
        out = dot(smalls[a], hidden[a], ((0,), (0,))).astype(jnp.bfloat16)
        for j in range(n):
            down[j % 2, j // 2, a * rank : (a + 1) * rank, :] = out[:, j * width : (j + 1) * width]
    down_swap.start()
    up_swap.wait_recv()
    up_all[chip] = (up[core].astype(jnp.float32) + up_pair[...].astype(jnp.float32)).astype(jnp.bfloat16)
    for c in ups:
        c.start()
    owner(0)
    down_swap.wait_recv()
    for j in range(chips):
        both = down[core, j].astype(jnp.float32) + down_pair[j].astype(jnp.float32)
        down_chip[j] = both.astype(jnp.bfloat16)
    for c in downs:
        c.start()
    for c in ups:
        c.wait_recv()
    mine = up_all[0].astype(jnp.float32)
    for j in range(1, chips):
        mine = mine + up_all[j].astype(jnp.float32)
    up_out[core] = mine
    up_back.start()
    mine = down[core, chip].astype(jnp.float32) + down_pair[chip].astype(jnp.float32)
    for i, c in enumerate(downs):
        c.wait_recv()
        mine = mine + down_in[i].astype(jnp.float32)
    down_out[...] = mine
    results = [
        pltpu.make_async_copy(down_out, down_result, out_sem.at[0]),
        pltpu.make_async_copy(up_out, up_result, out_sem.at[1]),
        pltpu.make_async_copy(prompt_out.at[0], prompt_result.at[0], out_sem.at[2]),
        pltpu.make_async_copy(prompt_out.at[1], prompt_result.at[1], out_sem.at[3]),
    ]
    results[0].start()
    prompt_sum(1)
    results[3].start()
    prompt_sum(0)
    results[2].start()
    up_back.wait_recv()
    results[1].start()
    for c in results:
        c.wait()
    for c in downs + ups + spread[0] + spread[1] + zero_to_one + [up_swap, down_swap, up_back]:
        c.wait_send()
    for i in range(2):

        @pl.when(core == 1)
        def _():
            near_back[i].wait_send()

        @pl.when(has_far)
        def _():
            far_back[i].wait_send()

        @pl.when(s >= 2)
        def _():
            two_back[i].wait_send()

    for i in range(2):

        @pl.when(has_two_on)
        def _():
            two_on[i].wait_send()

        @pl.when(has_three_on)
        def _():
            three_on[i].wait_send()

        @pl.when(core == 0)
        def _():
            next_on[i].wait_send()

        @pl.when(s >= 2)
        def _():
            hand_up[i].wait_send()


def gradients(n, nz, hidden, base, grad, down_w, up_w, lengths, offsets, keys, values):
    adapt_n, row_n, feature_n = base.shape
    stretch, hd = keys.shape
    rank, model = down_w.shape[1:]
    ranks = adapt_n * rank
    heads = 4
    wide = heads * row_n
    tiles = adapt_n * feature_n // (hd * heads)
    chunk = stretch
    quarter = stretch // nz
    up_shape = (2, ranks, feature_n // 2)
    down_shape = (n // 2, ranks, model // n)
    anywhere = pl.BlockSpec(memory_space=pl.ANY)
    dma = pltpu.SemaphoreType.DMA
    bf16 = jnp.bfloat16
    f32 = jnp.float32
    block = VMEM((2, stretch, hd), bf16)
    stat = VMEM((3, tiles, 1, wide), f32)
    return pl.pallas_call(
        functools.partial(attend_kernel, n, nz, heads, chunk),
        out_shape=(
            jax.ShapeDtypeStruct((ranks, model // n), f32),
            jax.ShapeDtypeStruct(up_shape, f32),
            jax.ShapeDtypeStruct((2, quarter, hd), f32),
        ),
        in_specs=[anywhere] * 9,
        out_specs=(anywhere,) * 3,
        scratch_shapes=[
            pltpu.SMEM(lengths.shape, jnp.int32),
            VMEM(down_w.shape, bf16),
            VMEM(up_w.shape, bf16),
            VMEM((adapt_n, 1, row_n), jnp.int32),
            VMEM((ranks, model // n), f32),
            VMEM(up_shape, f32),
            VMEM((2, quarter, hd), f32),
            VMEM((adapt_n, row_n, rank), bf16),
            VMEM((tiles, wide, hd), bf16),
            VMEM((4, 2, stretch, hd), bf16),
            VMEM(hidden.shape, bf16),
            VMEM(base.shape, bf16),
            VMEM(grad.shape, bf16),
            VMEM((tiles, wide, 2 * hd), bf16),
            VMEM((tiles, hd, wide), bf16),
            VMEM((tiles, hd, wide), bf16),
            VMEM((4, stretch, hd), bf16),
            VMEM((4, stretch, hd), bf16),
            VMEM((hd, 4 * stretch), bf16),
            VMEM((tiles, 3 * stretch, wide), f32),
            VMEM((tiles, 3 * stretch, wide), f32),
            stat, stat, stat, stat,
            VMEM((tiles, 1, wide), f32),
            VMEM((tiles, 1, wide), jnp.int32),
            VMEM((stretch, hd), f32),
            VMEM((tiles, hd, wide), f32),
            dma((9,)), dma((4,)), dma((3, 2)), dma((4, 2)),
            VMEM((2,) + down_shape, bf16),
            VMEM(up_shape, bf16),
            block, block, block, block, block, block,
            VMEM((nz - 1, 2, quarter, hd), bf16),
            VMEM(down_shape, bf16),
            VMEM(down_shape, bf16),
            VMEM((n // 2 - 1,) + down_shape[1:], bf16),
            VMEM(up_shape[1:], bf16),
            VMEM((n // 2,) + up_shape[1:], bf16),
            dma((2, 2)), dma((2, 2)), dma((2, 2)), dma((2, 2)), dma((nz - 1, 2)), dma((nz - 1, 2)),
            dma((n // 2 - 1,)), dma((n // 2 - 1,)), dma((n // 2 - 1,)), dma((n // 2 - 1,)), dma((3,)), dma((3,)),
        ],
        compiler_params=pltpu.CompilerParams(
            collective_id=0, has_side_effects=True, vmem_limit_bytes=60 * 1024 * 1024
        ),
        name="gradients",
    )(lengths, hidden, base, grad, down_w, up_w, offsets[:, None, :], keys, values)


def finish_kernel(down_hbm, up_hbm, prompt_hbm, down_out, up_out, key_out, value_out, down, up, sems):
    adapt_n, rank, _ = down_out.shape
    half = up.shape[2]
    pairs = ((up_hbm, up), (down_hbm, down), (prompt_hbm.at[0], key_out), (prompt_hbm.at[1], value_out))
    loads = [pltpu.make_async_copy(a, b, sems.at[i]) for i, (a, b) in enumerate(pairs)]
    for c in loads:
        c.start()
    for c in loads:
        c.wait()
    for a in range(adapt_n):
        down_out[a] = adapter_scale * down[a * rank : (a + 1) * rank, :]
        for j in range(2):
            up_out[a, :, j * half : (j + 1) * half] = adapter_scale * up[j, a * rank : (a + 1) * rank, :]


def finish(up_w, down, up, prompt):
    adapt_n, rank, feature_n = up_w.shape
    f32 = jnp.float32
    spec = pl.BlockSpec(memory_space=VMEM)
    side = jax.ShapeDtypeStruct(prompt.shape[1:], f32)
    return pl.pallas_call(
        finish_kernel,
        out_shape=(
            jax.ShapeDtypeStruct((adapt_n, rank, down.shape[1]), f32),
            jax.ShapeDtypeStruct(up_w.shape, f32),
            side,
            side,
        ),
        in_specs=[pl.BlockSpec(memory_space=pl.ANY)] * 3,
        out_specs=(spec,) * 4,
        scratch_shapes=[VMEM(down.shape, f32), VMEM(up.shape, f32), pltpu.SemaphoreType.DMA((4,))],
        name="finish",
    )(down, up, prompt)


def local(
    hidden,
    response_base_queries,
    attention_output_gradient,
    keys,
    values,
    adapter_down_weight,
    adapter_up_weight,
    lengths,
    offsets,
):
    n = lax.axis_size("seq")
    nz = lax.axis_size("adapter")
    sums = gradients(
        n,
        nz,
        hidden,
        response_base_queries,
        attention_output_gradient,
        adapter_down_weight,
        adapter_up_weight,
        lengths,
        offsets,
        keys,
        values,
    )
    return finish(adapter_up_weight, *sums)


def solution(mesh):
    return jax.shard_map(
        local,
        mesh=mesh,
        in_specs=(
            P("adapter", "seq", None),
            P("adapter", "seq", None),
            P("adapter", "seq", None),
            P("seq", None),
            P("seq", None),
            P("adapter", None, None),
            P("adapter", None, None),
            P("adapter"),
            P("adapter", "seq"),
        ),
        out_specs=(
            P("adapter", None, "seq"),
            P("adapter", None, None),
            P(("seq", "adapter"), None),
            P(("seq", "adapter"), None),
        ),
        check_vma=False,
    )
```

```python
import functools
import math

import jax
import jax.numpy as jnp
from jax import lax
from jax.experimental import pallas as pl
from jax.experimental.pallas import tpu as pltpu
from jax.sharding import PartitionSpec as P

adapter_scale = 2.0
at_once = 2
masked_score = -1e30
MESH = pl.DeviceIdType.MESH
VMEM = pltpu.VMEM


def to_seq(index):
    return dict(device_id={"seq": index}, device_id_type=MESH)


def to_adapter(index):
    return dict(device_id={"adapter": index}, device_id_type=MESH)


def remote(src, dst, send_sem, recv_sem, target):
    return pltpu.make_async_remote_copy(
        src_ref=src, dst_ref=dst, send_sem=send_sem, recv_sem=recv_sem, **target
    )


def dot(a, b, dims):
    return lax.dot_general(a, b, (dims, ((), ())), preferred_element_type=jnp.float32)


def attend_kernel(
    n, nz, heads, chunk,
    len_hbm, hidden_hbm, base_hbm, grad_hbm, down_hbm, up_hbm, offset_hbm, keys_hbm, values_hbm,
    down_result, up_result, prompt_result,
    len_ref, down_w, up_w, offset_ref, down_out, up_out, prompt_out, low_ref, dq_ref, part, hidden, base, grad, gq_all, g_turned, q_turned, k_all, v_all, kt, s_ref, dp_ref, peaks, totals, inners,
    weight, delta, place_ref, acc, dq_acc, load_sem, out_sem, send_sem, recv_sem,
    down, up, pair_a, pair_b, back_two, back_three, summed, total, z_in, down_pair, down_chip, down_in,
    up_pair, up_all, pair_send, pair_recv, back_send, back_recv, z_send, z_recv, d_send, d_recv, u_send, u_recv,
    swap_send, swap_recv,
):
    s = lax.axis_index("seq")
    z = lax.axis_index("adapter")
    barrier = pltpu.get_barrier_semaphore()
    for i in range(1, n):
        pl.semaphore_signal(barrier, inc=1, **to_seq((s + i) % n))
    for i in range(1, nz):
        pl.semaphore_signal(barrier, inc=1, **to_adapter((z + i) % nz))
    core = s % 2
    partner = s + 1 - 2 * core
    adapt_n, rows, _ = base.shape
    _, stretch, hd = k_all.shape
    tiles, wide, _ = gq_all.shape
    per = tiles // adapt_n
    factor = hd**-0.5
    slope = factor * math.log2(math.e)
    pieces = stretch // chunk
    pairs = (
        (down_hbm, down_w), (hidden_hbm, hidden), (len_hbm, len_ref), (offset_hbm, offset_ref), (up_hbm, up_w),
        (base_hbm, base), (grad_hbm, grad), (keys_hbm, k_all.at[0]), (values_hbm, v_all.at[0]),
    )
    loads = [pltpu.make_async_copy(a, b, load_sem.at[i]) for i, (a, b) in enumerate(pairs)]
    for c in loads:
        c.start()
    full = (k_all, v_all)
    own = (keys_hbm, values_hbm)

    def copy(i, src, slot, which, target):
        return remote(src, full[i].at[slot], send_sem.at[which, i], recv_sem.at[slot, i], to_seq(target))

    two_on = [copy(i, own[i], 2, 0, s + 2) for i in range(2)]
    three_on = [copy(i, own[i], 3, 1, s + 3) for i in range(2)]
    next_on = [copy(i, own[i], 1, 1, s + 1) for i in range(2)]
    hand_up = [copy(i, full[i].at[2], 3, 2, s + 1) for i in range(2)]
    hand_down = [copy(i, full[i].at[2], 1, 2, s - 1) for i in range(2)]

    def arrived(slot, i):
        @pl.when(s >= slot)
        def _():
            remote(
                full[i].at[slot], full[i].at[slot], send_sem.at[0, i], recv_sem.at[slot, i], to_seq(partner)
            ).wait_recv()

    has_three_in = (core == 1) & (s + 3 < n)
    pl.semaphore_wait(barrier, n - 1 + nz - 1)

    has_two_on = s + 2 < n
    has_three_on = (core == 1) & (s + 3 < n)
    for i in range(2):

        @pl.when(has_two_on)
        def _():
            two_on[i].start()

        @pl.when(has_three_on)
        def _():
            three_on[i].start()

        @pl.when(core == 0)
        def _():
            next_on[i].start()

    @pl.when(s + 2 >= n)
    def _():
        back_two[...] = jnp.zeros_like(back_two)

    @pl.when(jnp.logical_not(has_three_in))
    def _():
        back_three[...] = jnp.zeros_like(back_three)

    @pl.when(core == 1)
    def _():
        pair_b[...] = jnp.zeros_like(pair_b)

    for slot in (1, 2, 3):

        @pl.when(s < slot)
        def _():
            k_all[slot] = jnp.zeros(k_all.shape[1:], k_all.dtype)
            v_all[slot] = jnp.zeros(v_all.shape[1:], v_all.dtype)

    for c in loads:
        c.wait()
    for a in range(adapt_n):
        low = dot(hidden[a], down_w[a], ((1,), (1,))).astype(jnp.bfloat16)
        low_ref[a] = low
        place = jnp.concatenate([offset_ref[a]] * heads, axis=1) - s * stretch
        for t in range(per):
            place_ref[a * per + t] = place
        raised = dot(low, up_w[a], ((1,), (0,)))
        query = (base[a].astype(jnp.float32) + adapter_scale * raised).astype(jnp.bfloat16)
        live = s * rows + lax.broadcasted_iota(jnp.int32, (rows, 1), 0) < len_ref[a]
        g = jnp.where(live, grad[a], jnp.zeros_like(grad[a]))
        for h in range(per * heads):
            t, at_row = a * per + h // heads, (h % heads) * rows
            gq_all[t, at_row : at_row + rows, :hd] = g[:, h * hd : (h + 1) * hd]
            gq_all[t, at_row : at_row + rows, hd:] = query[:, h * hd : (h + 1) * hd]
            g_turned[t, :, at_row : at_row + rows] = g[:, h * hd : (h + 1) * hd].T
            q_turned[t, :, at_row : at_row + rows] = query[:, h * hd : (h + 1) * hd].T

    def hand(i):
        @pl.when(s >= 2)
        def _():
            @pl.when(core == 0)
            def _():
                hand_up[i].start()

            @pl.when(core == 1)
            def _():
                hand_down[i].start()

    def at(piece):
        return slice(piece * chunk, (piece + 1) * chunk)

    def each(first, last, most=at_once):
        step = math.gcd(most, last - first)

        def run(body):
            if last - first == step:
                for j in range(first, last):
                    body(j)
                return

            @pl.loop(first, last, step=step)
            def _(t):
                for j in range(step):
                    body(t + j)

        return run

    def before(piece, place):
        pos = piece * chunk + lax.broadcasted_iota(jnp.int32, (chunk, wide), 0)
        return pos <= place

    spots = {0: 0, 3: 1, 1: 2, 2: 3}

    def turned(d):
        kt[:, spots[d] * stretch : (spots[d] + 1) * stretch] = k_all[d].T

    def product(source, d, piece, other):
        return dot(source[d, at(piece), :], other, ((1,), (0,)))

    far_bias = jnp.where(s >= 3, 0.0, masked_score)

    @each(0, tiles, 4)
    def _(t):
        q = q_turned[t]
        g = g_turned[t]
        for piece in range(pieces):
            s_ref[t, at(piece), :] = product(k_all, 0, piece, q)
            dp_ref[t, at(piece), :] = product(v_all, 0, piece, g)

    def scores_of(d):
        @each(0, tiles, 4)
        def _(t):
            q = q_turned[t]
            peak = jnp.full((1, wide), masked_score, jnp.float32)
            for piece in range(pieces):
                score = product(k_all, d or 3, piece, q)
                if d == 0:
                    near = before(piece, place_ref[t])
                    score = jnp.where(near, s_ref[t, at(piece), :], score + far_bias)
                s_ref[t, at(d * pieces + piece), :] = score
                peak = jnp.maximum(peak, jnp.max(score, axis=0, keepdims=True))
            peaks[d, t] = peak

    def raise_of(d):
        @each(0, tiles, 4)
        def _(t):
            g = g_turned[t]
            peak = peaks[d, t]
            total = jnp.zeros((1, wide), jnp.float32)
            inner = jnp.zeros((1, wide), jnp.float32)
            for piece in range(pieces):
                spot = at(d * pieces + piece)
                e = jnp.exp2((s_ref[t, spot, :] - peak) * slope)
                dp = product(v_all, d or 3, piece, g)
                if d == 0:
                    dp = jnp.where(before(piece, place_ref[t]), dp_ref[t, spot, :], dp)
                s_ref[t, spot, :] = e
                dp_ref[t, spot, :] = dp
                total = total + jnp.sum(e, axis=0, keepdims=True)
                inner = inner + jnp.sum(e * dp, axis=0, keepdims=True)
            totals[d, t] = total
            inners[d, t] = inner

    arrived(2, 0)
    hand(0)
    turned(2)
    scores_of(2)
    arrived(1, 0)
    turned(1)
    scores_of(1)
    arrived(2, 1)
    hand(1)
    raise_of(2)
    arrived(1, 1)
    raise_of(1)
    arrived(3, 0)
    turned(3)
    turned(0)
    scores_of(0)
    arrived(3, 1)
    raise_of(0)

    @each(0, tiles, 4)
    def _(t):
        tops = [peaks[0, t]] + [jnp.where(s >= d, peaks[d, t], masked_score) for d in (1, 2)]
        peak = jnp.maximum(jnp.maximum(tops[0], tops[1]), tops[2])
        shares = [jnp.exp2((top - peak) * slope) for top in tops]
        total = jnp.zeros((1, wide), jnp.float32)
        inner = jnp.zeros((1, wide), jnp.float32)
        for d, share in enumerate(shares):
            total = total + totals[d, t] * share
            inner = inner + inners[d, t] * share
        inverse = 1.0 / total
        for d, share in enumerate(shares):
            weight[d, t] = share * inverse
        delta[t] = inner * inverse

    def rows_of(unit, piece):
        if isinstance(unit, int):
            return at(unit * pieces + piece)
        return pl.ds(pl.multiple_of(unit * stretch + piece * chunk, chunk), chunk)

    def gather_up(block, i, first=0, last=tiles):
        static = isinstance(block, int)
        unit = 0 if static else block
        if first == 0:
            acc[...] = jnp.zeros_like(acc)

        @each(first, last)
        def _(t):
            other = gq_all[t]
            share = weight[unit, t]
            lows = []
            for piece in range(pieces):
                spot = rows_of(unit, piece)
                if i == 0 and static and block == 0:
                    value = dp_ref[t, spot, :]
                else:
                    value = s_ref[t, spot, :] * share
                    if i == 0:
                        value = value * (dp_ref[t, spot, :] - delta[t])
                    if i == 0 and static:
                        dp_ref[t, spot, :] = value
                if static:
                    near = before(piece, place_ref[t])
                    value = jnp.where(near, 0.0, value) if block else jnp.where(near, value, 0.0)
                low = value.astype(jnp.bfloat16)
                both = dot(low, other, ((1,), (0,)))
                acc[at(piece), :] += both[:, :hd] if i else both[:, hd:]
                lows.append(low)
            if i == 0:
                if static:
                    turned_block = kt[:, spots[block] * stretch : (spots[block] + 1) * stretch]
                else:
                    turned_block = kt[:, pl.ds(pl.multiple_of((block + 1) * stretch, stretch), stretch)]
                dq = dot(turned_block, jnp.concatenate(lows, axis=0), ((1,), (0,)))
                if static and block == 3:
                    dq_acc[t] = dq
                else:
                    dq_acc[t] += dq

        if last == tiles:
            out = acc[...]
            part[block, i] = (out if i else out * factor).astype(jnp.bfloat16)

    quarter = prompt_out.shape[1]
    has_far = (core == 0) & (s >= 3)

    def pair_copy(d, to, i, j):
        return remote(part.at[d, i], to.at[i], pair_send.at[j, i], pair_recv.at[j, i], to_seq(partner))

    zero_to_one = [pair_copy(1, pair_a, i, 0) for i in range(2)]
    one_to_zero = [pair_copy(3, pair_a, i, 0) for i in range(2)]
    near_back = [pair_copy(1, pair_b, i, 1) for i in range(2)]
    far_back = [
        remote(part.at[3, i], back_three.at[i], back_send.at[1, i], back_recv.at[1, i], to_seq(s - 3))
        for i in range(2)
    ]
    two_back = [
        remote(summed.at[i], back_two.at[i], back_send.at[0, i], back_recv.at[0, i], to_seq(s - 2))
        for i in range(2)
    ]
    chips = n // 2
    chip = s // 2
    down_swap = remote(down.at[1 - core], down_pair, swap_send.at[0], swap_recv.at[0], to_seq(partner))
    up_swap = remote(up.at[1 - core], up_pair, swap_send.at[1], swap_recv.at[1], to_seq(partner))
    up_back = remote(up_out.at[core], up_out.at[core], swap_send.at[2], swap_recv.at[2], to_seq(partner))
    downs, ups = [], []
    for i in range(1, chips):
        peer = (chip + i) % chips
        target = to_seq(2 * peer + core)
        downs.append(remote(down_chip.at[peer], down_in.at[i - 1], d_send.at[i - 1], d_recv.at[i - 1], target))
        ups.append(remote(up_all.at[chip], up_all.at[chip], u_send.at[i - 1], u_recv.at[i - 1], target))

    def sum_pair(i):
        zero_to_one[i].wait_recv()
        summed[i] = (part[2, i].astype(jnp.float32) + pair_a[i].astype(jnp.float32)).astype(jnp.bfloat16)

        @pl.when(s >= 2)
        def _():
            two_back[i].start()

    spread = [[], []]

    def owner(i):
        @pl.when(core == 0)
        def _():
            near_back[i].wait_recv()

        @pl.when(s + 2 < n)
        def _():
            two_back[i].wait_recv()

        @pl.when(has_three_in)
        def _():
            far_back[i].wait_recv()

        total[i] = (
            part[0, i].astype(jnp.float32)
            + pair_b[i].astype(jnp.float32)
            + back_two[i].astype(jnp.float32)
            + back_three[i].astype(jnp.float32)
        ).astype(jnp.bfloat16)
        for j in range(1, nz):
            peer = (z + j) % nz
            c = remote(
                total.at[i, pl.ds(pl.multiple_of(peer * quarter, 16), quarter), :],
                z_in.at[j - 1, i], z_send.at[j - 1, i], z_recv.at[j - 1, i], to_adapter(peer),
            )
            c.start()
            spread[i].append(c)

    def prompt_sum(i):
        mine = total[i, pl.ds(pl.multiple_of(z * quarter, 16), quarter), :].astype(jnp.float32)
        for j, c in enumerate(spread[i]):
            c.wait_recv()
            mine = mine + z_in[j, i].astype(jnp.float32)
        prompt_out[i] = mine

    def far_out(i):
        @pl.when(core == 1)
        def _():
            one_to_zero[i].start()

        @pl.when(has_far)
        def _():
            far_back[i].start()

    def sum_on(which, i):
        @pl.when(core == which)
        def _():
            sum_pair(i)

    second = 1 + core
    third = 2 - core
    middle = tiles // 2

    def second_out(i):
        gather_up(second, i)

        @pl.when(core == 0)
        def _():
            zero_to_one[i].start()

    def third_out(i):
        gather_up(third, i, 0, middle)
        sum_on(1, i)
        gather_up(third, i, middle, tiles)
        sum_on(0, i)

        @pl.when(core == 1)
        def _():
            near_back[i].start()

    gather_up(3, 1)
    far_out(1)
    second_out(1)
    third_out(1)
    gather_up(3, 0)
    far_out(0)
    gather_up(0, 1)
    second_out(0)
    owner(1)
    third_out(0)
    gather_up(0, 0)

    @each(0, tiles)
    def _(t):
        dq_ref[t] = (dq_acc[t] * factor).T.astype(jnp.bfloat16)

    _, rank, feature_n = up_w.shape
    group = feature_n // hd
    half = feature_n // 2
    width = down_out.shape[1]
    smalls = []
    for a in range(adapt_n):
        small = jnp.zeros((rows, rank), jnp.float32)
        for h in range(group):
            place = a * group + h
            dq_h = dq_ref[place // heads, (place % heads) * rows : (place % heads + 1) * rows, :]
            up_h = dot(low_ref[a], dq_h, ((0,), (0,)))
            begin = h * hd % half
            up[h * hd // half, a * rank : (a + 1) * rank, begin : begin + hd] = up_h.astype(jnp.bfloat16)
            small = small + dot(dq_h, up_w[a, :, h * hd : (h + 1) * hd], ((1,), (1,)))
        smalls.append(small.astype(jnp.bfloat16))
    up_swap.start()
    for a in range(adapt_n):
        out = dot(smalls[a], hidden[a], ((0,), (0,))).astype(jnp.bfloat16)
        for j in range(n):
            down[j % 2, j // 2, a * rank : (a + 1) * rank, :] = out[:, j * width : (j + 1) * width]
    down_swap.start()
    up_swap.wait_recv()
    up_all[chip] = (up[core].astype(jnp.float32) + up_pair[...].astype(jnp.float32)).astype(jnp.bfloat16)
    for c in ups:
        c.start()
    owner(0)
    down_swap.wait_recv()
    for i, c in enumerate(downs):
        peer = (chip + i + 1) % chips
        both = down[core, peer].astype(jnp.float32) + down_pair[peer].astype(jnp.float32)
        down_chip[peer] = both.astype(jnp.bfloat16)
        c.start()
    for c in ups:
        c.wait_recv()
    mine = up_all[0].astype(jnp.float32)
    for j in range(1, chips):
        mine = mine + up_all[j].astype(jnp.float32)
    up_out[core] = mine
    up_back.start()
    mine = down[core, chip].astype(jnp.float32) + down_pair[chip].astype(jnp.float32)
    for i, c in enumerate(downs):
        c.wait_recv()
        mine = mine + down_in[i].astype(jnp.float32)
    down_out[...] = mine
    results = [
        pltpu.make_async_copy(down_out, down_result, out_sem.at[0]),
        pltpu.make_async_copy(up_out, up_result, out_sem.at[1]),
        pltpu.make_async_copy(prompt_out.at[0], prompt_result.at[0], out_sem.at[2]),
        pltpu.make_async_copy(prompt_out.at[1], prompt_result.at[1], out_sem.at[3]),
    ]
    results[0].start()
    prompt_sum(1)
    results[3].start()
    prompt_sum(0)
    results[2].start()
    up_back.wait_recv()
    results[1].start()
    for c in results:
        c.wait()
    for c in downs + ups + spread[0] + spread[1] + zero_to_one + [up_swap, down_swap, up_back]:
        c.wait_send()
    for i in range(2):

        @pl.when(core == 1)
        def _():
            near_back[i].wait_send()

        @pl.when(has_far)
        def _():
            far_back[i].wait_send()

        @pl.when(s >= 2)
        def _():
            two_back[i].wait_send()

    for i in range(2):

        @pl.when(has_two_on)
        def _():
            two_on[i].wait_send()

        @pl.when(has_three_on)
        def _():
            three_on[i].wait_send()

        @pl.when(core == 0)
        def _():
            next_on[i].wait_send()

        @pl.when(s >= 2)
        def _():
            hand_up[i].wait_send()


def gradients(n, nz, hidden, base, grad, down_w, up_w, lengths, offsets, keys, values):
    adapt_n, row_n, feature_n = base.shape
    stretch, hd = keys.shape
    rank, model = down_w.shape[1:]
    ranks = adapt_n * rank
    heads = 4
    wide = heads * row_n
    tiles = adapt_n * feature_n // (hd * heads)
    chunk = stretch
    quarter = stretch // nz
    up_shape = (2, ranks, feature_n // 2)
    down_shape = (n // 2, ranks, model // n)
    anywhere = pl.BlockSpec(memory_space=pl.ANY)
    dma = pltpu.SemaphoreType.DMA
    bf16 = jnp.bfloat16
    f32 = jnp.float32
    block = VMEM((2, stretch, hd), bf16)
    stat = VMEM((3, tiles, 1, wide), f32)
    return pl.pallas_call(
        functools.partial(attend_kernel, n, nz, heads, chunk),
        out_shape=(
            jax.ShapeDtypeStruct((ranks, model // n), f32),
            jax.ShapeDtypeStruct(up_shape, f32),
            jax.ShapeDtypeStruct((2, quarter, hd), f32),
        ),
        in_specs=[anywhere] * 9,
        out_specs=(anywhere,) * 3,
        scratch_shapes=[
            pltpu.SMEM(lengths.shape, jnp.int32),
            VMEM(down_w.shape, bf16),
            VMEM(up_w.shape, bf16),
            VMEM((adapt_n, 1, row_n), jnp.int32),
            VMEM((ranks, model // n), f32),
            VMEM(up_shape, f32),
            VMEM((2, quarter, hd), f32),
            VMEM((adapt_n, row_n, rank), bf16),
            VMEM((tiles, wide, hd), bf16),
            VMEM((4, 2, stretch, hd), bf16),
            VMEM(hidden.shape, bf16),
            VMEM(base.shape, bf16),
            VMEM(grad.shape, bf16),
            VMEM((tiles, wide, 2 * hd), bf16),
            VMEM((tiles, hd, wide), bf16),
            VMEM((tiles, hd, wide), bf16),
            VMEM((4, stretch, hd), bf16),
            VMEM((4, stretch, hd), bf16),
            VMEM((hd, 4 * stretch), bf16),
            VMEM((tiles, 3 * stretch, wide), f32),
            VMEM((tiles, 3 * stretch, wide), f32),
            stat, stat, stat, stat,
            VMEM((tiles, 1, wide), f32),
            VMEM((tiles, 1, wide), jnp.int32),
            VMEM((stretch, hd), f32),
            VMEM((tiles, hd, wide), f32),
            dma((9,)), dma((4,)), dma((3, 2)), dma((4, 2)),
            VMEM((2,) + down_shape, bf16),
            VMEM(up_shape, bf16),
            block, block, block, block, block, block,
            VMEM((nz - 1, 2, quarter, hd), bf16),
            VMEM(down_shape, bf16),
            VMEM(down_shape, bf16),
            VMEM((n // 2 - 1,) + down_shape[1:], bf16),
            VMEM(up_shape[1:], bf16),
            VMEM((n // 2,) + up_shape[1:], bf16),
            dma((2, 2)), dma((2, 2)), dma((2, 2)), dma((2, 2)), dma((nz - 1, 2)), dma((nz - 1, 2)),
            dma((n // 2 - 1,)), dma((n // 2 - 1,)), dma((n // 2 - 1,)), dma((n // 2 - 1,)), dma((3,)), dma((3,)),
        ],
        compiler_params=pltpu.CompilerParams(
            collective_id=0, has_side_effects=True, vmem_limit_bytes=60 * 1024 * 1024
        ),
        name="gradients",
    )(lengths, hidden, base, grad, down_w, up_w, offsets[:, None, :], keys, values)


def finish_kernel(down_hbm, up_hbm, prompt_hbm, down_out, up_out, key_out, value_out, down, up, sems):
    adapt_n, rank, _ = down_out.shape
    half = up.shape[2]
    pairs = ((up_hbm, up), (down_hbm, down), (prompt_hbm.at[0], key_out), (prompt_hbm.at[1], value_out))
    loads = [pltpu.make_async_copy(a, b, sems.at[i]) for i, (a, b) in enumerate(pairs)]
    for c in loads:
        c.start()
    for c in loads:
        c.wait()
    for a in range(adapt_n):
        down_out[a] = adapter_scale * down[a * rank : (a + 1) * rank, :]
        for j in range(2):
            up_out[a, :, j * half : (j + 1) * half] = adapter_scale * up[j, a * rank : (a + 1) * rank, :]


def finish(up_w, down, up, prompt):
    adapt_n, rank, feature_n = up_w.shape
    f32 = jnp.float32
    spec = pl.BlockSpec(memory_space=VMEM)
    side = jax.ShapeDtypeStruct(prompt.shape[1:], f32)
    return pl.pallas_call(
        finish_kernel,
        out_shape=(
            jax.ShapeDtypeStruct((adapt_n, rank, down.shape[1]), f32),
            jax.ShapeDtypeStruct(up_w.shape, f32),
            side,
            side,
        ),
        in_specs=[pl.BlockSpec(memory_space=pl.ANY)] * 3,
        out_specs=(spec,) * 4,
        scratch_shapes=[VMEM(down.shape, f32), VMEM(up.shape, f32), pltpu.SemaphoreType.DMA((4,))],
        name="finish",
    )(down, up, prompt)


def local(
    hidden,
    response_base_queries,
    attention_output_gradient,
    keys,
    values,
    adapter_down_weight,
    adapter_up_weight,
    lengths,
    offsets,
):
    n = lax.axis_size("seq")
    nz = lax.axis_size("adapter")
    sums = gradients(
        n,
        nz,
        hidden,
        response_base_queries,
        attention_output_gradient,
        adapter_down_weight,
        adapter_up_weight,
        lengths,
        offsets,
        keys,
        values,
    )
    return finish(adapter_up_weight, *sums)


def solution(mesh):
    return jax.shard_map(
        local,
        mesh=mesh,
        in_specs=(
            P("adapter", "seq", None),
            P("adapter", "seq", None),
            P("adapter", "seq", None),
            P("seq", None),
            P("seq", None),
            P("adapter", None, None),
            P("adapter", None, None),
            P("adapter"),
            P("adapter", "seq"),
        ),
        out_specs=(
            P("adapter", None, "seq"),
            P("adapter", None, None),
            P(("seq", "adapter"), None),
            P(("seq", "adapter"), None),
        ),
        check_vma=False,
    )
```
